64 devices in a mesh: req: 4 (over x, y), dap: 16 (over z, core).
Axes of the slice: x: 2, y: 2, z: 8, core: 2. Of those that a mesh axis runs over, the one named last changes fastest.
The devices are a block of a 4x4x8 slice.
Arguments:
- msa_act: bfloat16 [2048, 128, 256], P(('req', 'dap')), parts along dimension 0
- pair_act: bfloat16 [512, 128, 128], P(('req', 'dap')), parts along dimension 0
- msa_mask: int32 [2048, 128], P(('req', 'dap')), parts along dimension 0
- pair_mask: int32 [512, 128], P(('req', 'dap')), parts along dimension 0
- row_qkvg: bfloat16 [2, 256, 1024], replicated
- row_bias: bfloat16 [2, 128, 8], replicated
- row_out: bfloat16 [2, 256, 256], replicated
- col_qkvg: bfloat16 [2, 256, 1024], replicated
- col_out: bfloat16 [2, 256, 256], replicated
- mtr_in: bfloat16 [2, 256, 1024], replicated
- mtr_out: bfloat16 [2, 1024, 256], replicated
- opm_proj: bfloat16 [2, 256, 64], replicated
- opm_out: bfloat16 [2, 1024, 128], replicated
- tmo_proj: bfloat16 [2, 128, 640], replicated
- tmo_out: bfloat16 [2, 128, 128], replicated
- tmi_proj: bfloat16 [2, 128, 640], replicated
- tmi_out: bfloat16 [2, 128, 128], replicated
- tas_qkvg: bfloat16 [2, 128, 512], replicated
- tas_bias: bfloat16 [2, 128, 4], replicated
- tas_out: bfloat16 [2, 128, 128], replicated
- tae_qkvg: bfloat16 [2, 128, 512], replicated
- tae_bias: bfloat16 [2, 128, 4], replicated
- tae_out: bfloat16 [2, 128, 128], replicated
- ptr_in: bfloat16 [2, 128, 512], replicated
- ptr_out: bfloat16 [2, 512, 128], replicated
Outputs:
- output 1: bfloat16 [2048, 128, 256], P(('req', 'dap')), parts along dimension 0
- output 2: bfloat16 [512, 128, 128], P(('req', 'dap')), parts along dimension 0
There are 4 independent parts. The reference program is written for one: setup_inputs(seed, part) draws one part's arguments, and reference() takes and returns one part's arrays. A program takes and returns all parts, laid end to end along the dimension named above; an argument that names none is the same for every part.
All inputs are finite; a program needn't handle non-finite values.
Results may differ from the reference program's by a relative error of at most 0.02.
Values are sent between devices in bfloat16 or wider.
A program may use at most 768 MiB of HBM per device.

```python
import jax
import jax.numpy as jnp
from jax import lax

SEQ = 512
RES = 128
MSA_DIM = 256
PAIR_DIM = 128
MSA_HEADS = 8
MSA_HEAD_DIM = 32
PAIR_HEADS = 4
PAIR_HEAD_DIM = 32
OPM_DIM = 32
TRI_DIM = 128
LAYERS = 2

WEIGHT_NAMES = ('row_qkvg', 'row_bias', 'row_out', 'col_qkvg', 'col_out', 'mtr_in', 'mtr_out', 'opm_proj', 'opm_out', 'tmo_proj', 'tmo_out', 'tmi_proj', 'tmi_out', 'tas_qkvg', 'tas_bias', 'tas_out', 'tae_qkvg', 'tae_bias', 'tae_out', 'ptr_in', 'ptr_out')


def weight_fans():
    msa_width = MSA_HEADS * MSA_HEAD_DIM
    pair_width = PAIR_HEADS * PAIR_HEAD_DIM
    return ((MSA_DIM, 4 * msa_width), (PAIR_DIM, MSA_HEADS), (msa_width, MSA_DIM),
            (MSA_DIM, 4 * msa_width), (msa_width, MSA_DIM),
            (MSA_DIM, 4 * MSA_DIM), (4 * MSA_DIM, MSA_DIM),
            (MSA_DIM, 2 * OPM_DIM), (OPM_DIM * OPM_DIM, PAIR_DIM),
            (PAIR_DIM, 4 * TRI_DIM + PAIR_DIM), (TRI_DIM, PAIR_DIM),
            (PAIR_DIM, 4 * TRI_DIM + PAIR_DIM), (TRI_DIM, PAIR_DIM),
            (PAIR_DIM, 4 * pair_width), (PAIR_DIM, PAIR_HEADS), (pair_width, PAIR_DIM),
            (PAIR_DIM, 4 * pair_width), (PAIR_DIM, PAIR_HEADS), (pair_width, PAIR_DIM),
            (PAIR_DIM, 4 * PAIR_DIM), (4 * PAIR_DIM, PAIR_DIM))


def draw_masks(mask_key):
    key_list = jax.random.split(mask_key, 4)
    pad_len = jax.random.randint(key_list[0], (), 1, RES // 16 + 1)
    res_ids = jnp.arange(RES)
    seq_ids = jnp.arange(SEQ)[:, None]
    is_valid = res_ids < RES - pad_len
    shallow = jax.random.randint(key_list[1], (RES,), 0, 4) == 0
    depths = jnp.where(shallow, jax.random.randint(key_list[2], (RES,), 1, SEQ // 4 + 1), SEQ)
    kept_mask = (jax.random.randint(key_list[3], (SEQ, RES), 0, 8) != 0) | (seq_ids == 0)
    msa_mask = ((seq_ids < depths[None, :]) & kept_mask & is_valid[None, :]).astype(jnp.int32)
    pair_mask = (is_valid[:, None] & is_valid[None, :]).astype(jnp.int32)
    return msa_mask, pair_mask


def setup_inputs(seed: int = 0, part: int = 0) -> dict:
    part_key = jax.random.fold_in(jax.random.key(seed), part)
    key_list = jax.random.split(part_key, 3)
    shared = jax.random.normal(key_list[0], (1, RES, MSA_DIM), jnp.float32)
    spread = jax.random.normal(key_list[1], (SEQ, RES, MSA_DIM), jnp.float32)
    msa_act = (shared + spread).astype(jnp.bfloat16)
    pair_act = jax.random.normal(key_list[2], (RES, RES, PAIR_DIM), jnp.float32).astype(jnp.bfloat16)
    msa_mask, pair_mask = draw_masks(jax.random.fold_in(part_key, 5))
    inputs = {'msa_act': msa_act, 'pair_act': pair_act, 'msa_mask': msa_mask, 'pair_mask': pair_mask}
    weight_key = jax.random.key(seed + 1)
    for w_index, fan_pair in enumerate(weight_fans()):
        sample = jax.random.normal(jax.random.fold_in(weight_key, w_index), (LAYERS,) + fan_pair, jnp.float32)
        inputs[WEIGHT_NAMES[w_index]] = (sample * fan_pair[0] ** -0.5).astype(jnp.bfloat16)
    return inputs


def layer_norm(x):
    values = x.astype(jnp.float32)
    centered = values - jnp.mean(values, axis=-1, keepdims=True)
    variance = jnp.mean(centered * centered, axis=-1, keepdims=True)
    return (centered * lax.rsqrt(variance + 1e-5)).astype(jnp.bfloat16)


def linear(x, weight):
    flat_x = x.reshape(-1, x.shape[-1])
    result = jnp.dot(flat_x, weight, preferred_element_type=jnp.float32)
    return result.reshape(x.shape[:-1] + (weight.shape[-1],))


def residual(x, update):
    return (x.astype(jnp.float32) + update).astype(jnp.bfloat16)


def attend_row(x_row, bias_hij, mask_row, w_qkvg, w_out, num_heads):
    length = x_row.shape[0]
    head_width = w_out.shape[0]
    head_dim = head_width // num_heads
    projected = jnp.dot(x_row, w_qkvg, preferred_element_type=jnp.float32).astype(jnp.bfloat16).astype(jnp.float32)
    queries = projected[:, :head_width].reshape(length, num_heads, head_dim)
    keyset = projected[:, head_width:2 * head_width].reshape(length, num_heads, head_dim)
    valset = projected[:, 2 * head_width:3 * head_width].reshape(length, num_heads, head_dim)
    gate_act = jax.nn.sigmoid(projected[:, 3 * head_width:])
    logits = jnp.einsum('ihd,jhd->hij', queries, keyset) * head_dim ** -0.5 + bias_hij.astype(jnp.float32)
    logits = jnp.where(mask_row[None, None, :] > 0, logits, -1e9)
    attn_prob = jax.nn.softmax(logits, axis=-1).astype(jnp.bfloat16).astype(jnp.float32)
    attended = jnp.einsum('hij,jhd->ihd', attn_prob, valset).reshape(length, head_width)
    gated = (attended * gate_act).astype(jnp.bfloat16)
    return jnp.dot(gated, w_out, preferred_element_type=jnp.float32)


def row_attention(msa_act, pair_act, msa_mask, w_qkvg, w_bias, w_out):
    pair_bias = jnp.transpose(linear(layer_norm(pair_act), w_bias).astype(jnp.bfloat16), (2, 0, 1))
    msa_norm = layer_norm(msa_act)
    return lax.map(lambda item: attend_row(item[0], pair_bias, item[1], w_qkvg, w_out, w_bias.shape[1]), (msa_norm, msa_mask))


def column_attention(msa_act, msa_mask, w_qkvg, w_out, num_heads):
    msa_norm = jnp.swapaxes(layer_norm(msa_act), 0, 1)
    zero_bias = jnp.zeros((1, 1, 1), jnp.float32)
    update = lax.map(lambda item: attend_row(item[0], zero_bias, item[1], w_qkvg, w_out, num_heads), (msa_norm, msa_mask.T))
    return jnp.swapaxes(update, 0, 1)


def transition(x, w_in, w_out):
    hidden = jnp.maximum(linear(layer_norm(x), w_in), 0.0).astype(jnp.bfloat16)
    return linear(hidden, w_out)


def outer_product_mean(msa_act, msa_mask, w_proj, w_out):
    opm_dim = w_proj.shape[1] // 2
    projected = linear(layer_norm(msa_act), w_proj).astype(jnp.bfloat16)
    mask_bf = msa_mask.astype(jnp.bfloat16)[:, :, None]
    left_act = (projected[..., :opm_dim] * mask_bf).astype(jnp.float32)
    right_act = (projected[..., opm_dim:] * mask_bf).astype(jnp.float32)
    mask_f = msa_mask.astype(jnp.float32)
    overlap = jnp.dot(mask_f.T, mask_f)

    def outer_row(left_row):
        outer_prod = jnp.einsum('sc,sje->jce', left_row, right_act).astype(jnp.bfloat16)
        return linear(outer_prod.reshape(outer_prod.shape[0], opm_dim * opm_dim), w_out)

    update = lax.map(outer_row, jnp.swapaxes(left_act, 0, 1))
    return update / (1e-3 + overlap)[:, :, None]


def tri_mul(pair_act, pair_mask, w_proj, w_out, form):
    tri_dim = (w_proj.shape[1] - pair_act.shape[-1]) // 4
    projected = linear(layer_norm(pair_act), w_proj)
    mask_f = pair_mask.astype(jnp.float32)[:, :, None]
    left_act = (mask_f * jax.nn.sigmoid(projected[..., 2 * tri_dim:3 * tri_dim]) * projected[..., :tri_dim]).astype(jnp.bfloat16)
    right_act = (mask_f * jax.nn.sigmoid(projected[..., 3 * tri_dim:4 * tri_dim]) * projected[..., tri_dim:2 * tri_dim]).astype(jnp.bfloat16)
    gate_act = jax.nn.sigmoid(projected[..., 4 * tri_dim:])
    product = jnp.einsum(form, left_act.astype(jnp.float32), right_act.astype(jnp.float32))
    return gate_act * linear(layer_norm(product), w_out)


def tri_attention(pair_act, pair_mask, w_qkvg, w_bias, w_out):
    pair_norm = layer_norm(pair_act)
    pair_bias = jnp.transpose(linear(pair_norm, w_bias).astype(jnp.bfloat16), (2, 0, 1))
    return lax.map(lambda item: attend_row(item[0], pair_bias, item[1], w_qkvg, w_out, w_bias.shape[1]), (pair_norm, pair_mask))


def evoformer_block(msa_act, pair_act, msa_mask, pair_mask, layer_w):
    (row_qkvg, row_bias, row_out, col_qkvg, col_out, mtr_in, mtr_out, opm_proj, opm_out,
     tmo_proj, tmo_out, tmi_proj, tmi_out, tas_qkvg, tas_bias, tas_out,
     tae_qkvg, tae_bias, tae_out, ptr_in, ptr_out) = layer_w
    msa_act = residual(msa_act, row_attention(msa_act, pair_act, msa_mask, row_qkvg, row_bias, row_out))
    msa_act = residual(msa_act, column_attention(msa_act, msa_mask, col_qkvg, col_out, row_bias.shape[1]))
    msa_act = residual(msa_act, transition(msa_act, mtr_in, mtr_out))
    pair_act = residual(pair_act, outer_product_mean(msa_act, msa_mask, opm_proj, opm_out))
    pair_act = residual(pair_act, tri_mul(pair_act, pair_mask, tmo_proj, tmo_out, 'ikc,jkc->ijc'))
    pair_act = residual(pair_act, tri_mul(pair_act, pair_mask, tmi_proj, tmi_out, 'kic,kjc->ijc'))
    pair_act = residual(pair_act, tri_attention(pair_act, pair_mask, tas_qkvg, tas_bias, tas_out))
    pair_swap = jnp.swapaxes(pair_act, 0, 1)
    pair_act = residual(pair_act, jnp.swapaxes(tri_attention(pair_swap, pair_mask.T, tae_qkvg, tae_bias, tae_out), 0, 1))
    pair_act = residual(pair_act, transition(pair_act, ptr_in, ptr_out))
    return msa_act, pair_act


def reference(msa_act, pair_act, msa_mask, pair_mask, row_qkvg, row_bias, row_out, col_qkvg, col_out, mtr_in, mtr_out, opm_proj, opm_out, tmo_proj, tmo_out, tmi_proj, tmi_out, tas_qkvg, tas_bias, tas_out, tae_qkvg, tae_bias, tae_out, ptr_in, ptr_out):
    stacked = (row_qkvg, row_bias, row_out, col_qkvg, col_out, mtr_in, mtr_out, opm_proj, opm_out,
               tmo_proj, tmo_out, tmi_proj, tmi_out, tas_qkvg, tas_bias, tas_out,
               tae_qkvg, tae_bias, tae_out, ptr_in, ptr_out)

    def step(carry, layer_w):
        return evoformer_block(carry[0], carry[1], msa_mask, pair_mask, layer_w), None

    carried, ignored = lax.scan(step, (msa_act, pair_act), stacked)
    return carried[0], carried[1]
```

```python
import functools
import math

import jax
import jax.numpy as jnp
from jax import lax
from jax.experimental import pallas as pl
from jax.experimental.pallas import tpu as pltpu
from jax.sharding import PartitionSpec as P

GROUP_AXIS = 'dap'
PARTS_AXIS = 'req'
LOG2E = math.log2(math.e)
MASKED = -1e9 * LOG2E
LANES = 128
F32 = jnp.float32
BF16 = jnp.bfloat16
NT = (((1,), (1,)), ((), ()))
TN = (((0,), (0,)), ((), ()))


def layer_norm_f32(values):
    centered = values - jnp.mean(values, axis=-1, keepdims=True)
    variance = jnp.mean(centered * centered, axis=-1, keepdims=True)
    return (centered * lax.rsqrt(variance + 1e-5)).astype(BF16)


def layer_norm(x):
    return layer_norm_f32(x.astype(F32))


def residual(x, update):
    return (x.astype(F32) + update).astype(BF16)


def dense(x, weight):
    return jnp.einsum('...c,cf->...f', x, weight, preferred_element_type=F32)


def softmax_keys_first(logits):
    top = jnp.max(logits, axis=0, keepdims=True)
    raised = jnp.exp2(logits - top)
    total = jnp.sum(raised, axis=0, keepdims=True)
    return (raised * (1.0 / total)).astype(BF16)


def row_attention_kernel(heads, x_ref, mask_ref, bias_ref, w_ref, wo_ref, o_ref, proj, gated, *stage, swap_in, swap_out):
    width = wo_ref.shape[0]
    head_dim = width // heads
    scale = head_dim ** -0.5 * LOG2E
    n_seq = mask_ref.shape[0]
    length = mask_ref.shape[1]
    stage = list(stage)
    if swap_in:
        stage_in = stage.pop(0)
        for part in range(stage_in.shape[0]):
            stage_in[part] = x_ref[:, :, part * LANES:(part + 1) * LANES].astype(F32).reshape(stage_in.shape[1:])
    if swap_out:
        stage_out = stage.pop(0)

    def one_row(s, carry):
        if swap_in:
            x = jnp.concatenate([stage_in[part, pl.ds(s, length, stride=n_seq), :] for part in range(stage_in.shape[0])], -1)
        else:
            x = x_ref[s].astype(F32)
        x_norm = layer_norm_f32(x)
        proj[...] = lax.dot_general(w_ref[...], x_norm, NT, preferred_element_type=F32).astype(BF16)
        kept = mask_ref[s] > 0.0
        for h in range(heads):
            lo = h * head_dim
            q_t = proj[lo:lo + head_dim, :]
            k_t = proj[width + lo:width + lo + head_dim, :]
            v_t = proj[2 * width + lo:2 * width + lo + head_dim, :]
            g_t = proj[3 * width + lo:3 * width + lo + head_dim, :].astype(F32)
            logits = lax.dot_general(k_t, q_t, TN, preferred_element_type=F32) * scale + bias_ref[h]
            prob = softmax_keys_first(jnp.where(kept, logits, MASKED))
            out_t = jnp.dot(v_t, prob, preferred_element_type=F32)
            gated[lo:lo + head_dim, :] = (out_t * jax.nn.sigmoid(g_t)).astype(BF16)
        update = lax.dot_general(gated[...], wo_ref[...], TN, preferred_element_type=F32)
        result = x + update
        if swap_out:
            for part in range(stage_out.shape[0]):
                stage_out[part, pl.ds(s, length, stride=n_seq), :] = result[:, part * LANES:(part + 1) * LANES]
        else:
            o_ref[s] = result.astype(BF16)
        return carry

    lax.fori_loop(0, n_seq, one_row, 0)
    if swap_out:
        for part in range(stage_out.shape[0]):
            o_ref[:, :, part * LANES:(part + 1) * LANES] = stage_out[part].reshape(length, n_seq, LANES).astype(BF16)


def row_attention(x, mask_lanes, bias_t, w_qkvg_t, w_out, heads, block, swap_in=False, swap_out=False):
    n_rows, length = mask_lanes.shape[:2]
    dim = x.shape[-1]
    width = w_out.shape[0]
    natural = pl.BlockSpec((block, length, dim), lambda i: (i, 0, 0))
    swapped = pl.BlockSpec((length, block, dim), lambda i: (0, i, 0))
    whole2 = lambda shape: pl.BlockSpec(shape, lambda i: (0,) * len(shape))
    scratch = [pltpu.VMEM((4 * width, length), BF16), pltpu.VMEM((width, length), BF16)]
    scratch += [pltpu.VMEM((dim // LANES, length * block, LANES), F32)] * (int(swap_in) + int(swap_out))
    out_shape = (length, n_rows, dim) if swap_out else (n_rows, length, dim)
    return pl.pallas_call(
        functools.partial(row_attention_kernel, heads, swap_in=swap_in, swap_out=swap_out),
        grid=(n_rows // block,),
        in_specs=[
            swapped if swap_in else natural,
            pl.BlockSpec((block, length, length), lambda i: (i, 0, 0)),
            whole2(bias_t.shape), whole2(w_qkvg_t.shape), whole2(w_out.shape),
        ],
        out_specs=swapped if swap_out else natural,
        out_shape=jax.ShapeDtypeStruct(out_shape, BF16),
        scratch_shapes=scratch,
        cost_estimate=pl.CostEstimate(flops=n_rows * length * (dim * width * 10 + 4 * length * width), bytes_accessed=4 * x.size, transcendentals=n_rows * heads * length * length),
        name='row_attention',
    )(x, mask_lanes, bias_t, w_qkvg_t, w_out)


def column_kernel(heads, x_ref, mask_ref, mrow_ref, w_ref, wo_ref, win_ref, wtr_ref, wopm_ref, o_ref, ab_ref, proj, gated):
    width = wo_ref.shape[0]
    head_dim = width // heads
    scale = head_dim ** -0.5 * LOG2E
    length = mask_ref.shape[1]
    lanes = mask_ref.shape[2]
    x = x_ref[...].reshape(length, x_ref.shape[-1]).astype(F32)
    proj[...] = lax.dot_general(w_ref[...], layer_norm_f32(x), NT, preferred_element_type=F32).astype(BF16)

    def one_head(h, carry):
        lo = pl.multiple_of(h * head_dim, head_dim)
        keys = proj[pl.ds(width + lo, head_dim), :].T
        v_t = proj[pl.ds(2 * width + lo, head_dim), :]
        for c in range(length // lanes):
            cols = slice(c * lanes, (c + 1) * lanes)
            q_t = proj[pl.ds(lo, head_dim), cols]
            g_t = proj[pl.ds(3 * width + lo, head_dim), cols].astype(F32)
            logits = jnp.dot(keys, q_t, preferred_element_type=F32) * scale
            prob = softmax_keys_first(jnp.where(mask_ref[0] > 0.0, logits, MASKED))
            out_t = jnp.dot(v_t, prob, preferred_element_type=F32)
            gated[pl.ds(lo, head_dim), cols] = (out_t * jax.nn.sigmoid(g_t)).astype(BF16)
        return carry

    lax.fori_loop(0, heads, one_head, 0)
    update = lax.dot_general(gated[...], wo_ref[...], TN, preferred_element_type=F32)
    x = (x + update).astype(BF16).astype(F32)
    hidden = jnp.maximum(jnp.dot(layer_norm_f32(x), win_ref[...], preferred_element_type=F32), 0.0).astype(BF16)
    x = (x + jnp.dot(hidden, wtr_ref[...], preferred_element_type=F32)).astype(BF16)
    o_ref[...] = x.reshape(o_ref.shape)
    ab_t = lax.dot_general(wopm_ref[...], layer_norm_f32(x.astype(F32)), NT, preferred_element_type=F32).astype(BF16)
    ab_ref[0] = (ab_t.astype(F32) * mrow_ref[0]).astype(BF16)


def column_stack(x, mask_lanes, mask_row, w_qkvg_t, w_out, w_in, w_tr, w_opm_t, heads):
    n_dev, n_res, n_seq, dim = x.shape
    length = n_dev * n_seq
    width = w_out.shape[0]
    block = pl.BlockSpec((n_dev, 1, n_seq, dim), lambda r: (0, r, 0, 0))
    whole2 = lambda shape: pl.BlockSpec(shape, lambda i: (0,) * len(shape))
    n_opm = w_opm_t.shape[0]
    return pl.pallas_call(
        functools.partial(column_kernel, heads),
        grid=(n_res,),
        in_specs=[
            block,
            pl.BlockSpec((1, length, mask_lanes.shape[2]), lambda r: (r, 0, 0)),
            pl.BlockSpec((1, 1, length), lambda r: (r, 0, 0)),
            whole2(w_qkvg_t.shape), whole2(w_out.shape), whole2(w_in.shape), whole2(w_tr.shape), whole2(w_opm_t.shape),
        ],
        out_specs=[block, pl.BlockSpec((1, n_opm, length), lambda r: (r, 0, 0))],
        out_shape=[jax.ShapeDtypeStruct(x.shape, BF16), jax.ShapeDtypeStruct((n_res, n_opm, length), BF16)],
        scratch_shapes=[pltpu.VMEM((4 * width, length), BF16), pltpu.VMEM((width, length), BF16)],
        cost_estimate=pl.CostEstimate(flops=n_res * length * (dim * width * 26 + 4 * length * width), bytes_accessed=4 * x.size, transcendentals=n_res * heads * length * length),
        name='column_stack',
    )(x, mask_lanes, mask_row, w_qkvg_t, w_out, w_in, w_tr, w_opm_t)


def head_bias(pair_norm, w_bias):
    return jnp.einsum('ijc,ch->hij', pair_norm, w_bias, preferred_element_type=F32).astype(BF16)


def gather_bias(pair_rows, w_bias):
    full = lax.all_gather(head_bias(layer_norm(pair_rows), w_bias), GROUP_AXIS, axis=1, tiled=True)
    return jnp.swapaxes(full, 1, 2).astype(F32) * LOG2E


def transition(x, w_in, w_out):
    hidden = jnp.maximum(dense(layer_norm(x), w_in), 0.0).astype(BF16)
    return dense(hidden, w_out)


def outer_update(ab, overlap, w_out):
    opm_dim = ab.shape[1] // 2
    left_act = ab[:, :opm_dim]
    right_full = lax.all_gather(ab[:, opm_dim:], GROUP_AXIS, axis=0, tiled=True)
    outer_prod = jnp.einsum('ics,jes->ijce', left_act, right_full, preferred_element_type=F32).astype(BF16)
    n_rows, n_cols = outer_prod.shape[:2]
    update = dense(outer_prod.reshape(n_rows, n_cols, opm_dim * opm_dim), w_out)
    return update / (1e-3 + overlap)[:, :, None]


def tri_gates(pair_rows, mask_rows, w_proj):
    tri_dim = (w_proj.shape[1] - pair_rows.shape[-1]) // 4
    projected = dense(layer_norm(pair_rows), w_proj)
    mask_f = mask_rows[:, :, None]
    left_act = (mask_f * jax.nn.sigmoid(projected[..., 2 * tri_dim:3 * tri_dim]) * projected[..., :tri_dim]).astype(BF16)
    right_act = (mask_f * jax.nn.sigmoid(projected[..., 3 * tri_dim:4 * tri_dim]) * projected[..., tri_dim:2 * tri_dim]).astype(BF16)
    gate_act = jax.nn.sigmoid(projected[..., 4 * tri_dim:])
    return left_act, right_act, gate_act


def tri_finish(product, gate_act, w_out):
    return gate_act * dense(layer_norm(product), w_out)


def tri_attention(pair_rows, mask_lanes, w_qkvg, w_bias, w_out):
    bias_t = gather_bias(pair_rows, w_bias)
    return row_attention(pair_rows, mask_lanes, bias_t, w_qkvg.T, w_out, w_bias.shape[1], pair_rows.shape[0])


def pair_stack(pair_loc, masks, pair_w):
    (tmo_proj, tmo_out, tmi_proj, tmi_out, tas_qkvg, tas_bias, tas_out,
     tae_qkvg, tae_bias, tae_out, ptr_in, ptr_out) = pair_w
    pair_mask = masks['pair_rows']
    left_act, right_act, gate_act = tri_gates(pair_loc, pair_mask, tmo_proj)
    right_full = lax.all_gather(right_act, GROUP_AXIS, axis=0, tiled=True)
    product = jnp.einsum('ikc,jkc->ijc', left_act, right_full, preferred_element_type=F32)
    pair_loc = residual(pair_loc, tri_finish(product, gate_act, tmo_out))
    left_act, right_act, gate_act = tri_gates(pair_loc, pair_mask, tmi_proj)
    left_cols = lax.all_to_all(left_act, GROUP_AXIS, 1, 0, tiled=True)
    right_full = lax.all_gather(right_act, GROUP_AXIS, axis=0, tiled=True)
    product = jnp.einsum('kic,kjc->ijc', left_cols, right_full, preferred_element_type=F32)
    pair_loc = residual(pair_loc, tri_finish(product, gate_act, tmi_out))
    pair_loc = tri_attention(pair_loc, masks['start'], tas_qkvg, tas_bias, tas_out)
    pair_cols = lax.all_to_all(pair_loc, GROUP_AXIS, 1, 0, tiled=True)
    pair_t = jnp.swapaxes(pair_cols, 0, 1)
    pair_t = tri_attention(pair_t, masks['end'], tae_qkvg, tae_bias, tae_out)
    pair_loc = lax.all_to_all(jnp.swapaxes(pair_t, 0, 1), GROUP_AXIS, 0, 1, tiled=True)
    return residual(pair_loc, transition(pair_loc, ptr_in, ptr_out))


def evoformer_block(value_a7, pair_loc, masks, layer_w, first):
    (row_qkvg, row_bias, row_out, col_qkvg, col_out, mtr_in, mtr_out, opm_proj, opm_out) = layer_w[:9]
    heads = row_bias.shape[1]
    n_dev = masks['n_dev']
    bias_t = gather_bias(pair_loc, row_bias)
    value_a7 = row_attention(value_a7, masks['seq'], bias_t, row_qkvg.T, row_out, heads, 16, swap_in=not first, swap_out=True)
    length, n_seq, dim = value_a7.shape
    by_dev = value_a7.reshape(n_dev, length // n_dev, n_seq, dim)
    by_res = lax.all_to_all(by_dev, GROUP_AXIS, 0, 0, tiled=True)
    by_res, ab = column_stack(by_res, masks['res'], masks['res_row'], col_qkvg.T, col_out, mtr_in, mtr_out, opm_proj.T, heads)
    pair_loc = residual(pair_loc, outer_update(ab, masks['overlap'], opm_out))
    pair_loc = pair_stack(pair_loc, masks, layer_w[9:])
    value_a7 = lax.all_to_all(by_res, GROUP_AXIS, 0, 0, tiled=True).reshape(length, n_seq, dim)
    return value_a7, pair_loc


def make_masks(msa_mask, pair_mask, n_dev):
    shard_idx = lax.axis_index(GROUP_AXIS)
    n_seq, length = msa_mask.shape
    n_res = pair_mask.shape[0]
    packed = jnp.concatenate([msa_mask, pair_mask], 0).astype(BF16)
    full = lax.all_gather(packed, GROUP_AXIS, axis=0, tiled=True).reshape(n_dev, n_seq + n_res, length).astype(F32)
    full_msa = full[:, :n_seq].reshape(n_dev * n_seq, length)
    full_pair = full[:, n_seq:].reshape(n_dev * n_res, length)
    res_mask = lax.dynamic_slice_in_dim(full_msa, shard_idx * n_res, n_res, 1).T
    end_mask = lax.dynamic_slice_in_dim(full_pair, shard_idx * n_res, n_res, 1).T
    lanes = lambda mask: jnp.broadcast_to(mask.astype(F32)[:, :, None], mask.shape + (length,))
    return {
        'n_dev': n_dev,
        'seq': lanes(msa_mask),
        'res': lanes(res_mask),
        'res_row': res_mask[:, None, :],
        'pair_rows': pair_mask.astype(F32),
        'start': lanes(pair_mask),
        'end': lanes(end_mask),
        'overlap': jnp.dot(res_mask, full_msa, precision=lax.Precision.DEFAULT, preferred_element_type=F32),
    }


def solution(mesh):
    row_spec = P((PARTS_AXIS, GROUP_AXIS))
    n_dev = mesh.shape[GROUP_AXIS]

    def local_body(value_a7, pair_loc, msa_mask, pair_mask, *weights):
        masks = make_masks(msa_mask, pair_mask, n_dev)
        for layer_idx in range(weights[0].shape[0]):
            layer_w = tuple(weight[layer_idx] for weight in weights)
            value_a7, pair_loc = evoformer_block(value_a7, pair_loc, masks, layer_w, layer_idx == 0)
        return jnp.swapaxes(value_a7, 0, 1), pair_loc

    def run_blocks(*arrays):
        n_weights = len(arrays) - 4
        return jax.shard_map(local_body, mesh=mesh, in_specs=(row_spec,) * 4 + (P(),) * n_weights, out_specs=(row_spec, row_spec), check_vma=False)(*arrays)

    return run_blocks
```

```python
import functools
import math

import jax
import jax.numpy as jnp
from jax import lax
from jax.experimental import pallas as pl
from jax.experimental.pallas import tpu as pltpu
from jax.sharding import PartitionSpec as P

GROUP_AXIS = 'dap'
PARTS_AXIS = 'req'
LOG2E = math.log2(math.e)
MASKED = -1e9 * LOG2E
LANES = 128
AHEAD = 4
F32 = jnp.float32
BF16 = jnp.bfloat16
NT = (((1,), (1,)), ((), ()))
TN = (((0,), (0,)), ((), ()))


def layer_norm_f32(values):
    centered = values - jnp.mean(values, axis=-1, keepdims=True)
    variance = jnp.mean(centered * centered, axis=-1, keepdims=True)
    return (centered * lax.rsqrt(variance + 1e-5)).astype(BF16)


def layer_norm(x):
    return layer_norm_f32(x.astype(F32))


def residual(x, update):
    return (x.astype(F32) + update).astype(BF16)


def dense(x, weight):
    return jnp.einsum('...c,cf->...f', x, weight, preferred_element_type=F32)


def softmax_keys_first(logits):
    top = jnp.max(logits, axis=0, keepdims=True)
    raised = jnp.exp2(logits - top)
    total = jnp.sum(raised, axis=0, keepdims=True)
    return (raised * (1.0 / total)).astype(BF16)


def pipelined_units(units, ahead, first_stage, second_stage):
    ready = {}
    for idx in range(min(ahead, len(units))):
        ready[idx] = first_stage(*units[idx])
    for idx in range(len(units)):
        if idx + ahead < len(units):
            ready[idx + ahead] = first_stage(*units[idx + ahead])
        second_stage(ready.pop(idx), *units[idx])


def row_attention_kernel(heads, group, x_ref, mask_ref, bias_ref, w_ref, wo_ref, o_ref, proj, gated, *stage, swap_in, swap_out):
    width = wo_ref.shape[0]
    head_dim = width // heads
    scale = head_dim ** -0.5 * LOG2E
    n_seq = mask_ref.shape[0]
    length = mask_ref.shape[1]
    stage = list(stage)
    if swap_in:
        stage_in = stage.pop(0)
        for part in range(stage_in.shape[0]):
            stage_in[part] = x_ref[:, :, part * LANES:(part + 1) * LANES].astype(F32).reshape(stage_in.shape[1:])
    if swap_out:
        stage_out = stage.pop(0)

    def load_row(s):
        if swap_in:
            return jnp.concatenate([stage_in[part, pl.ds(s, length, stride=n_seq), :] for part in range(stage_in.shape[0])], -1)
        return x_ref[s].astype(F32)

    def head_rows(j, part, h):
        lo = part * width + h * head_dim
        return proj[j, lo:lo + head_dim, :]

    def some_rows(t, carry):
        base = t * group
        normed = [layer_norm_f32(load_row(base + j)) for j in range(group)]
        for j in range(group):
            proj[j] = lax.dot_general(w_ref[...], normed[j], NT, preferred_element_type=F32).astype(BF16)

        def logits_of(j, h):
            return lax.dot_general(head_rows(j, 1, h), head_rows(j, 0, h), TN, preferred_element_type=F32)

        def finish(raw, j, h):
            logits = jnp.where(mask_ref[base + j] > 0.0, raw * scale + bias_ref[h], MASKED)
            out_t = jnp.dot(head_rows(j, 2, h), softmax_keys_first(logits), preferred_element_type=F32)
            gate = jax.nn.sigmoid(head_rows(j, 3, h).astype(F32))
            gated[j, h * head_dim:(h + 1) * head_dim, :] = (out_t * gate).astype(BF16)

        pipelined_units([(j, h) for j in range(group) for h in range(heads)], AHEAD, logits_of, finish)
        for j in range(group):
            s = base + j
            result = load_row(s) + lax.dot_general(gated[j], wo_ref[...], TN, preferred_element_type=F32)
            if swap_out:
                for part in range(stage_out.shape[0]):
                    stage_out[part, pl.ds(s, length, stride=n_seq), :] = result[:, part * LANES:(part + 1) * LANES]
            else:
                o_ref[s] = result.astype(BF16)
        return carry

    lax.fori_loop(0, n_seq // group, some_rows, 0)
    if swap_out:
        for part in range(stage_out.shape[0]):
            o_ref[:, :, part * LANES:(part + 1) * LANES] = stage_out[part].reshape(length, n_seq, LANES).astype(BF16)


def row_attention(x, mask_lanes, bias_t, w_qkvg_t, w_out, heads, block, group, swap_in=False, swap_out=False):
    n_rows, length = mask_lanes.shape[:2]
    dim = x.shape[-1]
    width = w_out.shape[0]
    natural = pl.BlockSpec((block, length, dim), lambda i: (i, 0, 0))
    swapped = pl.BlockSpec((length, block, dim), lambda i: (0, i, 0))
    whole2 = lambda shape: pl.BlockSpec(shape, lambda i: (0,) * len(shape))
    scratch = [pltpu.VMEM((group, 4 * width, length), BF16), pltpu.VMEM((group, width, length), BF16)]
    scratch += [pltpu.VMEM((dim // LANES, length * block, LANES), F32)] * (int(swap_in) + int(swap_out))
    out_shape = (length, n_rows, dim) if swap_out else (n_rows, length, dim)
    return pl.pallas_call(
        functools.partial(row_attention_kernel, heads, group, swap_in=swap_in, swap_out=swap_out),
        grid=(n_rows // block,),
        in_specs=[
            swapped if swap_in else natural,
            pl.BlockSpec((block, length, length), lambda i: (i, 0, 0)),
            whole2(bias_t.shape), whole2(w_qkvg_t.shape), whole2(w_out.shape),
        ],
        out_specs=swapped if swap_out else natural,
        out_shape=jax.ShapeDtypeStruct(out_shape, BF16),
        scratch_shapes=scratch,
        cost_estimate=pl.CostEstimate(flops=n_rows * length * (dim * width * 10 + 4 * length * width), bytes_accessed=4 * x.size, transcendentals=n_rows * heads * length * length),
        name='row_attention',
    )(x, mask_lanes, bias_t, w_qkvg_t, w_out)


def column_kernel(heads, x_ref, mask_ref, mrow_ref, w_ref, wo_ref, win_ref, wtr_ref, wopm_ref, o_ref, ab_ref, proj, gated):
    width = wo_ref.shape[0]
    head_dim = width // heads
    scale = head_dim ** -0.5 * LOG2E
    length = mask_ref.shape[1]
    lanes = mask_ref.shape[2]
    x = x_ref[...].reshape(length, x_ref.shape[-1]).astype(F32)
    proj[...] = lax.dot_general(w_ref[...], layer_norm_f32(x), NT, preferred_element_type=F32).astype(BF16)

    def head_rows(part, h, cols=slice(None)):
        lo = part * width + h * head_dim
        return proj[lo:lo + head_dim, cols]

    def columns(c):
        return slice(c * lanes, (c + 1) * lanes)

    def logits_of(h, c):
        return lax.dot_general(head_rows(1, h), head_rows(0, h, columns(c)), TN, preferred_element_type=F32)

    def finish(raw, h, c):
        logits = jnp.where(mask_ref[0] > 0.0, raw * scale, MASKED)
        out_t = jnp.dot(head_rows(2, h), softmax_keys_first(logits), preferred_element_type=F32)
        gate = jax.nn.sigmoid(head_rows(3, h, columns(c)).astype(F32))
        gated[h * head_dim:(h + 1) * head_dim, columns(c)] = (out_t * gate).astype(BF16)

    pipelined_units([(h, c) for h in range(heads) for c in range(length // lanes)], AHEAD, logits_of, finish)
    update = lax.dot_general(gated[...], wo_ref[...], TN, preferred_element_type=F32)
    x = (x + update).astype(BF16).astype(F32)
    hidden = jnp.maximum(jnp.dot(layer_norm_f32(x), win_ref[...], preferred_element_type=F32), 0.0).astype(BF16)
    x = (x + jnp.dot(hidden, wtr_ref[...], preferred_element_type=F32)).astype(BF16)
    o_ref[...] = x.reshape(o_ref.shape)
    ab_t = lax.dot_general(wopm_ref[...], layer_norm_f32(x.astype(F32)), NT, preferred_element_type=F32).astype(BF16)
    ab_ref[0] = (ab_t.astype(F32) * mrow_ref[0]).astype(BF16)


def column_stack(x, mask_lanes, mask_row, w_qkvg_t, w_out, w_in, w_tr, w_opm_t, heads):
    n_dev, n_res, n_seq, dim = x.shape
    length = n_dev * n_seq
    width = w_out.shape[0]
    block = pl.BlockSpec((n_dev, 1, n_seq, dim), lambda r: (0, r, 0, 0))
    whole2 = lambda shape: pl.BlockSpec(shape, lambda i: (0,) * len(shape))
    n_opm = w_opm_t.shape[0]
    return pl.pallas_call(
        functools.partial(column_kernel, heads),
        grid=(n_res,),
        in_specs=[
            block,
            pl.BlockSpec((1, length, mask_lanes.shape[2]), lambda r: (r, 0, 0)),
            pl.BlockSpec((1, 1, length), lambda r: (r, 0, 0)),
            whole2(w_qkvg_t.shape), whole2(w_out.shape), whole2(w_in.shape), whole2(w_tr.shape), whole2(w_opm_t.shape),
        ],
        out_specs=[block, pl.BlockSpec((1, n_opm, length), lambda r: (r, 0, 0))],
        out_shape=[jax.ShapeDtypeStruct(x.shape, BF16), jax.ShapeDtypeStruct((n_res, n_opm, length), BF16)],
        scratch_shapes=[pltpu.VMEM((4 * width, length), BF16), pltpu.VMEM((width, length), BF16)],
        cost_estimate=pl.CostEstimate(flops=n_res * length * (dim * width * 26 + 4 * length * width), bytes_accessed=4 * x.size, transcendentals=n_res * heads * length * length),
        name='column_stack',
    )(x, mask_lanes, mask_row, w_qkvg_t, w_out, w_in, w_tr, w_opm_t)


class Exchange:
    def __init__(self, n_dev, me, sends, recvs):
        self.n_dev, self.me, self.sends, self.recvs, self.used = n_dev, me, sends, recvs, 0

    def start(self, source, target, broadcast=False):
        phase = self.used
        self.used += 1
        pick = (lambda d: source) if broadcast else (lambda d: source.at[d])

        def copy(dst_dev, slot):
            return pltpu.make_async_remote_copy(
                src_ref=pick(dst_dev), dst_ref=target.at[slot], send_sem=self.sends.at[phase, dst_dev], recv_sem=self.recvs.at[phase, slot],
                device_id={GROUP_AXIS: dst_dev}, device_id_type=pl.DeviceIdType.MESH)

        def send(step, carry):
            copy(lax.rem(self.me + step, self.n_dev), self.me).start()
            return carry

        lax.fori_loop(1, self.n_dev, send, 0)
        target[self.me] = source[...] if broadcast else source[self.me]

        def finish():
            def wait(step, carry):
                other = lax.rem(self.me + step, self.n_dev)
                copy(other, other).wait_recv()
                copy(other, self.me).wait_send()
                return carry

            lax.fori_loop(1, self.n_dev, wait, 0)

        return finish


def entry_barrier(n_dev, me):
    barrier = pltpu.get_barrier_semaphore()

    def signal(step, carry):
        pl.semaphore_signal(barrier, inc=1, device_id={GROUP_AXIS: lax.rem(me + step, n_dev)}, device_id_type=pl.DeviceIdType.MESH)
        return carry

    lax.fori_loop(1, n_dev, signal, 0)
    pl.semaphore_wait(barrier, n_dev - 1)


def pair_kernel(n_dev, with_bias, *refs):
    (z_ref, mrow_ref, start_ref, end_ref, m_ref,
     tmo_w, tmo_g, tmo_out, tmi_w, tmi_g, tmi_out, tas_w, tas_b, tas_out, tae_w, tae_b, tae_out, ptr_in, ptr_out, next_b,
     o_ref, mback_ref, bias_ref,
     zbuf, tbuf, stage, ab_send, ab_recv, x_send, x_recv, ln_stage, gate, proj, gated, bias_t, bias_send, bias_recv, z_send, z_recv, zb_recv, nb_send, nb_recv,
     sends, recvs, m_sends, m_recvs, m_own) = refs
    n_res, length, dim = z_ref.shape
    tri = tmo_out.shape[0]
    n_chan = tri // n_dev
    tokens = n_res * length
    me = lax.axis_index(GROUP_AXIS)
    entry_barrier(n_dev, me)
    exchange = Exchange(n_dev, me, sends, recvs)

    def m_copy(dst_dev, slot):
        return pltpu.make_async_remote_copy(
            src_ref=m_ref.at[dst_dev], dst_ref=mback_ref.at[slot], send_sem=m_sends.at[dst_dev], recv_sem=m_recvs.at[slot],
            device_id={GROUP_AXIS: dst_dev}, device_id_type=pl.DeviceIdType.MESH)

    own = pltpu.make_async_copy(m_ref.at[me], mback_ref.at[me], m_own)
    own.start()

    def m_steps(lo, hi):
        def send(step, carry):
            m_copy(lax.rem(me + step, n_dev), me).start()
            return carry
        lax.fori_loop(lo, hi, send, 0)

    def normed_tokens():
        return layer_norm_f32(zbuf[...].astype(F32).reshape(tokens, dim))

    def tri_mul(turn, w_ref, g_ref, out_ref, contract):
        x_norm = normed_tokens()
        for part in range(2):
            value = lax.dot_general(w_ref[part * tri:(part + 1) * tri, :], x_norm, NT, preferred_element_type=F32)
            opened = lax.dot_general(w_ref[(2 + part) * tri:(3 + part) * tri, :], x_norm, NT, preferred_element_type=F32)
            gated_t = mrow_ref[...] * jax.nn.sigmoid(opened) * value
            for d in range(n_dev):
                for i in range(n_res):
                    tile = gated_t[d * n_chan:(d + 1) * n_chan, i * length:(i + 1) * length]
                    stage[pl.ds(d * n_chan * n_res + i, n_chan, stride=n_res), :] = tile
            ab_send[turn, :, part] = stage[...].reshape(n_dev, n_chan, n_res, length).astype(BF16)
        arrived = exchange.start(ab_send.at[turn], ab_recv.at[turn])
        m_steps(1 + 4 * turn, 3 + 4 * turn)
        gate[...] = jax.nn.sigmoid(jnp.dot(x_norm, g_ref[...], preferred_element_type=F32))
        arrived()
        for c in range(n_chan):
            left = ab_recv[turn, :, 0, c].astype(F32).reshape(length, length).astype(BF16)
            right = ab_recv[turn, :, 1, c].astype(F32).reshape(length, length).astype(BF16)
            product = lax.dot_general(left, right, contract, preferred_element_type=F32)
            x_send[turn, :, c] = product.reshape(n_dev, n_res, length)
        arrived = exchange.start(x_send.at[turn], x_recv.at[turn])
        m_steps(3 + 4 * turn, 5 + 4 * turn)
        arrived()
        values = x_recv[turn].reshape(tri, n_res, length)
        centered = values - jnp.mean(values, axis=0, keepdims=True)
        inverse = lax.rsqrt(jnp.mean(centered * centered, axis=0, keepdims=True) + 1e-5)
        pitch = tri + 8
        for c in range(tri):
            ln_stage[pl.ds(c, n_res, stride=pitch), :] = centered[c] * inverse[0]
        for i in range(n_res):
            columns = ln_stage[i * pitch:i * pitch + tri, :].astype(BF16)
            update = gate[i * length:(i + 1) * length, :] * lax.dot_general(columns, out_ref[...], TN, preferred_element_type=F32)
            zbuf[i] = (zbuf[i].astype(F32) + update).astype(BF16)

    def local_bias(x_norm, b_ref, send_ref):
        heads_pad = b_ref.shape[0]
        rows = lax.dot_general(b_ref[...], x_norm, NT, preferred_element_type=F32)
        for i in range(n_res):
            stage[pl.ds(i, heads_pad, stride=n_res), :] = rows[:, i * length:(i + 1) * length]
        heads = send_ref.shape[0]
        send_ref[...] = stage[0:heads * n_res, :].reshape(heads, n_res, length).astype(BF16)

    def attention(source, w_ref, out_ref, mask_ref, heads):
        width = out_ref.shape[0]
        head_dim = width // heads
        scale = head_dim ** -0.5 * LOG2E
        half = proj.shape[0]
        head_rows = lambda j, part, h: proj[j, part * width + h * head_dim:part * width + (h + 1) * head_dim, :]

        def some(t, carry):
            base = t * half
            normed = [layer_norm_f32(source[base + j].astype(F32)) for j in range(half)]
            for j in range(half):
                proj[j] = lax.dot_general(w_ref[...], normed[j], NT, preferred_element_type=F32).astype(BF16)

            def logits_of(j, h):
                return lax.dot_general(head_rows(j, 1, h), head_rows(j, 0, h), TN, preferred_element_type=F32)

            def finish(raw, j, h):
                logits = jnp.where(mask_ref[base + j] > 0.0, raw * scale + bias_t[h], MASKED)
                out_t = jnp.dot(head_rows(j, 2, h), softmax_keys_first(logits), preferred_element_type=F32)
                opened = jax.nn.sigmoid(head_rows(j, 3, h).astype(F32))
                gated[j, h * head_dim:(h + 1) * head_dim, :] = (out_t * opened).astype(BF16)

            pipelined_units([(j, h) for j in range(half) for h in range(heads)], AHEAD, logits_of, finish)
            for j in range(half):
                update = lax.dot_general(gated[j], out_ref[...], TN, preferred_element_type=F32)
                source[base + j] = (source[base + j].astype(F32) + update).astype(BF16)
            return carry

        lax.fori_loop(0, n_res // half, some, 0)

    def swap_blocks(source):
        for i in range(n_res):
            row = source[i].astype(F32)
            for d in range(n_dev):
                stage[pl.ds(d * n_res * n_res + i, n_res, stride=n_res), :] = row[d * n_res:(d + 1) * n_res, :]
        return stage[...].reshape(n_dev, n_res, n_res, dim).astype(BF16)

    def rows_of(received, i):
        return received[:, i].astype(F32).reshape(length, dim).astype(BF16)

    heads = bias_send.shape[1]
    zbuf[...] = z_ref[...]
    tri_mul(0, tmo_w, tmo_g, tmo_out, NT)
    tri_mul(1, tmi_w, tmi_g, tmi_out, TN)
    local_bias(normed_tokens(), tas_b, bias_send.at[0])
    arrived = exchange.start(bias_send.at[0], bias_recv.at[0], broadcast=True)
    m_steps(9, 11)
    arrived()
    for h in range(heads):
        bias_t[h] = rows_of(bias_recv.at[0], h).astype(F32).T * LOG2E
    attention(zbuf, tas_w, tas_out, start_ref, heads)
    local_bias(normed_tokens(), tae_b, bias_send.at[1])
    bias_arrived = exchange.start(bias_send.at[1], bias_recv.at[1], broadcast=True)
    z_send[0] = swap_blocks(zbuf)
    arrived = exchange.start(z_send.at[0], z_recv)
    m_steps(11, 13)
    bias_arrived()
    for h in range(heads):
        bias_t[h] = rows_of(bias_recv.at[1], h).astype(F32) * LOG2E
    arrived()
    for j in range(n_res):
        tbuf[j] = rows_of(z_recv, j)
    attention(tbuf, tae_w, tae_out, end_ref, heads)
    z_send[1] = swap_blocks(tbuf)
    arrived = exchange.start(z_send.at[1], zb_recv)
    m_steps(13, n_dev)
    arrived()
    for i in range(n_res):
        zbuf[i] = rows_of(zb_recv, i)
    x_norm = normed_tokens()
    hidden = jnp.maximum(jnp.dot(x_norm, ptr_in[...], preferred_element_type=F32), 0.0).astype(BF16)
    update = jnp.dot(hidden, ptr_out[...], preferred_element_type=F32)
    result = (zbuf[...].astype(F32) + update.reshape(n_res, length, dim)).astype(BF16)
    o_ref[...] = result
    if with_bias:
        zbuf[...] = result
        local_bias(normed_tokens(), next_b, nb_send)
        arrived = exchange.start(nb_send, nb_recv, broadcast=True)
        arrived()
        for h in range(bias_ref.shape[0]):
            bias_ref[h] = rows_of(nb_recv, h).astype(F32).T * LOG2E
    else:
        bias_ref[...] = jnp.zeros_like(bias_ref)
    own.wait()

    def m_wait(step, carry):
        other = lax.rem(me + step, n_dev)
        m_copy(other, other).wait_recv()
        m_copy(other, me).wait_send()
        return carry

    lax.fori_loop(1, n_dev, m_wait, 0)


def pair_stack(pair_loc, by_res, masks, pair_w, next_bias, collective_id):
    (tmo_proj, tmo_out, tmi_proj, tmi_out, tas_qkvg, tas_bias, tas_out,
     tae_qkvg, tae_bias, tae_out, ptr_in, ptr_out) = pair_w
    n_res, length, dim = pair_loc.shape
    n_dev = masks['n_dev']
    tri = tmo_out.shape[0]
    heads = tas_bias.shape[1]
    n_chan = tri // n_dev
    row_heads = (next_bias if next_bias is not None else masks['row_bias']).shape[1]
    padded = lambda w: jnp.pad(w.T, ((0, -w.shape[1] % 8), (0, 0)))
    weights = (tmo_proj[:, :4 * tri].T, tmo_proj[:, 4 * tri:], tmo_out, tmi_proj[:, :4 * tri].T, tmi_proj[:, 4 * tri:], tmi_out,
               tas_qkvg.T, padded(tas_bias), tas_out, tae_qkvg.T, padded(tae_bias), tae_out, ptr_in, ptr_out,
               padded(next_bias if next_bias is not None else masks['row_bias']))
    vmem = pl.BlockSpec(memory_space=pltpu.VMEM)
    any_space = pl.BlockSpec(memory_space=pl.ANY)
    n_phases = 9
    width = tas_out.shape[0]
    scratch = [
        pltpu.VMEM((n_res, length, dim), BF16), pltpu.VMEM((n_res, length, dim), BF16),
        pltpu.VMEM((n_dev * n_res * n_res, LANES), F32),
        pltpu.VMEM((2, n_dev, 2, n_chan, n_res, length), BF16), pltpu.VMEM((2, n_dev, 2, n_chan, n_res, length), BF16),
        pltpu.VMEM((2, n_dev, n_chan, n_res, length), F32), pltpu.VMEM((2, n_dev, n_chan, n_res, length), F32),
        pltpu.VMEM((n_res * (tri + 8), length), F32), pltpu.VMEM((n_res * length, dim), F32),
        pltpu.VMEM((n_res, 4 * width, length), BF16), pltpu.VMEM((n_res, width, length), BF16),
        pltpu.VMEM((heads, length, length), F32),
        pltpu.VMEM((2, heads, n_res, length), BF16), pltpu.VMEM((2, n_dev, heads, n_res, length), BF16),
        pltpu.VMEM((2, n_dev, n_res, n_res, dim), BF16), pltpu.VMEM((n_dev, n_res, n_res, dim), BF16), pltpu.VMEM((n_dev, n_res, n_res, dim), BF16),
        pltpu.VMEM((row_heads, n_res, length), BF16), pltpu.VMEM((n_dev, row_heads, n_res, length), BF16),
        pltpu.SemaphoreType.DMA((n_phases, n_dev)), pltpu.SemaphoreType.DMA((n_phases, n_dev)),
        pltpu.SemaphoreType.DMA((n_dev,)), pltpu.SemaphoreType.DMA((n_dev,)), pltpu.SemaphoreType.DMA,
    ]
    return pl.pallas_call(
        functools.partial(pair_kernel, n_dev, next_bias is not None),
        in_specs=[vmem] * 4 + [any_space] + [vmem] * len(weights),
        out_specs=[vmem, any_space, vmem],
        out_shape=[jax.ShapeDtypeStruct(pair_loc.shape, BF16), jax.ShapeDtypeStruct(by_res.shape, BF16), jax.ShapeDtypeStruct((row_heads, length, length), F32)],
        scratch_shapes=scratch,
        compiler_params=pltpu.CompilerParams(collective_id=collective_id, has_side_effects=True),
        cost_estimate=pl.CostEstimate(flops=4_000_000_000, bytes_accessed=16_000_000, transcendentals=4_000_000),
        name='pair_stack',
    )(pair_loc, masks['pair_rows'].reshape(1, n_res * length), masks['start'], masks['end'], by_res, *weights)


def head_bias(pair_norm, w_bias):
    return jnp.einsum('ijc,ch->hij', pair_norm, w_bias, preferred_element_type=F32).astype(BF16)


def gather_bias(pair_rows, w_bias):
    full = lax.all_gather(head_bias(layer_norm(pair_rows), w_bias), GROUP_AXIS, axis=1, tiled=True)
    return jnp.swapaxes(full, 1, 2).astype(F32) * LOG2E


def outer_update(ab, overlap, w_out):
    opm_dim = ab.shape[1] // 2
    left_act = ab[:, :opm_dim]
    right_full = lax.all_gather(ab[:, opm_dim:], GROUP_AXIS, axis=0, tiled=True)
    outer_prod = jnp.einsum('ics,jes->ijce', left_act, right_full, preferred_element_type=F32).astype(BF16)
    n_rows, n_cols = outer_prod.shape[:2]
    update = dense(outer_prod.reshape(n_rows, n_cols, opm_dim * opm_dim), w_out)
    return update / (1e-3 + overlap)[:, :, None]


def evoformer_block(value_a7, pair_loc, bias_t, masks, layer_w, next_bias, layer_idx):
    (row_qkvg, row_bias, row_out, col_qkvg, col_out, mtr_in, mtr_out, opm_proj, opm_out) = layer_w[:9]
    heads = row_bias.shape[1]
    n_dev = masks['n_dev']
    value_a7 = row_attention(value_a7, masks['seq'], bias_t, row_qkvg.T, row_out, heads, 16, 4, swap_in=layer_idx > 0, swap_out=True)
    length, n_seq, dim = value_a7.shape
    by_dev = value_a7.reshape(n_dev, length // n_dev, n_seq, dim)
    by_res = lax.all_to_all(by_dev, GROUP_AXIS, 0, 0, tiled=True)
    by_res, ab = column_stack(by_res, masks['res'], masks['res_row'], col_qkvg.T, col_out, mtr_in, mtr_out, opm_proj.T, heads)
    pair_loc = residual(pair_loc, outer_update(ab, masks['overlap'], opm_out))
    pair_loc, value_a7, bias_t = pair_stack(pair_loc, by_res, masks, layer_w[9:], next_bias, layer_idx)
    return value_a7.reshape(length, n_seq, dim), pair_loc, bias_t


def make_masks(msa_mask, pair_mask, n_dev):
    shard_idx = lax.axis_index(GROUP_AXIS)
    n_seq, length = msa_mask.shape
    n_res = pair_mask.shape[0]
    packed = jnp.concatenate([msa_mask, pair_mask], 0).astype(BF16)
    full = lax.all_gather(packed, GROUP_AXIS, axis=0, tiled=True).reshape(n_dev, n_seq + n_res, length).astype(F32)
    full_msa = full[:, :n_seq].reshape(n_dev * n_seq, length)
    full_pair = full[:, n_seq:].reshape(n_dev * n_res, length)
    res_mask = lax.dynamic_slice_in_dim(full_msa, shard_idx * n_res, n_res, 1).T
    end_mask = lax.dynamic_slice_in_dim(full_pair, shard_idx * n_res, n_res, 1).T
    lanes = lambda mask: jnp.broadcast_to(mask.astype(F32)[:, :, None], mask.shape + (length,))
    return {
        'n_dev': n_dev,
        'seq': lanes(msa_mask),
        'res': lanes(res_mask),
        'res_row': res_mask[:, None, :],
        'pair_rows': pair_mask.astype(F32),
        'start': lanes(pair_mask),
        'end': lanes(end_mask),
        'overlap': jnp.dot(res_mask, full_msa, precision=lax.Precision.DEFAULT, preferred_element_type=F32),
    }


def solution(mesh):
    row_spec = P((PARTS_AXIS, GROUP_AXIS))
    n_dev = mesh.shape[GROUP_AXIS]

    def local_body(value_a7, pair_loc, msa_mask, pair_mask, *weights):
        masks = make_masks(msa_mask, pair_mask, n_dev)
        masks['row_bias'] = weights[1][0]
        bias_t = gather_bias(pair_loc, weights[1][0])
        n_layers = weights[0].shape[0]
        for layer_idx in range(n_layers):
            layer_w = tuple(weight[layer_idx] for weight in weights)
            next_bias = weights[1][layer_idx + 1] if layer_idx + 1 < n_layers else None
            value_a7, pair_loc, bias_t = evoformer_block(value_a7, pair_loc, bias_t, masks, layer_w, next_bias, layer_idx)
        return jnp.swapaxes(value_a7, 0, 1), pair_loc

    def run_blocks(*arrays):
        n_weights = len(arrays) - 4
        return jax.shard_map(local_body, mesh=mesh, in_specs=(row_spec,) * 4 + (P(),) * n_weights, out_specs=(row_spec, row_spec), check_vma=False)(*arrays)

    return run_blocks
```

```python
import functools
import math

import jax
import jax.numpy as jnp
from jax import lax
from jax.experimental import pallas as pl
from jax.experimental.pallas import tpu as pltpu
from jax.sharding import PartitionSpec as P

GROUP_AXIS = 'dap'
PARTS_AXIS = 'req'
LOG2E = math.log2(math.e)
MASKED = -1e9 * LOG2E
LANES = 128
AHEAD = 4
F32 = jnp.float32
BF16 = jnp.bfloat16
NT = (((1,), (1,)), ((), ()))
TN = (((0,), (0,)), ((), ()))


def layer_norm_f32(values):
    centered = values - jnp.mean(values, axis=-1, keepdims=True)
    variance = jnp.mean(centered * centered, axis=-1, keepdims=True)
    return (centered * lax.rsqrt(variance + 1e-5)).astype(BF16)


def layer_norm(x):
    return layer_norm_f32(x.astype(F32))


def residual(x, update):
    return (x.astype(F32) + update).astype(BF16)


def dense(x, weight):
    return jnp.einsum('...c,cf->...f', x, weight, preferred_element_type=F32)


def softmax_keys_first(logits):
    top = jnp.max(logits, axis=0, keepdims=True)
    raised = jnp.exp2(logits - top)
    total = jnp.sum(raised, axis=0, keepdims=True)
    return (raised * (1.0 / total)).astype(BF16)


def pipelined_units(units, ahead, first_stage, second_stage):
    ready = {}
    for idx in range(min(ahead, len(units))):
        ready[idx] = first_stage(*units[idx])
    for idx in range(len(units)):
        if idx + ahead < len(units):
            ready[idx + ahead] = first_stage(*units[idx + ahead])
        second_stage(ready.pop(idx), *units[idx])


def attention_rows(proj, gated, base, rows, heads, width, load_row, w_t, w_out, mask_of, bias_of, store_row):
    head_dim = width // heads
    scale = head_dim ** -0.5 * LOG2E

    def head_rows(j, part, h):
        lo = part * width + h * head_dim
        return proj[j, lo:lo + head_dim, :]

    normed = [layer_norm_f32(load_row(base + j)) for j in range(rows)]
    for j in range(rows):
        proj[j] = lax.dot_general(w_t, normed[j], NT, preferred_element_type=F32).astype(BF16)

    def logits_of(j, h):
        return lax.dot_general(head_rows(j, 1, h), head_rows(j, 0, h), TN, preferred_element_type=F32)

    def finish(raw, j, h):
        logits = jnp.where(mask_of(base + j) > 0.0, raw * scale + bias_of(h), MASKED)
        out_t = jnp.dot(head_rows(j, 2, h), softmax_keys_first(logits), preferred_element_type=F32)
        gate = jax.nn.sigmoid(head_rows(j, 3, h).astype(F32))
        gated[j, h * head_dim:(h + 1) * head_dim, :] = (out_t * gate).astype(BF16)

    pipelined_units([(j, h) for j in range(rows) for h in range(heads)], AHEAD, logits_of, finish)
    for j in range(rows):
        store_row(base + j, load_row(base + j) + lax.dot_general(gated[j], w_out, TN, preferred_element_type=F32))


def column_residue(heads, x, proj, gated, mask_ref, mrow, w_ref, wo_ref, win_ref, wtr_ref, wopm_ref):
    width = wo_ref.shape[0]
    head_dim = width // heads
    scale = head_dim ** -0.5 * LOG2E
    length, lanes = mask_ref.shape
    proj[...] = lax.dot_general(w_ref[...], layer_norm_f32(x), NT, preferred_element_type=F32).astype(BF16)

    def head_rows(part, h, cols=slice(None)):
        lo = part * width + h * head_dim
        return proj[lo:lo + head_dim, cols]

    def columns(c):
        return slice(c * lanes, (c + 1) * lanes)

    def logits_of(h, c):
        return lax.dot_general(head_rows(1, h), head_rows(0, h, columns(c)), TN, preferred_element_type=F32)

    def finish(raw, h, c):
        logits = jnp.where(mask_ref[...] > 0.0, raw * scale, MASKED)
        out_t = jnp.dot(head_rows(2, h), softmax_keys_first(logits), preferred_element_type=F32)
        gate = jax.nn.sigmoid(head_rows(3, h, columns(c)).astype(F32))
        gated[h * head_dim:(h + 1) * head_dim, columns(c)] = (out_t * gate).astype(BF16)

    pipelined_units([(h, c) for h in range(heads) for c in range(length // lanes)], AHEAD, logits_of, finish)
    update = lax.dot_general(gated[...], wo_ref[...], TN, preferred_element_type=F32)
    x = (x + update).astype(BF16).astype(F32)
    hidden = jnp.maximum(jnp.dot(layer_norm_f32(x), win_ref[...], preferred_element_type=F32), 0.0).astype(BF16)
    x = (x + jnp.dot(hidden, wtr_ref[...], preferred_element_type=F32)).astype(BF16)
    ab_t = lax.dot_general(wopm_ref[...], layer_norm_f32(x.astype(F32)), NT, preferred_element_type=F32).astype(BF16)
    return x, (ab_t.astype(F32) * mrow).astype(BF16)


def peer_copy(source, target, send_sem, recv_sem, dst_dev):
    return pltpu.make_async_remote_copy(src_ref=source, dst_ref=target, send_sem=send_sem, recv_sem=recv_sem,
                                        device_id={GROUP_AXIS: dst_dev}, device_id_type=pl.DeviceIdType.MESH)


def for_peers(n_dev, me, body, lo=1, hi=None):
    def step(k, carry):
        body(lax.rem(me + k, n_dev))
        return carry
    lax.fori_loop(lo, n_dev if hi is None else hi, step, 0)


def rows_and_columns_kernel(heads, n_dev, first, group, *refs):
    n_m = 1 if first else 2
    m_refs, refs = refs[:n_m], refs[n_m:]
    (mask_ref, bias_ref, cmask_ref, mrow_ref, rw_ref, rwo_ref, cw_ref, cwo_ref, win_ref, wtr_ref, wopm_ref,
     o_ref, ab_ref, late_ref, proj, gated, cproj, cgated, stage_out, s_buf, r_buf, sends, recvs, own_sem) = refs[:24]
    n_seq, length = mask_ref.shape[:2]
    half = late_ref.shape[2]
    block = s_buf.shape[3]
    n_blocks = n_seq // block
    width = rwo_ref.shape[0]
    parts = stage_out.shape[0]
    me = lax.axis_index(GROUP_AXIS)
    entry_barrier(n_dev, me)
    if first:
        load_row = lambda s: m_refs[0][s].astype(F32)
    else:
        stage_in = refs[24]
        for part in range(parts):
            for d in range(n_dev):
                for k in range(2):
                    lo = (d * 2 + k) * half * n_seq
                    stage_in[part, lo:lo + half * n_seq, :] = m_refs[k][d, :, :, part * LANES:(part + 1) * LANES].astype(F32).reshape(half * n_seq, LANES)
        load_row = lambda s: jnp.concatenate([stage_in[part, pl.ds(s, length, stride=n_seq), :] for part in range(parts)], -1)

    def early(b, dst_dev, slot):
        return peer_copy(s_buf.at[b, dst_dev, pl.ds(0, half)], r_buf.at[slot, b], sends.at[0, b, dst_dev], recvs.at[0, b, slot], dst_dev)

    def late(b, dst_dev, slot):
        return peer_copy(s_buf.at[b, dst_dev, pl.ds(half, half)], late_ref.at[slot, b], sends.at[1, b, dst_dev], recvs.at[1, b, slot], dst_dev)

    def row_block(b, carry):
        def store_row(s, value):
            for part in range(parts):
                stage_out[part, pl.ds(s - b * block, length, stride=block), :] = value[:, part * LANES:(part + 1) * LANES]

        def some_rows(t, inner):
            attention_rows(proj, gated, b * block + t * group, group, heads, width, load_row, rw_ref[...], rwo_ref[...],
                           lambda s: mask_ref[s], lambda h: bias_ref[h], store_row)
            return inner

        lax.fori_loop(0, block // group, some_rows, 0)
        for part in range(parts):
            s_buf[b, :, :, :, part * LANES:(part + 1) * LANES] = stage_out[part].reshape(n_dev, 2 * half, block, LANES).astype(BF16)
        for_peers(n_dev, me, lambda d: early(b, d, me).start())
        r_buf[me, b] = s_buf[b, me, 0:half]
        return carry

    lax.fori_loop(0, n_blocks, row_block, 0)
    own = [pltpu.make_async_copy(s_buf.at[b, me, pl.ds(half, half)], late_ref.at[me, b], own_sem.at[b]) for b in range(n_blocks)]
    for b in range(n_blocks):
        for_peers(n_dev, me, lambda d: late(b, d, me).start())
        own[b].start()
    for b in range(n_blocks):
        for_peers(n_dev, me, lambda d: early(b, d, d).wait_recv())

    def residue(r, carry):
        x = r_buf[:, :, r].astype(F32).reshape(n_dev * n_seq, -1)
        x, ab = column_residue(heads, x, cproj, cgated, cmask_ref.at[r], mrow_ref[r], cw_ref, cwo_ref, win_ref, wtr_ref, wopm_ref)
        o_ref[:, r] = x.reshape(n_dev, n_seq, -1)
        ab_ref[r] = ab
        return carry

    lax.fori_loop(0, half, residue, 0)
    for b in range(n_blocks):
        own[b].wait()
        for_peers(n_dev, me, lambda d: late(b, d, d).wait_recv())
        for_peers(n_dev, me, lambda d: early(b, d, me).wait_send())
        for_peers(n_dev, me, lambda d: late(b, d, me).wait_send())


def layer_of(stacked, layer):
    return pl.BlockSpec((None,) + stacked.shape[1:], lambda step: (layer,) + (0,) * (stacked.ndim - 1))


VMEM_SPEC = pl.BlockSpec(memory_space=pltpu.VMEM)
ANY_SPEC = pl.BlockSpec(memory_space=pl.ANY)


def rows_and_columns(m_arrays, bias_t, masks, stacked, layer, heads, group=4, block=8):
    n_dev = masks['n_dev']
    n_seq, length = masks['seq'].shape[:2]
    first = len(m_arrays) == 1
    dim = m_arrays[0].shape[-1]
    half = length // n_dev // 2
    n_blocks = n_seq // block
    seq_all = n_dev * n_seq
    weights = [stacked[k] for k in ('row_qkvg', 'row_out', 'col_qkvg', 'col_out', 'mtr_in', 'mtr_out', 'opm_proj')]
    width = stacked['row_out'].shape[1]
    n_opm = stacked['opm_proj'].shape[1]
    scratch = [
        pltpu.VMEM((group, 4 * width, length), BF16), pltpu.VMEM((group, width, length), BF16),
        pltpu.VMEM((4 * width, seq_all), BF16), pltpu.VMEM((width, seq_all), BF16),
        pltpu.VMEM((dim // LANES, length * block, LANES), F32),
        pltpu.VMEM((n_blocks, n_dev, 2 * half, block, dim), BF16), pltpu.VMEM((n_dev, n_blocks, half, block, dim), BF16),
        pltpu.SemaphoreType.DMA((2, n_blocks, n_dev)), pltpu.SemaphoreType.DMA((2, n_blocks, n_dev)), pltpu.SemaphoreType.DMA((n_blocks,)),
    ]
    if not first:
        scratch.append(pltpu.VMEM((dim // LANES, length * n_seq, LANES), F32))
    n_data = len(m_arrays) + 4
    return pl.pallas_call(
        functools.partial(rows_and_columns_kernel, heads, n_dev, first, group),
        grid=(1,),
        in_specs=[VMEM_SPEC] * n_data + [layer_of(w, layer) for w in weights],
        out_specs=[VMEM_SPEC, VMEM_SPEC, ANY_SPEC],
        out_shape=[jax.ShapeDtypeStruct((n_dev, half, n_seq, dim), BF16), jax.ShapeDtypeStruct((half, n_opm, seq_all), BF16),
                   jax.ShapeDtypeStruct((n_dev, n_blocks, half, block, dim), BF16)],
        scratch_shapes=scratch,
        compiler_params=pltpu.CompilerParams(collective_id=3 * layer, has_side_effects=True),
        cost_estimate=pl.CostEstimate(flops=20_000_000_000, bytes_accessed=12_000_000, transcendentals=16_000_000),
        name='rows_and_columns',
    )(*m_arrays, masks['seq'], bias_t, masks['res'][:half], masks['res_row'][:half], *weights)


def late_columns_kernel(heads, n_dev, late_ref, cmask_ref, mrow_ref, m_ref, cw_ref, cwo_ref, win_ref, wtr_ref, wopm_ref,
                        o_ref, ab_ref, mback_ref, cproj, cgated, sends, recvs, own_sem):
    me = lax.axis_index(GROUP_AXIS)
    half = late_ref.shape[2]
    n_seq = late_ref.shape[1] * late_ref.shape[3]
    entry_barrier(n_dev, me)
    copy = lambda d, slot: peer_copy(m_ref.at[d], mback_ref.at[slot], sends.at[d], recvs.at[slot], d)
    own = pltpu.make_async_copy(m_ref.at[me], mback_ref.at[me], own_sem)
    own.start()
    for_peers(n_dev, me, lambda d: copy(d, me).start())

    def residue(r, carry):
        x = late_ref[:, :, r].astype(F32).reshape(n_dev * n_seq, -1)
        x, ab = column_residue(heads, x, cproj, cgated, cmask_ref.at[r], mrow_ref[r], cw_ref, cwo_ref, win_ref, wtr_ref, wopm_ref)
        o_ref[:, r] = x.reshape(n_dev, n_seq, -1)
        ab_ref[r] = ab
        return carry

    lax.fori_loop(0, half, residue, 0)
    own.wait()
    for_peers(n_dev, me, lambda d: copy(d, d).wait_recv())
    for_peers(n_dev, me, lambda d: copy(d, me).wait_send())


def late_columns(late, m_half, masks, stacked, layer, heads):
    n_dev, n_blocks, half, block, dim = late.shape
    seq_all = n_dev * n_blocks * block
    weights = [stacked[k] for k in ('col_qkvg', 'col_out', 'mtr_in', 'mtr_out', 'opm_proj')]
    width = stacked['row_out'].shape[1]
    n_opm = stacked['opm_proj'].shape[1]
    return pl.pallas_call(
        functools.partial(late_columns_kernel, heads, n_dev),
        grid=(1,),
        in_specs=[VMEM_SPEC] * 3 + [ANY_SPEC] + [layer_of(w, layer) for w in weights],
        out_specs=[VMEM_SPEC, VMEM_SPEC, ANY_SPEC],
        out_shape=[jax.ShapeDtypeStruct(m_half.shape, BF16), jax.ShapeDtypeStruct((half, n_opm, seq_all), BF16), jax.ShapeDtypeStruct(m_half.shape, BF16)],
        scratch_shapes=[pltpu.VMEM((4 * width, seq_all), BF16), pltpu.VMEM((width, seq_all), BF16),
                        pltpu.SemaphoreType.DMA((n_dev,)), pltpu.SemaphoreType.DMA((n_dev,)), pltpu.SemaphoreType.DMA],
        compiler_params=pltpu.CompilerParams(collective_id=3 * layer + 1, has_side_effects=True),
        cost_estimate=pl.CostEstimate(flops=20_000_000_000, bytes_accessed=12_000_000, transcendentals=8_000_000),
        name='late_columns',
    )(late, masks['res'][half:], masks['res_row'][half:], m_half, *weights)


class Exchange:
    def __init__(self, n_dev, me, sends, recvs):
        self.n_dev, self.me, self.sends, self.recvs, self.used = n_dev, me, sends, recvs, 0

    def start(self, source, target, broadcast=False):
        phase = self.used
        self.used += 1
        pick = (lambda d: source) if broadcast else (lambda d: source.at[d])

        def copy(dst_dev, slot):
            return pltpu.make_async_remote_copy(
                src_ref=pick(dst_dev), dst_ref=target.at[slot], send_sem=self.sends.at[phase, dst_dev], recv_sem=self.recvs.at[phase, slot],
                device_id={GROUP_AXIS: dst_dev}, device_id_type=pl.DeviceIdType.MESH)

        def send(step, carry):
            copy(lax.rem(self.me + step, self.n_dev), self.me).start()
            return carry

        lax.fori_loop(1, self.n_dev, send, 0)
        target[self.me] = source[...] if broadcast else source[self.me]

        def finish():
            def wait(step, carry):
                other = lax.rem(self.me + step, self.n_dev)
                copy(other, other).wait_recv()
                copy(other, self.me).wait_send()
                return carry

            lax.fori_loop(1, self.n_dev, wait, 0)

        return finish


def entry_barrier(n_dev, me):
    barrier = pltpu.get_barrier_semaphore()

    def signal(step, carry):
        pl.semaphore_signal(barrier, inc=1, device_id={GROUP_AXIS: lax.rem(me + step, n_dev)}, device_id_type=pl.DeviceIdType.MESH)
        return carry

    lax.fori_loop(1, n_dev, signal, 0)
    pl.semaphore_wait(barrier, n_dev - 1)


def pair_kernel(n_dev, with_bias, *refs):
    (z_ref, mrow_ref, start_ref, end_ref, m_ref,
     tmo_w, tmo_p, tmo_out, tmi_w, tmi_p, tmi_out, tas_w, tas_b, tas_out, tae_w, tae_b, tae_out, ptr_in, ptr_out, next_b,
     o_ref, mback_ref, bias_ref,
     zbuf, tbuf, stage, ab_send, ab_recv, x_send, x_recv, ln_stage, gate, proj, gated, bias_t, bias_send, bias_recv, z_send, z_recv, zb_recv, nb_send, nb_recv,
     sends, recvs, m_sends, m_recvs, m_own) = refs
    n_res, length, dim = z_ref.shape
    tri = tmo_out.shape[0]
    n_chan = tri // n_dev
    tokens = n_res * length
    me = lax.axis_index(GROUP_AXIS)
    entry_barrier(n_dev, me)
    exchange = Exchange(n_dev, me, sends, recvs)

    def m_copy(dst_dev, slot):
        return pltpu.make_async_remote_copy(
            src_ref=m_ref.at[dst_dev], dst_ref=mback_ref.at[slot], send_sem=m_sends.at[dst_dev], recv_sem=m_recvs.at[slot],
            device_id={GROUP_AXIS: dst_dev}, device_id_type=pl.DeviceIdType.MESH)

    own = pltpu.make_async_copy(m_ref.at[me], mback_ref.at[me], m_own)
    own.start()

    def m_steps(lo, hi):
        def send(step, carry):
            m_copy(lax.rem(me + step, n_dev), me).start()
            return carry
        lax.fori_loop(lo, hi, send, 0)

    def normed_tokens():
        return layer_norm_f32(zbuf[...].astype(F32).reshape(tokens, dim))

    def tri_mul(turn, w_ref, p_ref, out_ref, contract):
        x_norm = normed_tokens()
        for part in range(2):
            value = lax.dot_general(w_ref[part * tri:(part + 1) * tri, :], x_norm, NT, preferred_element_type=F32)
            opened = lax.dot_general(w_ref[(2 + part) * tri:(3 + part) * tri, :], x_norm, NT, preferred_element_type=F32)
            gated_t = mrow_ref[...] * jax.nn.sigmoid(opened) * value
            for d in range(n_dev):
                for i in range(n_res):
                    tile = gated_t[d * n_chan:(d + 1) * n_chan, i * length:(i + 1) * length]
                    stage[pl.ds(d * n_chan * n_res + i, n_chan, stride=n_res), :] = tile
            ab_send[turn, :, part] = stage[...].reshape(n_dev, n_chan, n_res, length).astype(BF16)
        arrived = exchange.start(ab_send.at[turn], ab_recv.at[turn])
        m_steps(1 + 4 * turn, 3 + 4 * turn)
        gate[...] = jax.nn.sigmoid(jnp.dot(x_norm, p_ref[:, 4 * tri:], preferred_element_type=F32))
        arrived()
        for c in range(n_chan):
            left = ab_recv[turn, :, 0, c].astype(F32).reshape(length, length).astype(BF16)
            right = ab_recv[turn, :, 1, c].astype(F32).reshape(length, length).astype(BF16)
            product = lax.dot_general(left, right, contract, preferred_element_type=F32)
            x_send[turn, :, c] = product.reshape(n_dev, n_res, length)
        arrived = exchange.start(x_send.at[turn], x_recv.at[turn])
        m_steps(3 + 4 * turn, 5 + 4 * turn)
        arrived()
        values = x_recv[turn].reshape(tri, n_res, length)
        centered = values - jnp.mean(values, axis=0, keepdims=True)
        inverse = lax.rsqrt(jnp.mean(centered * centered, axis=0, keepdims=True) + 1e-5)
        pitch = tri + 8
        for c in range(tri):
            ln_stage[pl.ds(c, n_res, stride=pitch), :] = centered[c] * inverse[0]
        for i in range(n_res):
            columns = ln_stage[i * pitch:i * pitch + tri, :].astype(BF16)
            update = gate[i * length:(i + 1) * length, :] * lax.dot_general(columns, out_ref[...], TN, preferred_element_type=F32)
            zbuf[i] = (zbuf[i].astype(F32) + update).astype(BF16)

    def local_bias(x_norm, b_ref, send_ref):
        heads_pad = b_ref.shape[0]
        rows = lax.dot_general(b_ref[...], x_norm, NT, preferred_element_type=F32)
        for i in range(n_res):
            stage[pl.ds(i, heads_pad, stride=n_res), :] = rows[:, i * length:(i + 1) * length]
        heads = send_ref.shape[0]
        send_ref[...] = stage[0:heads * n_res, :].reshape(heads, n_res, length).astype(BF16)

    def attention(source, w_ref, out_ref, mask_ref, heads):
        def store_row(j, value):
            source[j] = value.astype(BF16)

        attention_rows(proj, gated, 0, n_res, heads, out_ref.shape[0], lambda j: source[j].astype(F32), w_ref[...], out_ref[...],
                       lambda j: mask_ref[j], lambda h: bias_t[h], store_row)

    def swap_blocks(source):
        for i in range(n_res):
            row = source[i].astype(F32)
            for d in range(n_dev):
                stage[pl.ds(d * n_res * n_res + i, n_res, stride=n_res), :] = row[d * n_res:(d + 1) * n_res, :]
        return stage[...].reshape(n_dev, n_res, n_res, dim).astype(BF16)

    def rows_of(received, i):
        return received[:, i].astype(F32).reshape(length, dim).astype(BF16)

    heads = bias_send.shape[1]
    zbuf[...] = z_ref[...]
    tri_mul(0, tmo_w, tmo_p, tmo_out, NT)
    tri_mul(1, tmi_w, tmi_p, tmi_out, TN)
    local_bias(normed_tokens(), tas_b, bias_send.at[0])
    arrived = exchange.start(bias_send.at[0], bias_recv.at[0], broadcast=True)
    m_steps(9, 11)
    arrived()
    for h in range(heads):
        bias_t[h] = rows_of(bias_recv.at[0], h).astype(F32).T * LOG2E
    attention(zbuf, tas_w, tas_out, start_ref, heads)
    local_bias(normed_tokens(), tae_b, bias_send.at[1])
    bias_arrived = exchange.start(bias_send.at[1], bias_recv.at[1], broadcast=True)
    z_send[0] = swap_blocks(zbuf)
    arrived = exchange.start(z_send.at[0], z_recv)
    m_steps(11, 13)
    bias_arrived()
    for h in range(heads):
        bias_t[h] = rows_of(bias_recv.at[1], h).astype(F32) * LOG2E
    arrived()
    for j in range(n_res):
        tbuf[j] = rows_of(z_recv, j)
    attention(tbuf, tae_w, tae_out, end_ref, heads)
    z_send[1] = swap_blocks(tbuf)
    arrived = exchange.start(z_send.at[1], zb_recv)
    m_steps(13, n_dev)
    arrived()
    for i in range(n_res):
        zbuf[i] = rows_of(zb_recv, i)
    x_norm = normed_tokens()
    hidden = jnp.maximum(jnp.dot(x_norm, ptr_in[...], preferred_element_type=F32), 0.0).astype(BF16)
    update = jnp.dot(hidden, ptr_out[...], preferred_element_type=F32)
    result = (zbuf[...].astype(F32) + update.reshape(n_res, length, dim)).astype(BF16)
    o_ref[...] = result
    if with_bias:
        zbuf[...] = result
        local_bias(normed_tokens(), next_b, nb_send)
        arrived = exchange.start(nb_send, nb_recv, broadcast=True)
        arrived()
        for h in range(bias_ref.shape[0]):
            bias_ref[h] = rows_of(nb_recv, h).astype(F32).T * LOG2E
    else:
        bias_ref[...] = jnp.zeros_like(bias_ref)
    own.wait()

    def m_wait(step, carry):
        other = lax.rem(me + step, n_dev)
        m_copy(other, other).wait_recv()
        m_copy(other, me).wait_send()
        return carry

    lax.fori_loop(1, n_dev, m_wait, 0)


def pair_stack(pair_loc, m_half, masks, stacked, layer, with_bias):
    n_res, length, dim = pair_loc.shape
    n_dev = masks['n_dev']
    tri = stacked['tmo_out'].shape[1]
    heads = masks['pair_heads']
    row_heads = stacked['row_bias'].shape[1]
    n_chan = tri // n_dev
    next_layer = layer + 1 if with_bias else layer
    names = ('tmo_w', 'tmo_proj', 'tmo_out', 'tmi_w', 'tmi_proj', 'tmi_out', 'tas_qkvg', 'tas_bias', 'tas_out', 'tae_qkvg', 'tae_bias', 'tae_out', 'ptr_in', 'ptr_out')
    weights = [stacked[k] for k in names] + [stacked['row_bias']]
    specs = [layer_of(w, layer) for w in weights[:-1]] + [layer_of(weights[-1], next_layer)]
    width = stacked['tas_out'].shape[1]
    n_phases = 9
    scratch = [
        pltpu.VMEM((n_res, length, dim), BF16), pltpu.VMEM((n_res, length, dim), BF16),
        pltpu.VMEM((n_dev * n_res * n_res, LANES), F32),
        pltpu.VMEM((2, n_dev, 2, n_chan, n_res, length), BF16), pltpu.VMEM((2, n_dev, 2, n_chan, n_res, length), BF16),
        pltpu.VMEM((2, n_dev, n_chan, n_res, length), F32), pltpu.VMEM((2, n_dev, n_chan, n_res, length), F32),
        pltpu.VMEM((n_res * (tri + 8), length), F32), pltpu.VMEM((n_res * length, dim), F32),
        pltpu.VMEM((n_res, 4 * width, length), BF16), pltpu.VMEM((n_res, width, length), BF16),
        pltpu.VMEM((heads, length, length), F32),
        pltpu.VMEM((2, heads, n_res, length), BF16), pltpu.VMEM((2, n_dev, heads, n_res, length), BF16),
        pltpu.VMEM((2, n_dev, n_res, n_res, dim), BF16), pltpu.VMEM((n_dev, n_res, n_res, dim), BF16), pltpu.VMEM((n_dev, n_res, n_res, dim), BF16),
        pltpu.VMEM((row_heads, n_res, length), BF16), pltpu.VMEM((n_dev, row_heads, n_res, length), BF16),
        pltpu.SemaphoreType.DMA((n_phases, n_dev)), pltpu.SemaphoreType.DMA((n_phases, n_dev)),
        pltpu.SemaphoreType.DMA((n_dev,)), pltpu.SemaphoreType.DMA((n_dev,)), pltpu.SemaphoreType.DMA,
    ]
    return pl.pallas_call(
        functools.partial(pair_kernel, n_dev, with_bias),
        grid=(1,),
        in_specs=[VMEM_SPEC] * 4 + [ANY_SPEC] + specs,
        out_specs=[VMEM_SPEC, ANY_SPEC, VMEM_SPEC],
        out_shape=[jax.ShapeDtypeStruct(pair_loc.shape, BF16), jax.ShapeDtypeStruct(m_half.shape, BF16), jax.ShapeDtypeStruct((row_heads, length, length), F32)],
        scratch_shapes=scratch,
        compiler_params=pltpu.CompilerParams(collective_id=3 * layer + 2, has_side_effects=True),
        cost_estimate=pl.CostEstimate(flops=4_000_000_000, bytes_accessed=16_000_000, transcendentals=4_000_000),
        name='pair_stack',
    )(pair_loc, masks['pair_rows'].reshape(1, n_res * length), masks['start'], masks['end'], m_half, *weights)


def head_bias(pair_norm, w_bias):
    return jnp.einsum('ijc,ch->hij', pair_norm, w_bias, preferred_element_type=F32).astype(BF16)


def gather_bias(pair_rows, w_bias):
    full = lax.all_gather(head_bias(layer_norm(pair_rows), w_bias), GROUP_AXIS, axis=1, tiled=True)
    return jnp.swapaxes(full, 1, 2).astype(F32) * LOG2E


def outer_product(left_act, right_half, w_out):
    opm_dim = left_act.shape[1]
    right_full = lax.all_gather(right_half, GROUP_AXIS, axis=0, tiled=True)
    outer_prod = jnp.einsum('ics,jes->ijce', left_act, right_full, preferred_element_type=F32).astype(BF16)
    n_rows, n_cols = outer_prod.shape[:2]
    return dense(outer_prod.reshape(n_rows, n_cols, opm_dim * opm_dim), w_out)


def outer_update(ab_halves, overlap, w_out, n_dev):
    opm_dim = ab_halves[0].shape[1] // 2
    left_act = jnp.concatenate([ab[:, :opm_dim] for ab in ab_halves], 0)
    halves = [outer_product(left_act, ab[:, opm_dim:], w_out) for ab in ab_halves]
    n_rows, n_cols, dim = halves[0].shape
    update = jnp.stack([part.reshape(n_rows, n_dev, n_cols // n_dev, dim) for part in halves], 2).reshape(n_rows, 2 * n_cols, dim)
    return update / (1e-3 + overlap)[:, :, None]


def evoformer_block(m_arrays, pair_loc, bias_t, masks, stacked, layer, with_bias):
    heads = masks['msa_heads']
    early, ab_early, late = rows_and_columns(m_arrays, bias_t, masks, stacked, layer, heads)
    late, ab_late, m_early = late_columns(late, early, masks, stacked, layer, heads)
    pair_loc = residual(pair_loc, outer_update((ab_early, ab_late), masks['overlap'], stacked['opm_out'][layer], masks['n_dev']))
    pair_loc, m_late, bias_t = pair_stack(pair_loc, late, masks, stacked, layer, with_bias)
    return (m_early, m_late), pair_loc, bias_t


WEIGHT_NAMES = ('row_qkvg', 'row_bias', 'row_out', 'col_qkvg', 'col_out', 'mtr_in', 'mtr_out', 'opm_proj', 'opm_out', 'tmo_proj', 'tmo_out',
                'tmi_proj', 'tmi_out', 'tas_qkvg', 'tas_bias', 'tas_out', 'tae_qkvg', 'tae_bias', 'tae_out', 'ptr_in', 'ptr_out')


def prepare_weights(weights):
    stacked = dict(zip(WEIGHT_NAMES, weights))
    for kind in ('tmo', 'tmi'):
        tri = stacked[kind + '_out'].shape[1]
        stacked[kind + '_w'] = jnp.swapaxes(stacked[kind + '_proj'][:, :, :4 * tri], 1, 2)
    for name in ('row_qkvg', 'col_qkvg', 'opm_proj', 'tas_qkvg', 'tae_qkvg'):
        stacked[name] = jnp.swapaxes(stacked[name], 1, 2)
    for name in ('row_bias', 'tas_bias', 'tae_bias'):
        stacked[name] = jnp.pad(jnp.swapaxes(stacked[name], 1, 2), ((0, 0), (0, -stacked[name].shape[2] % 8), (0, 0)))
    return stacked


def make_masks(msa_mask, pair_mask, n_dev):
    shard_idx = lax.axis_index(GROUP_AXIS)
    n_seq, length = msa_mask.shape
    n_res = pair_mask.shape[0]
    packed = jnp.concatenate([msa_mask, pair_mask], 0).astype(BF16)
    full = lax.all_gather(packed, GROUP_AXIS, axis=0, tiled=True).reshape(n_dev, n_seq + n_res, length).astype(F32)
    full_msa = full[:, :n_seq].reshape(n_dev * n_seq, length)
    full_pair = full[:, n_seq:].reshape(n_dev * n_res, length)
    res_mask = lax.dynamic_slice_in_dim(full_msa, shard_idx * n_res, n_res, 1).T
    end_mask = lax.dynamic_slice_in_dim(full_pair, shard_idx * n_res, n_res, 1).T
    lanes = lambda mask: jnp.broadcast_to(mask.astype(F32)[:, :, None], mask.shape + (length,))
    return {
        'n_dev': n_dev,
        'seq': lanes(msa_mask),
        'res': lanes(res_mask),
        'res_row': res_mask[:, None, :],
        'pair_rows': pair_mask.astype(F32),
        'start': lanes(pair_mask),
        'end': lanes(end_mask),
        'overlap': jnp.dot(res_mask, full_msa, precision=lax.Precision.DEFAULT, preferred_element_type=F32),
    }


def solution(mesh):
    row_spec = P((PARTS_AXIS, GROUP_AXIS))
    n_dev = mesh.shape[GROUP_AXIS]

    def local_body(value_a7, pair_loc, msa_mask, pair_mask, *weights):
        masks = make_masks(msa_mask, pair_mask, n_dev)
        stacked = prepare_weights(weights)
        masks['msa_heads'] = weights[1].shape[2]
        masks['pair_heads'] = weights[14].shape[2]
        bias_t = gather_bias(pair_loc, weights[1][0])
        n_layers = weights[0].shape[0]
        m_arrays = (value_a7,)
        for layer in range(n_layers):
            m_arrays, pair_loc, bias_t = evoformer_block(m_arrays, pair_loc, bias_t, masks, stacked, layer, layer + 1 < n_layers)
        n_seq, length, dim = value_a7.shape
        value_a7 = jnp.transpose(jnp.stack(m_arrays, 1), (3, 0, 1, 2, 4)).reshape(n_seq, length, dim)
        return value_a7, pair_loc

    def run_blocks(*arrays):
        n_weights = len(arrays) - 4
        return jax.shard_map(local_body, mesh=mesh, in_specs=(row_spec,) * 4 + (P(),) * n_weights, out_specs=(row_spec, row_spec), check_vma=False)(*arrays)

    return run_blocks
```

```python
import functools
import math

import jax
import jax.numpy as jnp
from jax import lax
from jax.experimental import pallas as pl
from jax.experimental.pallas import tpu as pltpu
from jax.sharding import PartitionSpec as P

GROUP_AXIS = 'dap'
PARTS_AXIS = 'req'
LOG2E = math.log2(math.e)
MASKED = -1e9 * LOG2E
LANES = 128
AHEAD = 4
F32 = jnp.float32
BF16 = jnp.bfloat16
NT = (((1,), (1,)), ((), ()))
TN = (((0,), (0,)), ((), ()))


def layer_norm_f32(values):
    centered = values - jnp.mean(values, axis=-1, keepdims=True)
    variance = jnp.mean(centered * centered, axis=-1, keepdims=True)
    return (centered * lax.rsqrt(variance + 1e-5)).astype(BF16)


def layer_norm(x):
    return layer_norm_f32(x.astype(F32))


def residual(x, update):
    return (x.astype(F32) + update).astype(BF16)


def dense(x, weight):
    return jnp.einsum('...c,cf->...f', x, weight, preferred_element_type=F32)


def softmax_keys_first(logits):
    top = jnp.max(logits, axis=0, keepdims=True)
    raised = jnp.exp2(logits - top)
    total = jnp.sum(raised, axis=0, keepdims=True)
    return (raised * (1.0 / total)).astype(BF16)


def pipelined_units(units, ahead, first_stage, second_stage):
    ready = {}
    for idx in range(min(ahead, len(units))):
        ready[idx] = first_stage(*units[idx])
    for idx in range(len(units)):
        if idx + ahead < len(units):
            ready[idx + ahead] = first_stage(*units[idx + ahead])
        second_stage(ready.pop(idx), *units[idx])


def attention_rows(proj, gated, base, rows, heads, width, load_row, w_t, w_out, mask_of, bias_of, store_row):
    head_dim = width // heads
    scale = head_dim ** -0.5 * LOG2E

    def head_rows(j, part, h):
        lo = part * width + h * head_dim
        return proj[j, lo:lo + head_dim, :]

    normed = [layer_norm_f32(load_row(base + j)) for j in range(rows)]
    for j in range(rows):
        proj[j] = lax.dot_general(w_t, normed[j], NT, preferred_element_type=F32).astype(BF16)

    def logits_of(j, h):
        return lax.dot_general(head_rows(j, 1, h), head_rows(j, 0, h), TN, preferred_element_type=F32)

    def finish(raw, j, h):
        logits = jnp.where(mask_of(base + j) > 0.0, raw * scale + bias_of(h), MASKED)
        out_t = jnp.dot(head_rows(j, 2, h), softmax_keys_first(logits), preferred_element_type=F32)
        gate = jax.nn.sigmoid(head_rows(j, 3, h).astype(F32))
        gated[j, h * head_dim:(h + 1) * head_dim, :] = (out_t * gate).astype(BF16)

    pipelined_units([(j, h) for j in range(rows) for h in range(heads)], AHEAD, logits_of, finish)
    for j in range(rows):
        store_row(base + j, load_row(base + j) + lax.dot_general(gated[j], w_out, TN, preferred_element_type=F32))


def column_residue(heads, x, proj, gated, mask_ref, mrow, w_ref, wo_ref, win_ref, wtr_ref, wopm_ref):
    width = wo_ref.shape[0]
    head_dim = width // heads
    scale = head_dim ** -0.5 * LOG2E
    length, lanes = mask_ref.shape
    proj[...] = lax.dot_general(w_ref[...], layer_norm_f32(x), NT, preferred_element_type=F32).astype(BF16)

    def head_rows(part, h, cols=slice(None)):
        lo = part * width + h * head_dim
        return proj[lo:lo + head_dim, cols]

    def columns(c):
        return slice(c * lanes, (c + 1) * lanes)

    def logits_of(h, c):
        return lax.dot_general(head_rows(1, h), head_rows(0, h, columns(c)), TN, preferred_element_type=F32)

    def finish(raw, h, c):
        logits = jnp.where(mask_ref[...] > 0.0, raw * scale, MASKED)
        out_t = jnp.dot(head_rows(2, h), softmax_keys_first(logits), preferred_element_type=F32)
        gate = jax.nn.sigmoid(head_rows(3, h, columns(c)).astype(F32))
        gated[h * head_dim:(h + 1) * head_dim, columns(c)] = (out_t * gate).astype(BF16)

    pipelined_units([(h, c) for h in range(heads) for c in range(length // lanes)], AHEAD, logits_of, finish)
    update = lax.dot_general(gated[...], wo_ref[...], TN, preferred_element_type=F32)
    x = (x + update).astype(BF16).astype(F32)
    hidden = jnp.maximum(jnp.dot(layer_norm_f32(x), win_ref[...], preferred_element_type=F32), 0.0).astype(BF16)
    x = (x + jnp.dot(hidden, wtr_ref[...], preferred_element_type=F32)).astype(BF16)
    ab_t = lax.dot_general(wopm_ref[...], layer_norm_f32(x.astype(F32)), NT, preferred_element_type=F32).astype(BF16)
    return x, (ab_t.astype(F32) * mrow).astype(BF16)


def peer_copy(source, target, send_sem, recv_sem, dst_dev):
    return pltpu.make_async_remote_copy(src_ref=source, dst_ref=target, send_sem=send_sem, recv_sem=recv_sem,
                                        device_id={GROUP_AXIS: dst_dev}, device_id_type=pl.DeviceIdType.MESH)


def for_peers(n_dev, me, body, lo=1, hi=None):
    def step(k, carry):
        body(lax.rem(me + k, n_dev))
        return carry
    lax.fori_loop(lo, n_dev if hi is None else hi, step, 0)


def rows_and_columns_kernel(heads, n_dev, first, group, *refs):
    n_m = 1 if first else 2
    m_refs, refs = refs[:n_m], refs[n_m:]
    (mask_ref, bias_ref, cmask_ref, mrow_ref, rw_ref, rwo_ref, cw_ref, cwo_ref, win_ref, wtr_ref, wopm_ref,
     o_ref, ab_ref, late_ref, proj, gated, cproj, cgated, stage_out, s_buf, r_buf, sends, recvs, own_sem) = refs[:24]
    n_seq, length = mask_ref.shape[:2]
    half = late_ref.shape[2]
    block = s_buf.shape[3]
    n_blocks = n_seq // block
    width = rwo_ref.shape[0]
    parts = stage_out.shape[0]
    me = lax.axis_index(GROUP_AXIS)
    entry_barrier(n_dev, me)
    if first:
        load_row = lambda s: m_refs[0][s].astype(F32)
    else:
        stage_in = refs[24]
        for part in range(parts):
            for d in range(n_dev):
                for k in range(2):
                    lo = (d * 2 + k) * half * n_seq
                    stage_in[part, lo:lo + half * n_seq, :] = m_refs[k][d, :, :, part * LANES:(part + 1) * LANES].astype(F32).reshape(half * n_seq, LANES)
        load_row = lambda s: jnp.concatenate([stage_in[part, pl.ds(s, length, stride=n_seq), :] for part in range(parts)], -1)

    def early(b, dst_dev, slot):
        return peer_copy(s_buf.at[b, dst_dev, pl.ds(0, half)], r_buf.at[slot, b], sends.at[0, b, dst_dev], recvs.at[0, b, slot], dst_dev)

    def late(b, dst_dev, slot):
        return peer_copy(s_buf.at[b, dst_dev, pl.ds(half, half)], late_ref.at[slot, b], sends.at[1, b, dst_dev], recvs.at[1, b, slot], dst_dev)

    def row_block(b, carry):
        def store_row(s, value):
            for part in range(parts):
                stage_out[part, pl.ds(s - b * block, length, stride=block), :] = value[:, part * LANES:(part + 1) * LANES]

        def some_rows(t, inner):
            attention_rows(proj, gated, b * block + t * group, group, heads, width, load_row, rw_ref[...], rwo_ref[...],
                           lambda s: mask_ref[s], lambda h: bias_ref[h], store_row)
            return inner

        lax.fori_loop(0, block // group, some_rows, 0)
        for part in range(parts):
            s_buf[b, :, :, :, part * LANES:(part + 1) * LANES] = stage_out[part].reshape(n_dev, 2 * half, block, LANES).astype(BF16)
        for_peers(n_dev, me, lambda d: early(b, d, me).start())
        r_buf[me, b] = s_buf[b, me, 0:half]
        return carry

    lax.fori_loop(0, n_blocks, row_block, 0)
    own = [pltpu.make_async_copy(s_buf.at[b, me, pl.ds(half, half)], late_ref.at[me, b], own_sem.at[b]) for b in range(n_blocks)]
    for b in range(n_blocks):
        for_peers(n_dev, me, lambda d: late(b, d, me).start())
        own[b].start()
    for b in range(n_blocks):
        for_peers(n_dev, me, lambda d: early(b, d, d).wait_recv())

    def residue(r, carry):
        x = r_buf[:, :, r].astype(F32).reshape(n_dev * n_seq, -1)
        x, ab = column_residue(heads, x, cproj, cgated, cmask_ref.at[r], mrow_ref[r], cw_ref, cwo_ref, win_ref, wtr_ref, wopm_ref)
        o_ref[:, r] = x.reshape(n_dev, n_seq, -1)
        ab_ref[r] = ab
        return carry

    lax.fori_loop(0, half, residue, 0)
    for b in range(n_blocks):
        own[b].wait()
        for_peers(n_dev, me, lambda d: late(b, d, d).wait_recv())
        for_peers(n_dev, me, lambda d: early(b, d, me).wait_send())
        for_peers(n_dev, me, lambda d: late(b, d, me).wait_send())


def layer_of(stacked, layer):
    return pl.BlockSpec((None,) + stacked.shape[1:], lambda step: (layer,) + (0,) * (stacked.ndim - 1))


VMEM_SPEC = pl.BlockSpec(memory_space=pltpu.VMEM)
ANY_SPEC = pl.BlockSpec(memory_space=pl.ANY)


def rows_and_columns(m_arrays, bias_t, masks, stacked, layer, heads, group=4, block=8):
    n_dev = masks['n_dev']
    n_seq, length = masks['seq'].shape[:2]
    first = len(m_arrays) == 1
    dim = m_arrays[0].shape[-1]
    half = length // n_dev // 2
    n_blocks = n_seq // block
    seq_all = n_dev * n_seq
    weights = [stacked[k] for k in ('row_qkvg', 'row_out', 'col_qkvg', 'col_out', 'mtr_in', 'mtr_out', 'opm_proj')]
    width = stacked['row_out'].shape[1]
    n_opm = stacked['opm_proj'].shape[1]
    scratch = [
        pltpu.VMEM((group, 4 * width, length), BF16), pltpu.VMEM((group, width, length), BF16),
        pltpu.VMEM((4 * width, seq_all), BF16), pltpu.VMEM((width, seq_all), BF16),
        pltpu.VMEM((dim // LANES, length * block, LANES), F32),
        pltpu.VMEM((n_blocks, n_dev, 2 * half, block, dim), BF16), pltpu.VMEM((n_dev, n_blocks, half, block, dim), BF16),
        pltpu.SemaphoreType.DMA((2, n_blocks, n_dev)), pltpu.SemaphoreType.DMA((2, n_blocks, n_dev)), pltpu.SemaphoreType.DMA((n_blocks,)),
    ]
    if not first:
        scratch.append(pltpu.VMEM((dim // LANES, length * n_seq, LANES), F32))
    n_data = len(m_arrays) + 4
    return pl.pallas_call(
        functools.partial(rows_and_columns_kernel, heads, n_dev, first, group),
        grid=(1,),
        in_specs=[VMEM_SPEC] * n_data + [layer_of(w, layer) for w in weights],
        out_specs=[VMEM_SPEC, VMEM_SPEC, ANY_SPEC],
        out_shape=[jax.ShapeDtypeStruct((n_dev, half, n_seq, dim), BF16), jax.ShapeDtypeStruct((half, n_opm, seq_all), BF16),
                   jax.ShapeDtypeStruct((n_dev, n_blocks, half, block, dim), BF16)],
        scratch_shapes=scratch,
        compiler_params=pltpu.CompilerParams(collective_id=3 * layer, has_side_effects=True),
        cost_estimate=pl.CostEstimate(flops=20_000_000_000, bytes_accessed=12_000_000, transcendentals=16_000_000),
        name='rows_and_columns',
    )(*m_arrays, masks['seq'], bias_t, masks['res'][:half], masks['res_row'][:half], *weights)


def late_columns_kernel(heads, n_dev, late_ref, cmask_ref, mrow_ref, m_ref, cw_ref, cwo_ref, win_ref, wtr_ref, wopm_ref,
                        o_ref, ab_ref, mback_ref, cproj, cgated, sends, recvs, own_sem):
    me = lax.axis_index(GROUP_AXIS)
    half = late_ref.shape[2]
    n_seq = late_ref.shape[1] * late_ref.shape[3]
    entry_barrier(n_dev, me)
    copy = lambda d, slot: peer_copy(m_ref.at[d], mback_ref.at[slot], sends.at[d], recvs.at[slot], d)
    own = pltpu.make_async_copy(m_ref.at[me], mback_ref.at[me], own_sem)
    own.start()
    for_peers(n_dev, me, lambda d: copy(d, me).start())

    def residue(r, carry):
        x = late_ref[:, :, r].astype(F32).reshape(n_dev * n_seq, -1)
        x, ab = column_residue(heads, x, cproj, cgated, cmask_ref.at[r], mrow_ref[r], cw_ref, cwo_ref, win_ref, wtr_ref, wopm_ref)
        o_ref[:, r] = x.reshape(n_dev, n_seq, -1)
        ab_ref[r] = ab
        return carry

    lax.fori_loop(0, half, residue, 0)
    own.wait()
    for_peers(n_dev, me, lambda d: copy(d, d).wait_recv())
    for_peers(n_dev, me, lambda d: copy(d, me).wait_send())


def late_columns(late, m_half, masks, stacked, layer, heads):
    n_dev, n_blocks, half, block, dim = late.shape
    seq_all = n_dev * n_blocks * block
    weights = [stacked[k] for k in ('col_qkvg', 'col_out', 'mtr_in', 'mtr_out', 'opm_proj')]
    width = stacked['row_out'].shape[1]
    n_opm = stacked['opm_proj'].shape[1]
    return pl.pallas_call(
        functools.partial(late_columns_kernel, heads, n_dev),
        grid=(1,),
        in_specs=[VMEM_SPEC] * 3 + [ANY_SPEC] + [layer_of(w, layer) for w in weights],
        out_specs=[VMEM_SPEC, VMEM_SPEC, ANY_SPEC],
        out_shape=[jax.ShapeDtypeStruct(m_half.shape, BF16), jax.ShapeDtypeStruct((half, n_opm, seq_all), BF16), jax.ShapeDtypeStruct(m_half.shape, BF16)],
        scratch_shapes=[pltpu.VMEM((4 * width, seq_all), BF16), pltpu.VMEM((width, seq_all), BF16),
                        pltpu.SemaphoreType.DMA((n_dev,)), pltpu.SemaphoreType.DMA((n_dev,)), pltpu.SemaphoreType.DMA],
        compiler_params=pltpu.CompilerParams(collective_id=3 * layer + 1, has_side_effects=True),
        cost_estimate=pl.CostEstimate(flops=20_000_000_000, bytes_accessed=12_000_000, transcendentals=8_000_000),
        name='late_columns',
    )(late, masks['res'][half:], masks['res_row'][half:], m_half, *weights)


class Exchange:
    def __init__(self, n_dev, me, sends, recvs):
        self.n_dev, self.me, self.sends, self.recvs, self.used = n_dev, me, sends, recvs, 0

    def start(self, source, target, broadcast=False):
        phase = self.used
        self.used += 1
        pick = (lambda d: source) if broadcast else (lambda d: source.at[d])

        def copy(dst_dev, slot):
            return pltpu.make_async_remote_copy(
                src_ref=pick(dst_dev), dst_ref=target.at[slot], send_sem=self.sends.at[phase, dst_dev], recv_sem=self.recvs.at[phase, slot],
                device_id={GROUP_AXIS: dst_dev}, device_id_type=pl.DeviceIdType.MESH)

        def send(step, carry):
            copy(lax.rem(self.me + step, self.n_dev), self.me).start()
            return carry

        lax.fori_loop(1, self.n_dev, send, 0)
        target[self.me] = source[...] if broadcast else source[self.me]

        def finish():
            def wait(step, carry):
                other = lax.rem(self.me + step, self.n_dev)
                copy(other, other).wait_recv()
                copy(other, self.me).wait_send()
                return carry

            lax.fori_loop(1, self.n_dev, wait, 0)

        return finish


def entry_barrier(n_dev, me):
    barrier = pltpu.get_barrier_semaphore()

    def signal(step, carry):
        pl.semaphore_signal(barrier, inc=1, device_id={GROUP_AXIS: lax.rem(me + step, n_dev)}, device_id_type=pl.DeviceIdType.MESH)
        return carry

    lax.fori_loop(1, n_dev, signal, 0)
    pl.semaphore_wait(barrier, n_dev - 1)


def pair_kernel(n_dev, with_bias, *refs):
    (z_ref, mrow_ref, start_ref, end_ref, m_ref,
     tmo_w, tmo_p, tmo_out, tmi_w, tmi_p, tmi_out, tas_w, tas_b, tas_out, tae_w, tae_b, tae_out, ptr_in, ptr_out, next_b,
     o_ref, mback_ref, bias_ref,
     zbuf, tbuf, stage, ab_send, ab_recv, x_send, x_recv, ln_stage, gate, proj, gated, bias_t, bias_send, bias_recv, z_send, z_recv, zb_recv, nb_send, nb_recv,
     sends, recvs, m_sends, m_recvs, m_own) = refs
    n_res, length, dim = z_ref.shape
    tri = tmo_out.shape[0]
    n_chan = tri // n_dev
    tokens = n_res * length
    me = lax.axis_index(GROUP_AXIS)
    entry_barrier(n_dev, me)
    exchange = Exchange(n_dev, me, sends, recvs)

    def m_copy(dst_dev, slot):
        return pltpu.make_async_remote_copy(
            src_ref=m_ref.at[dst_dev], dst_ref=mback_ref.at[slot], send_sem=m_sends.at[dst_dev], recv_sem=m_recvs.at[slot],
            device_id={GROUP_AXIS: dst_dev}, device_id_type=pl.DeviceIdType.MESH)

    own = pltpu.make_async_copy(m_ref.at[me], mback_ref.at[me], m_own)
    own.start()

    def m_steps(lo, hi):
        def send(step, carry):
            m_copy(lax.rem(me + step, n_dev), me).start()
            return carry
        lax.fori_loop(lo, hi, send, 0)

    def normed_tokens():
        return layer_norm_f32(zbuf[...].astype(F32).reshape(tokens, dim))

    def tri_mul(turn, w_ref, p_ref, out_ref, contract):
        x_norm = normed_tokens()
        for part in range(2):
            value = lax.dot_general(w_ref[part * tri:(part + 1) * tri, :], x_norm, NT, preferred_element_type=F32)
            opened = lax.dot_general(w_ref[(2 + part) * tri:(3 + part) * tri, :], x_norm, NT, preferred_element_type=F32)
            gated_t = mrow_ref[...] * jax.nn.sigmoid(opened) * value
            for d in range(n_dev):
                for i in range(n_res):
                    tile = gated_t[d * n_chan:(d + 1) * n_chan, i * length:(i + 1) * length]
                    stage[pl.ds(d * n_chan * n_res + i, n_chan, stride=n_res), :] = tile
            ab_send[turn, :, part] = stage[...].reshape(n_dev, n_chan, n_res, length).astype(BF16)
        arrived = exchange.start(ab_send.at[turn], ab_recv.at[turn])
        m_steps(3 + 2 * turn, 4 + 2 * turn)
        gate[...] = jax.nn.sigmoid(jnp.dot(x_norm, p_ref[:, 4 * tri:], preferred_element_type=F32))
        arrived()
        for c in range(n_chan):
            left = ab_recv[turn, :, 0, c].astype(F32).reshape(length, length).astype(BF16)
            right = ab_recv[turn, :, 1, c].astype(F32).reshape(length, length).astype(BF16)
            product = lax.dot_general(left, right, contract, preferred_element_type=F32)
            x_send[turn, :, c] = product.reshape(n_dev, n_res, length)
        arrived = exchange.start(x_send.at[turn], x_recv.at[turn])
        m_steps(4 + 2 * turn, 5 + 2 * turn)
        arrived()
        values = x_recv[turn].reshape(tri, n_res, length)
        centered = values - jnp.mean(values, axis=0, keepdims=True)
        inverse = lax.rsqrt(jnp.mean(centered * centered, axis=0, keepdims=True) + 1e-5)
        pitch = tri + 8
        for c in range(tri):
            ln_stage[pl.ds(c, n_res, stride=pitch), :] = centered[c] * inverse[0]
        for i in range(n_res):
            columns = ln_stage[i * pitch:i * pitch + tri, :].astype(BF16)
            update = gate[i * length:(i + 1) * length, :] * lax.dot_general(columns, out_ref[...], TN, preferred_element_type=F32)
            zbuf[i] = (zbuf[i].astype(F32) + update).astype(BF16)

    def local_bias(x_norm, b_ref, send_ref):
        heads_pad = b_ref.shape[0]
        rows = lax.dot_general(b_ref[...], x_norm, NT, preferred_element_type=F32)
        for i in range(n_res):
            stage[pl.ds(i, heads_pad, stride=n_res), :] = rows[:, i * length:(i + 1) * length]
        heads = send_ref.shape[0]
        send_ref[...] = stage[0:heads * n_res, :].reshape(heads, n_res, length).astype(BF16)

    def attention(source, w_ref, out_ref, mask_ref, heads):
        def store_row(j, value):
            source[j] = value.astype(BF16)

        attention_rows(proj, gated, 0, n_res, heads, out_ref.shape[0], lambda j: source[j].astype(F32), w_ref[...], out_ref[...],
                       lambda j: mask_ref[j], lambda h: bias_t[h], store_row)

    def swap_blocks(source):
        for i in range(n_res):
            row = source[i].astype(F32)
            for d in range(n_dev):
                stage[pl.ds(d * n_res * n_res + i, n_res, stride=n_res), :] = row[d * n_res:(d + 1) * n_res, :]
        return stage[...].reshape(n_dev, n_res, n_res, dim).astype(BF16)

    def rows_of(received, i):
        return received[:, i].astype(F32).reshape(length, dim).astype(BF16)

    heads = bias_send.shape[1]
    m_steps(1, 3)
    zbuf[...] = z_ref[...]
    tri_mul(0, tmo_w, tmo_p, tmo_out, NT)
    tri_mul(1, tmi_w, tmi_p, tmi_out, TN)
    local_bias(normed_tokens(), tas_b, bias_send.at[0])
    arrived = exchange.start(bias_send.at[0], bias_recv.at[0], broadcast=True)
    arrived()
    m_steps(7, 10)
    for h in range(heads):
        bias_t[h] = rows_of(bias_recv.at[0], h).astype(F32).T * LOG2E
    attention(zbuf, tas_w, tas_out, start_ref, heads)
    local_bias(normed_tokens(), tae_b, bias_send.at[1])
    bias_arrived = exchange.start(bias_send.at[1], bias_recv.at[1], broadcast=True)
    z_send[0] = swap_blocks(zbuf)
    arrived = exchange.start(z_send.at[0], z_recv)
    bias_arrived()
    for h in range(heads):
        bias_t[h] = rows_of(bias_recv.at[1], h).astype(F32) * LOG2E
    arrived()
    m_steps(10, 13)
    for j in range(n_res):
        tbuf[j] = rows_of(z_recv, j)
    attention(tbuf, tae_w, tae_out, end_ref, heads)
    z_send[1] = swap_blocks(tbuf)
    arrived = exchange.start(z_send.at[1], zb_recv)
    m_steps(13, n_dev)
    arrived()
    for i in range(n_res):
        zbuf[i] = rows_of(zb_recv, i)
    x_norm = normed_tokens()
    hidden = jnp.maximum(jnp.dot(x_norm, ptr_in[...], preferred_element_type=F32), 0.0).astype(BF16)
    update = jnp.dot(hidden, ptr_out[...], preferred_element_type=F32)
    result = (zbuf[...].astype(F32) + update.reshape(n_res, length, dim)).astype(BF16)
    o_ref[...] = result
    if with_bias:
        zbuf[...] = result
        local_bias(normed_tokens(), next_b, nb_send)
        arrived = exchange.start(nb_send, nb_recv, broadcast=True)
        arrived()
        for h in range(bias_ref.shape[0]):
            bias_ref[h] = rows_of(nb_recv, h).astype(F32).T * LOG2E
    else:
        bias_ref[...] = jnp.zeros_like(bias_ref)
    own.wait()

    def m_wait(step, carry):
        other = lax.rem(me + step, n_dev)
        m_copy(other, other).wait_recv()
        m_copy(other, me).wait_send()
        return carry

    lax.fori_loop(1, n_dev, m_wait, 0)


def pair_stack(pair_loc, m_half, masks, stacked, layer, with_bias):
    n_res, length, dim = pair_loc.shape
    n_dev = masks['n_dev']
    tri = stacked['tmo_out'].shape[1]
    heads = masks['pair_heads']
    row_heads = stacked['row_bias'].shape[1]
    n_chan = tri // n_dev
    next_layer = layer + 1 if with_bias else layer
    names = ('tmo_w', 'tmo_proj', 'tmo_out', 'tmi_w', 'tmi_proj', 'tmi_out', 'tas_qkvg', 'tas_bias', 'tas_out', 'tae_qkvg', 'tae_bias', 'tae_out', 'ptr_in', 'ptr_out')
    weights = [stacked[k] for k in names] + [stacked['row_bias']]
    specs = [layer_of(w, layer) for w in weights[:-1]] + [layer_of(weights[-1], next_layer)]
    width = stacked['tas_out'].shape[1]
    n_phases = 9
    scratch = [
        pltpu.VMEM((n_res, length, dim), BF16), pltpu.VMEM((n_res, length, dim), BF16),
        pltpu.VMEM((n_dev * n_res * n_res, LANES), F32),
        pltpu.VMEM((2, n_dev, 2, n_chan, n_res, length), BF16), pltpu.VMEM((2, n_dev, 2, n_chan, n_res, length), BF16),
        pltpu.VMEM((2, n_dev, n_chan, n_res, length), F32), pltpu.VMEM((2, n_dev, n_chan, n_res, length), F32),
        pltpu.VMEM((n_res * (tri + 8), length), F32), pltpu.VMEM((n_res * length, dim), F32),
        pltpu.VMEM((n_res, 4 * width, length), BF16), pltpu.VMEM((n_res, width, length), BF16),
        pltpu.VMEM((heads, length, length), F32),
        pltpu.VMEM((2, heads, n_res, length), BF16), pltpu.VMEM((2, n_dev, heads, n_res, length), BF16),
        pltpu.VMEM((2, n_dev, n_res, n_res, dim), BF16), pltpu.VMEM((n_dev, n_res, n_res, dim), BF16), pltpu.VMEM((n_dev, n_res, n_res, dim), BF16),
        pltpu.VMEM((row_heads, n_res, length), BF16), pltpu.VMEM((n_dev, row_heads, n_res, length), BF16),
        pltpu.SemaphoreType.DMA((n_phases, n_dev)), pltpu.SemaphoreType.DMA((n_phases, n_dev)),
        pltpu.SemaphoreType.DMA((n_dev,)), pltpu.SemaphoreType.DMA((n_dev,)), pltpu.SemaphoreType.DMA,
    ]
    return pl.pallas_call(
        functools.partial(pair_kernel, n_dev, with_bias),
        grid=(1,),
        in_specs=[VMEM_SPEC] * 4 + [ANY_SPEC] + specs,
        out_specs=[VMEM_SPEC, ANY_SPEC, VMEM_SPEC],
        out_shape=[jax.ShapeDtypeStruct(pair_loc.shape, BF16), jax.ShapeDtypeStruct(m_half.shape, BF16), jax.ShapeDtypeStruct((row_heads, length, length), F32)],
        scratch_shapes=scratch,
        compiler_params=pltpu.CompilerParams(collective_id=3 * layer + 2, has_side_effects=True),
        cost_estimate=pl.CostEstimate(flops=4_000_000_000, bytes_accessed=16_000_000, transcendentals=4_000_000),
        name='pair_stack',
    )(pair_loc, masks['pair_rows'].reshape(1, n_res * length), masks['start'], masks['end'], m_half, *weights)


def pair_stack(pair_loc, m_half, masks, stacked, layer, with_bias):
    n_res, length, dim = pair_loc.shape
    n_dev = masks['n_dev']
    tri = stacked['tmo_out'].shape[1]
    heads = masks['pair_heads']
    row_heads = stacked['row_bias'].shape[1]
    n_chan = tri // n_dev
    next_layer = layer + 1 if with_bias else layer
    names = ('tmo_w', 'tmo_proj', 'tmo_out', 'tmi_w', 'tmi_proj', 'tmi_out', 'tas_qkvg', 'tas_bias', 'tas_out', 'tae_qkvg', 'tae_bias', 'tae_out', 'ptr_in', 'ptr_out')
    weights = [stacked[k] for k in names] + [stacked['row_bias']]
    specs = [layer_of(w, layer) for w in weights[:-1]] + [layer_of(weights[-1], next_layer)]
    width = stacked['tas_out'].shape[1]
    n_phases = 9
    scratch = [
        pltpu.VMEM((n_res, length, dim), BF16), pltpu.VMEM((n_res, length, dim), BF16),
        pltpu.VMEM((n_dev * n_res * n_res, LANES), F32),
        pltpu.VMEM((2, n_dev, 2, n_chan, n_res, length), BF16), pltpu.VMEM((2, n_dev, 2, n_chan, n_res, length), BF16),
        pltpu.VMEM((2, n_dev, n_chan, n_res, length), F32), pltpu.VMEM((2, n_dev, n_chan, n_res, length), F32),
        pltpu.VMEM((n_res * (tri + 8), length), F32), pltpu.VMEM((n_res * length, dim), F32),
        pltpu.VMEM((n_res, 4 * width, length), BF16), pltpu.VMEM((n_res, width, length), BF16),
        pltpu.VMEM((heads, length, length), F32),
        pltpu.VMEM((2, heads, n_res, length), BF16), pltpu.VMEM((2, n_dev, heads, n_res, length), BF16),
        pltpu.VMEM((2, n_dev, n_res, n_res, dim), BF16), pltpu.VMEM((n_dev, n_res, n_res, dim), BF16), pltpu.VMEM((n_dev, n_res, n_res, dim), BF16),
        pltpu.VMEM((row_heads, n_res, length), BF16), pltpu.VMEM((n_dev, row_heads, n_res, length), BF16),
        pltpu.SemaphoreType.DMA((n_phases, n_dev)), pltpu.SemaphoreType.DMA((n_phases, n_dev)),
        pltpu.SemaphoreType.DMA((n_dev,)), pltpu.SemaphoreType.DMA((n_dev,)), pltpu.SemaphoreType.DMA,
    ]
    return pl.pallas_call(
        functools.partial(pair_kernel, n_dev, with_bias),
        grid=(1,),
        in_specs=[VMEM_SPEC] * 4 + [ANY_SPEC] + specs,
        out_specs=[VMEM_SPEC, ANY_SPEC, VMEM_SPEC],
        out_shape=[jax.ShapeDtypeStruct(pair_loc.shape, BF16), jax.ShapeDtypeStruct(m_half.shape, BF16), jax.ShapeDtypeStruct((row_heads, length, length), F32)],
        scratch_shapes=scratch,
        compiler_params=pltpu.CompilerParams(collective_id=3 * layer + 2, has_side_effects=True),
        cost_estimate=pl.CostEstimate(flops=4_000_000_000, bytes_accessed=16_000_000, transcendentals=4_000_000),
        name='pair_stack',
    )(pair_loc, masks['pair_rows'].reshape(1, n_res * length), masks['start'], masks['end'], m_half, *weights)


def head_bias(pair_norm, w_bias):
    return jnp.einsum('ijc,ch->hij', pair_norm, w_bias, preferred_element_type=F32).astype(BF16)


def gather_bias(pair_rows, w_bias):
    full = lax.all_gather(head_bias(layer_norm(pair_rows), w_bias), GROUP_AXIS, axis=1, tiled=True)
    return jnp.swapaxes(full, 1, 2).astype(F32) * LOG2E


def residues_inside(right_ref, stage, store):
    n_rows, n_e, length = right_ref.shape
    pitch = stage.shape[1] // n_e

    def one(j, carry):
        tile = right_ref[j].astype(F32)
        for part in range(length // LANES):
            for lo in range(0, n_e, 8):
                stage[part, pl.ds(lo * pitch + j, 8, stride=pitch), :] = tile[lo:lo + 8, part * LANES:(part + 1) * LANES]
        return carry

    lax.fori_loop(0, n_rows, one, 0)
    for e in range(n_e):
        for part in range(length // LANES):
            store(e, part, stage[part, e * pitch:e * pitch + n_rows, :].astype(BF16))


def outer_layout_kernel(right_ref, o_ref, stage):
    def store(e, part, value):
        o_ref[e, :, part * LANES:(part + 1) * LANES] = value
    residues_inside(right_ref, stage, store)


def outer_product_kernel(early_ref, late_ref, right_ref, right_late_ref, w_ref, o_ref, stage, left, rows, flat):
    half = early_ref.shape[0]
    n_half = right_ref.shape[1]
    dim = early_ref.shape[1] // 2
    for k, ab_ref in enumerate((early_ref, late_ref)):
        for r in range(half):
            left[(k * half + r) * dim:(k * half + r + 1) * dim, :] = ab_ref[r, 0:dim, :]

    def store(e, part, value):
        rows[e, n_half:2 * n_half, part * LANES:(part + 1) * LANES] = value

    residues_inside(right_late_ref, stage, store)
    for e in range(dim):
        rows[e, 0:n_half, :] = right_ref[e]

    def one(step, carry):
        some = [step * 4 + k for k in range(4)]
        products = [lax.dot_general(left[...], rows[e], NT, preferred_element_type=F32).astype(BF16) for e in some]
        for e, product in zip(some, products):
            for i in range(2 * half):
                flat[i, pl.ds(pl.multiple_of(e * dim, dim), dim), :] = product[i * dim:(i + 1) * dim, :]
        return carry

    lax.fori_loop(0, dim // 4, one, 0)
    for i in range(2 * half):
        o_ref[i] = jnp.dot(w_ref[...], flat[i], preferred_element_type=F32).T


def outer_update(ab_halves, overlap, stacked, layer, n_dev):
    half, n_ab, seq_all = ab_halves[0].shape
    opm_dim = n_ab // 2
    n_half = n_dev * half
    length = 2 * n_half
    dim = stacked['opm_w'].shape[1]
    gathered = [lax.all_gather(ab[:, opm_dim:], GROUP_AXIS, axis=0, tiled=True) for ab in ab_halves]
    stage = pltpu.VMEM((seq_all // LANES, opm_dim * (n_half + 8), LANES), F32)
    early_rows = pl.pallas_call(
        outer_layout_kernel,
        in_specs=[VMEM_SPEC], out_specs=VMEM_SPEC,
        out_shape=jax.ShapeDtypeStruct((opm_dim, n_half, seq_all), BF16),
        scratch_shapes=[stage],
        cost_estimate=pl.CostEstimate(flops=2_000_000_000, bytes_accessed=4_000_000, transcendentals=0),
        name='outer_layout',
    )(gathered[0])
    update = pl.pallas_call(
        outer_product_kernel,
        grid=(1,),
        in_specs=[VMEM_SPEC] * 4 + [layer_of(stacked['opm_w'], layer)], out_specs=VMEM_SPEC,
        out_shape=jax.ShapeDtypeStruct((2 * half, length, dim), F32),
        scratch_shapes=[stage, pltpu.VMEM((2 * half * opm_dim, seq_all), BF16), pltpu.VMEM((opm_dim, length, seq_all), BF16),
                        pltpu.VMEM((2 * half, opm_dim * opm_dim, length), BF16)],
        cost_estimate=pl.CostEstimate(flops=4_000_000_000, bytes_accessed=6_000_000, transcendentals=0),
        name='outer_product',
    )(ab_halves[0], ab_halves[1], early_rows, gathered[1], stacked['opm_w'])
    update = update.reshape(2 * half, 2, n_dev, half, dim)
    update = jnp.swapaxes(update, 1, 2).reshape(2 * half, length, dim)
    return update / (1e-3 + overlap)[:, :, None]


def first_gather_kernel(n_dev, z_ref, b_ref, masks_ref, bias_ref, full_ref, stage, bias_send, bias_recv, sends, recvs):
    n_res, length, dim = z_ref.shape
    me = lax.axis_index(GROUP_AXIS)
    entry_barrier(n_dev, me)
    exchange = Exchange(n_dev, me, sends, recvs)
    masks_arrived = exchange.start(masks_ref, full_ref, broadcast=True)
    rows = lax.dot_general(b_ref[...], layer_norm_f32(z_ref[...].astype(F32).reshape(n_res * length, dim)), NT, preferred_element_type=F32)
    heads = bias_send.shape[0]
    for i in range(n_res):
        stage[pl.ds(i, heads, stride=n_res), :] = rows[:, i * length:(i + 1) * length]
    bias_send[...] = stage[...].reshape(heads, n_res, length).astype(BF16)
    exchange.start(bias_send, bias_recv, broadcast=True)()
    for h in range(heads):
        bias_ref[h] = bias_recv[:, h].astype(F32).reshape(length, length).T * LOG2E
    masks_arrived()


def first_gather(pair_loc, packed_masks, stacked, n_dev):
    n_res, length, dim = pair_loc.shape
    heads = stacked['row_bias'].shape[1]
    return pl.pallas_call(
        functools.partial(first_gather_kernel, n_dev),
        grid=(1,),
        in_specs=[VMEM_SPEC, layer_of(stacked['row_bias'], 0), VMEM_SPEC], out_specs=[VMEM_SPEC, VMEM_SPEC],
        out_shape=[jax.ShapeDtypeStruct((heads, length, length), F32), jax.ShapeDtypeStruct((n_dev,) + packed_masks.shape, BF16)],
        scratch_shapes=[pltpu.VMEM((heads * n_res, length), F32), pltpu.VMEM((heads, n_res, length), BF16), pltpu.VMEM((n_dev, heads, n_res, length), BF16),
                        pltpu.SemaphoreType.DMA((2, n_dev)), pltpu.SemaphoreType.DMA((2, n_dev))],
        compiler_params=pltpu.CompilerParams(collective_id=3 * stacked['row_bias'].shape[0], has_side_effects=True),
        cost_estimate=pl.CostEstimate(flops=1_000_000_000, bytes_accessed=2_000_000, transcendentals=0),
        name='first_gather',
    )(pair_loc, stacked['row_bias'], packed_masks)


def evoformer_block(m_arrays, pair_loc, bias_t, masks, stacked, layer, with_bias):
    heads = masks['msa_heads']
    early, ab_early, late = rows_and_columns(m_arrays, bias_t, masks, stacked, layer, heads)
    late, ab_late, m_early = late_columns(late, early, masks, stacked, layer, heads)
    pair_loc = residual(pair_loc, outer_update((ab_early, ab_late), masks['overlap'], stacked, layer, masks['n_dev']))
    pair_loc, m_late, bias_t = pair_stack(pair_loc, late, masks, stacked, layer, with_bias)
    return (m_early, m_late), pair_loc, bias_t


WEIGHT_NAMES = ('row_qkvg', 'row_bias', 'row_out', 'col_qkvg', 'col_out', 'mtr_in', 'mtr_out', 'opm_proj', 'opm_out', 'tmo_proj', 'tmo_out',
                'tmi_proj', 'tmi_out', 'tas_qkvg', 'tas_bias', 'tas_out', 'tae_qkvg', 'tae_bias', 'tae_out', 'ptr_in', 'ptr_out')


def prepare_weights(weights):
    stacked = dict(zip(WEIGHT_NAMES, weights))
    for kind in ('tmo', 'tmi'):
        tri = stacked[kind + '_out'].shape[1]
        stacked[kind + '_w'] = jnp.swapaxes(stacked[kind + '_proj'][:, :, :4 * tri], 1, 2)
    for name in ('row_qkvg', 'col_qkvg', 'opm_proj', 'tas_qkvg', 'tae_qkvg'):
        stacked[name] = jnp.swapaxes(stacked[name], 1, 2)
    for name in ('row_bias', 'tas_bias', 'tae_bias'):
        stacked[name] = jnp.pad(jnp.swapaxes(stacked[name], 1, 2), ((0, 0), (0, -stacked[name].shape[2] % 8), (0, 0)))
    n_layers, flat, dim = stacked['opm_out'].shape
    opm_dim = stacked['opm_proj'].shape[1] // 2
    stacked['opm_w'] = jnp.transpose(stacked['opm_out'].reshape(n_layers, opm_dim, opm_dim, dim), (0, 3, 2, 1)).reshape(n_layers, dim, flat)
    return stacked


def pack_masks(msa_mask, pair_mask):
    return jnp.concatenate([msa_mask, pair_mask], 0).astype(BF16)


def make_masks(msa_mask, pair_mask, full, n_dev):
    shard_idx = lax.axis_index(GROUP_AXIS)
    n_seq, length = msa_mask.shape
    n_res = pair_mask.shape[0]
    full = full.astype(F32)
    full_msa = full[:, :n_seq].reshape(n_dev * n_seq, length)
    full_pair = full[:, n_seq:].reshape(n_dev * n_res, length)
    res_mask = lax.dynamic_slice_in_dim(full_msa, shard_idx * n_res, n_res, 1).T
    end_mask = lax.dynamic_slice_in_dim(full_pair, shard_idx * n_res, n_res, 1).T
    lanes = lambda mask: jnp.broadcast_to(mask.astype(F32)[:, :, None], mask.shape + (length,))
    return {
        'n_dev': n_dev,
        'seq': lanes(msa_mask),
        'res': lanes(res_mask),
        'res_row': res_mask[:, None, :],
        'pair_rows': pair_mask.astype(F32),
        'start': lanes(pair_mask),
        'end': lanes(end_mask),
        'overlap': jnp.dot(res_mask, full_msa, precision=lax.Precision.DEFAULT, preferred_element_type=F32),
    }


def solution(mesh):
    row_spec = P((PARTS_AXIS, GROUP_AXIS))
    n_dev = mesh.shape[GROUP_AXIS]

    def local_body(value_a7, pair_loc, msa_mask, pair_mask, *weights):
        stacked = prepare_weights(weights)
        bias_t, full = first_gather(pair_loc, pack_masks(msa_mask, pair_mask), stacked, n_dev)
        masks = make_masks(msa_mask, pair_mask, full, n_dev)
        masks['msa_heads'] = weights[1].shape[2]
        masks['pair_heads'] = weights[14].shape[2]
        n_layers = weights[0].shape[0]
        m_arrays = (value_a7,)
        for layer in range(n_layers):
            m_arrays, pair_loc, bias_t = evoformer_block(m_arrays, pair_loc, bias_t, masks, stacked, layer, layer + 1 < n_layers)
        n_seq, length, dim = value_a7.shape
        value_a7 = jnp.transpose(jnp.stack(m_arrays, 1), (3, 0, 1, 2, 4)).reshape(n_seq, length, dim)
        return value_a7, pair_loc

    def run_blocks(*arrays):
        n_weights = len(arrays) - 4
        return jax.shard_map(local_body, mesh=mesh, in_specs=(row_spec,) * 4 + (P(),) * n_weights, out_specs=(row_spec, row_spec), check_vma=False)(*arrays)

    return run_blocks
```

```python
import functools
import math

import jax
import jax.numpy as jnp
from jax import lax
from jax.experimental import pallas as pl
from jax.experimental.pallas import tpu as pltpu
from jax.sharding import PartitionSpec as P

GROUP_AXIS = 'dap'
PARTS_AXIS = 'req'
LOG2E = math.log2(math.e)
MASKED = -1e9 * LOG2E
LANES = 128
AHEAD = 4
F32 = jnp.float32
BF16 = jnp.bfloat16
NT = (((1,), (1,)), ((), ()))
TN = (((0,), (0,)), ((), ()))


def layer_norm_f32(values):
    centered = values - jnp.mean(values, axis=-1, keepdims=True)
    variance = jnp.mean(centered * centered, axis=-1, keepdims=True)
    return (centered * lax.rsqrt(variance + 1e-5)).astype(BF16)


def layer_norm(x):
    return layer_norm_f32(x.astype(F32))


def residual(x, update):
    return (x.astype(F32) + update).astype(BF16)


def dense(x, weight):
    return jnp.einsum('...c,cf->...f', x, weight, preferred_element_type=F32)


def softmax_keys_first(logits):
    top = jnp.max(logits, axis=0, keepdims=True)
    raised = jnp.exp2(logits - top)
    total = jnp.sum(raised, axis=0, keepdims=True)
    return (raised * (1.0 / total)).astype(BF16)


def pipelined_units(units, ahead, first_stage, second_stage):
    ready = {}
    for idx in range(min(ahead, len(units))):
        ready[idx] = first_stage(*units[idx])
    for idx in range(len(units)):
        if idx + ahead < len(units):
            ready[idx + ahead] = first_stage(*units[idx + ahead])
        second_stage(ready.pop(idx), *units[idx])


def attention_rows(proj, gated, base, rows, heads, width, load_row, w_t, w_out, mask_of, bias_of, store_row):
    head_dim = width // heads
    scale = head_dim ** -0.5 * LOG2E

    def head_rows(j, part, h):
        lo = part * width + h * head_dim
        return proj[j, lo:lo + head_dim, :]

    normed = [layer_norm_f32(load_row(base + j)) for j in range(rows)]
    for j in range(rows):
        proj[j] = lax.dot_general(w_t, normed[j], NT, preferred_element_type=F32).astype(BF16)

    def logits_of(j, h):
        return lax.dot_general(head_rows(j, 1, h), head_rows(j, 0, h), TN, preferred_element_type=F32)

    def finish(raw, j, h):
        logits = jnp.where(mask_of(base + j) > 0.0, raw * scale + bias_of(h), MASKED)
        out_t = jnp.dot(head_rows(j, 2, h), softmax_keys_first(logits), preferred_element_type=F32)
        gate = jax.nn.sigmoid(head_rows(j, 3, h).astype(F32))
        gated[j, h * head_dim:(h + 1) * head_dim, :] = (out_t * gate).astype(BF16)

    pipelined_units([(j, h) for j in range(rows) for h in range(heads)], AHEAD, logits_of, finish)
    for j in range(rows):
        store_row(base + j, load_row(base + j) + lax.dot_general(gated[j], w_out, TN, preferred_element_type=F32))


def column_residue(heads, x, proj, gated, mask_ref, mrow, w_ref, wo_ref, win_ref, wtr_ref, wopm_ref):
    width = wo_ref.shape[0]
    head_dim = width // heads
    scale = head_dim ** -0.5 * LOG2E
    length, lanes = mask_ref.shape
    proj[...] = lax.dot_general(w_ref[...], layer_norm_f32(x), NT, preferred_element_type=F32).astype(BF16)

    def head_rows(part, h, cols=slice(None)):
        lo = part * width + h * head_dim
        return proj[lo:lo + head_dim, cols]

    def columns(c):
        return slice(c * lanes, (c + 1) * lanes)

    def logits_of(h, c):
        return lax.dot_general(head_rows(1, h), head_rows(0, h, columns(c)), TN, preferred_element_type=F32)

    def finish(raw, h, c):
        logits = jnp.where(mask_ref[...] > 0.0, raw * scale, MASKED)
        out_t = jnp.dot(head_rows(2, h), softmax_keys_first(logits), preferred_element_type=F32)
        gate = jax.nn.sigmoid(head_rows(3, h, columns(c)).astype(F32))
        gated[h * head_dim:(h + 1) * head_dim, columns(c)] = (out_t * gate).astype(BF16)

    pipelined_units([(h, c) for h in range(heads) for c in range(length // lanes)], AHEAD, logits_of, finish)
    update = lax.dot_general(gated[...], wo_ref[...], TN, preferred_element_type=F32)
    x = (x + update).astype(BF16).astype(F32)
    hidden = jnp.maximum(jnp.dot(layer_norm_f32(x), win_ref[...], preferred_element_type=F32), 0.0).astype(BF16)
    x = (x + jnp.dot(hidden, wtr_ref[...], preferred_element_type=F32)).astype(BF16)
    ab_t = lax.dot_general(wopm_ref[...], layer_norm_f32(x.astype(F32)), NT, preferred_element_type=F32).astype(BF16)
    return x, (ab_t.astype(F32) * mrow).astype(BF16)


def peer_copy(source, target, send_sem, recv_sem, dst_dev):
    return pltpu.make_async_remote_copy(src_ref=source, dst_ref=target, send_sem=send_sem, recv_sem=recv_sem,
                                        device_id={GROUP_AXIS: dst_dev}, device_id_type=pl.DeviceIdType.MESH)


def for_peers(n_dev, me, body, lo=1, hi=None):
    def step(k, carry):
        body(lax.rem(me + k, n_dev))
        return carry
    lax.fori_loop(lo, n_dev if hi is None else hi, step, 0)


def rows_and_columns_kernel(heads, n_dev, first, group, *refs):
    n_m = 1 if first else 2
    m_refs, refs = refs[:n_m], refs[n_m:]
    (mask_ref, bias_ref, cmask_ref, mrow_ref, rw_ref, rwo_ref, cw_ref, cwo_ref, win_ref, wtr_ref, wopm_ref,
     o_ref, ab_ref, late_ref, proj, gated, cproj, cgated, stage_out, s_buf, r_buf, sends, recvs, own_sem) = refs[:24]
    n_seq, length = mask_ref.shape[:2]
    half = late_ref.shape[2]
    block = s_buf.shape[3]
    n_blocks = n_seq // block
    width = rwo_ref.shape[0]
    parts = stage_out.shape[0]
    me = lax.axis_index(GROUP_AXIS)
    entry_barrier(n_dev, me)
    if first:
        load_row = lambda s: m_refs[0][s].astype(F32)
    else:
        stage_in = refs[24]
        for part in range(parts):
            for d in range(n_dev):
                for k in range(2):
                    lo = (d * 2 + k) * half * n_seq
                    stage_in[part, lo:lo + half * n_seq, :] = m_refs[k][d, :, :, part * LANES:(part + 1) * LANES].astype(F32).reshape(half * n_seq, LANES)
        load_row = lambda s: jnp.concatenate([stage_in[part, pl.ds(s, length, stride=n_seq), :] for part in range(parts)], -1)

    def early(b, dst_dev, slot):
        return peer_copy(s_buf.at[b, dst_dev, pl.ds(0, half)], r_buf.at[slot, b], sends.at[0, b, dst_dev], recvs.at[0, b, slot], dst_dev)

    def late(b, dst_dev, slot):
        return peer_copy(s_buf.at[b, dst_dev, pl.ds(half, half)], late_ref.at[slot, b], sends.at[1, b, dst_dev], recvs.at[1, b, slot], dst_dev)

    def row_block(b, carry):
        def store_row(s, value):
            for part in range(parts):
                stage_out[part, pl.ds(s - b * block, length, stride=block), :] = value[:, part * LANES:(part + 1) * LANES]

        def some_rows(t, inner):
            attention_rows(proj, gated, b * block + t * group, group, heads, width, load_row, rw_ref[...], rwo_ref[...],
                           lambda s: mask_ref[s], lambda h: bias_ref[h], store_row)
            return inner

        lax.fori_loop(0, block // group, some_rows, 0)
        for part in range(parts):
            s_buf[b, :, :, :, part * LANES:(part + 1) * LANES] = stage_out[part].reshape(n_dev, 2 * half, block, LANES).astype(BF16)
        for_peers(n_dev, me, lambda d: early(b, d, me).start())
        r_buf[me, b] = s_buf[b, me, 0:half]
        return carry

    lax.fori_loop(0, n_blocks, row_block, 0)
    own = [pltpu.make_async_copy(s_buf.at[b, me, pl.ds(half, half)], late_ref.at[me, b], own_sem.at[b]) for b in range(n_blocks)]
    for b in range(n_blocks):
        for_peers(n_dev, me, lambda d: late(b, d, me).start())
        own[b].start()
    for b in range(n_blocks):
        for_peers(n_dev, me, lambda d: early(b, d, d).wait_recv())

    def residue(r, carry):
        x = r_buf[:, :, r].astype(F32).reshape(n_dev * n_seq, -1)
        x, ab = column_residue(heads, x, cproj, cgated, cmask_ref.at[r], mrow_ref[r], cw_ref, cwo_ref, win_ref, wtr_ref, wopm_ref)
        o_ref[:, r] = x.reshape(n_dev, n_seq, -1)
        ab_ref[r] = ab
        return carry

    lax.fori_loop(0, half, residue, 0)
    for b in range(n_blocks):
        own[b].wait()
        for_peers(n_dev, me, lambda d: late(b, d, d).wait_recv())
        for_peers(n_dev, me, lambda d: early(b, d, me).wait_send())
        for_peers(n_dev, me, lambda d: late(b, d, me).wait_send())


def layer_of(stacked, layer):
    return pl.BlockSpec((None,) + stacked.shape[1:], lambda step: (layer,) + (0,) * (stacked.ndim - 1))


VMEM_SPEC = pl.BlockSpec(memory_space=pltpu.VMEM)
ANY_SPEC = pl.BlockSpec(memory_space=pl.ANY)


def rows_and_columns(m_arrays, bias_t, masks, stacked, layer, heads, group=4, block=8):
    n_dev = masks['n_dev']
    n_seq, length = masks['seq'].shape[:2]
    first = len(m_arrays) == 1
    dim = m_arrays[0].shape[-1]
    half = length // n_dev // 2
    n_blocks = n_seq // block
    seq_all = n_dev * n_seq
    weights = [stacked[k] for k in ('row_qkvg', 'row_out', 'col_qkvg', 'col_out', 'mtr_in', 'mtr_out', 'opm_proj')]
    width = stacked['row_out'].shape[1]
    n_opm = stacked['opm_proj'].shape[1]
    scratch = [
        pltpu.VMEM((group, 4 * width, length), BF16), pltpu.VMEM((group, width, length), BF16),
        pltpu.VMEM((4 * width, seq_all), BF16), pltpu.VMEM((width, seq_all), BF16),
        pltpu.VMEM((dim // LANES, length * block, LANES), F32),
        pltpu.VMEM((n_blocks, n_dev, 2 * half, block, dim), BF16), pltpu.VMEM((n_dev, n_blocks, half, block, dim), BF16),
        pltpu.SemaphoreType.DMA((2, n_blocks, n_dev)), pltpu.SemaphoreType.DMA((2, n_blocks, n_dev)), pltpu.SemaphoreType.DMA((n_blocks,)),
    ]
    if not first:
        scratch.append(pltpu.VMEM((dim // LANES, length * n_seq, LANES), F32))
    n_data = len(m_arrays) + 4
    return pl.pallas_call(
        functools.partial(rows_and_columns_kernel, heads, n_dev, first, group),
        grid=(1,),
        in_specs=[VMEM_SPEC] * n_data + [layer_of(w, layer) for w in weights],
        out_specs=[VMEM_SPEC, VMEM_SPEC, ANY_SPEC],
        out_shape=[jax.ShapeDtypeStruct((n_dev, half, n_seq, dim), BF16), jax.ShapeDtypeStruct((half, n_opm, seq_all), BF16),
                   jax.ShapeDtypeStruct((n_dev, n_blocks, half, block, dim), BF16)],
        scratch_shapes=scratch,
        compiler_params=pltpu.CompilerParams(collective_id=3 * layer, has_side_effects=True),
        cost_estimate=pl.CostEstimate(flops=20_000_000_000, bytes_accessed=12_000_000, transcendentals=16_000_000),
        name='rows_and_columns',
    )(*m_arrays, masks['seq'], bias_t, masks['res'][:half], masks['res_row'][:half], *weights)


def late_columns_kernel(heads, n_dev, late_ref, cmask_ref, mrow_ref, m_ref, ab_early_ref, cw_ref, cwo_ref, win_ref, wtr_ref, wopm_ref,
                        o_ref, ab_ref, mback_ref, b_ref, cproj, cgated, sends, recvs, own_sem, b_sem, *ring_sems):
    me = lax.axis_index(GROUP_AXIS)
    half = late_ref.shape[2]
    n_seq = late_ref.shape[1] * late_ref.shape[3]
    entry_barrier(n_dev, me)
    n_opm = ab_early_ref.shape[1] // 2
    b_own = ab_early_ref.at[:, pl.ds(n_opm, n_opm)]
    ring = ChipRing(n_dev, me, b_own, b_ref, *ring_sems)
    b_local = pltpu.make_async_copy(b_own, b_ref.at[me], b_sem)
    ring.send(1)
    b_local.start()
    copy = lambda d, slot: peer_copy(m_ref.at[d], mback_ref.at[slot], sends.at[d], recvs.at[slot], d)
    own = pltpu.make_async_copy(m_ref.at[me], mback_ref.at[me], own_sem)
    own.start()

    def residue(r):
        x = late_ref[:, :, r].astype(F32).reshape(n_dev * n_seq, -1)
        x, ab = column_residue(heads, x, cproj, cgated, cmask_ref.at[r], mrow_ref[r], cw_ref, cwo_ref, win_ref, wtr_ref, wopm_ref)
        o_ref[:, r] = x.reshape(n_dev, n_seq, -1)
        ab_ref[r] = ab

    share = -(-(n_dev - 1) // half)

    def step(r, carry):
        hop = r + 1

        def send_m(k, inner):
            @pl.when(k < n_dev)
            def _():
                d = lax.rem(me + k, n_dev)
                copy(d, me).start()
            return inner

        lax.fori_loop(1 + r * share, 1 + (r + 1) * share, send_m, 0)
        residue(r)

        @pl.when(hop <= ring.right_hops)
        def _():
            ring.receive_from(-hop)

        @pl.when(hop <= ring.left_hops)
        def _():
            ring.receive_from(hop)

        @pl.when(hop + 1 <= ring.right_hops)
        def _():
            ring.right(hop + 1).start()

        @pl.when(hop + 1 <= ring.left_hops)
        def _():
            ring.left(hop + 1).start()

        return carry

    lax.fori_loop(0, half, step, 0)
    for hop in range(half + 1, ring.right_hops + 1):
        ring.receive(hop)
        ring.send(hop + 1)
    own.wait()
    b_local.wait()
    for_peers(n_dev, me, lambda d: copy(d, d).wait_recv())
    for_peers(n_dev, me, lambda d: copy(d, me).wait_send())
    ring.receive_mate(0)
    for k in range(1, ring.right_hops + 1):
        for away in ring.arrivals(k):
            ring.receive_mate(away)
    ring.drain()


def late_columns(late, m_half, ab_early, masks, stacked, layer, heads):
    n_dev, n_blocks, half, block, dim = late.shape
    seq_all = n_dev * n_blocks * block
    weights = [stacked[k] for k in ('col_qkvg', 'col_out', 'mtr_in', 'mtr_out', 'opm_proj')]
    width = stacked['row_out'].shape[1]
    n_opm = stacked['opm_proj'].shape[1]
    return pl.pallas_call(
        functools.partial(late_columns_kernel, heads, n_dev),
        grid=(1,),
        in_specs=[VMEM_SPEC] * 3 + [ANY_SPEC] * 2 + [layer_of(w, layer) for w in weights],
        out_specs=[VMEM_SPEC, VMEM_SPEC, ANY_SPEC, ANY_SPEC],
        out_shape=[jax.ShapeDtypeStruct(m_half.shape, BF16), jax.ShapeDtypeStruct((half, n_opm, seq_all), BF16), jax.ShapeDtypeStruct(m_half.shape, BF16),
                   jax.ShapeDtypeStruct((n_dev, half, n_opm // 2, seq_all), BF16)],
        scratch_shapes=[pltpu.VMEM((4 * width, seq_all), BF16), pltpu.VMEM((width, seq_all), BF16),
                        pltpu.SemaphoreType.DMA((n_dev,)), pltpu.SemaphoreType.DMA((n_dev,)), pltpu.SemaphoreType.DMA, pltpu.SemaphoreType.DMA] + ring_semaphores(n_dev),
        compiler_params=pltpu.CompilerParams(collective_id=3 * layer + 1, has_side_effects=True),
        cost_estimate=pl.CostEstimate(flops=20_000_000_000, bytes_accessed=12_000_000, transcendentals=8_000_000),
        name='late_columns',
    )(late, masks['res'][half:], masks['res_row'][half:], m_half, ab_early, *weights)


class Exchange:
    def __init__(self, n_dev, me, sends, recvs):
        self.n_dev, self.me, self.sends, self.recvs, self.used = n_dev, me, sends, recvs, 0

    def start(self, source, target, broadcast=False):
        phase = self.used
        self.used += 1
        pick = (lambda d: source) if broadcast else (lambda d: source.at[d])

        def copy(dst_dev, slot):
            return pltpu.make_async_remote_copy(
                src_ref=pick(dst_dev), dst_ref=target.at[slot], send_sem=self.sends.at[phase, dst_dev], recv_sem=self.recvs.at[phase, slot],
                device_id={GROUP_AXIS: dst_dev}, device_id_type=pl.DeviceIdType.MESH)

        def send(step, carry):
            copy(lax.rem(self.me + step, self.n_dev), self.me).start()
            return carry

        lax.fori_loop(1, self.n_dev, send, 0)
        target[self.me] = source[...] if broadcast else source[self.me]

        def finish():
            def wait(step, carry):
                other = lax.rem(self.me + step, self.n_dev)
                copy(other, other).wait_recv()
                copy(other, self.me).wait_send()
                return carry

            lax.fori_loop(1, self.n_dev, wait, 0)

        return finish


class ChipRing:
    def __init__(self, n_dev, me, own, slots, recvs, rights, lefts, partners):
        self.n_dev, self.me, self.own, self.slots = n_dev, me, own, slots
        self.recvs, self.rights, self.lefts, self.partners = recvs, rights, lefts, partners
        chips = n_dev // 2
        self.right_hops, self.left_hops = chips // 2, (chips - 1) // 2
        self.partner = me + 1 - 2 * lax.rem(me, 2)

    def device(self, chips_away):
        return lax.rem(self.me + 2 * chips_away + self.n_dev, self.n_dev)

    def mate(self, src):
        return src + 1 - 2 * lax.rem(src, 2)

    def copy(self, src, first, send_sem, to):
        return peer_copy(self.own if first else self.slots.at[src], self.slots.at[src], send_sem, self.recvs.at[src], to)

    def right(self, hop):
        return self.copy(self.device(1 - hop), isinstance(hop, int) and hop == 1, self.rights.at[hop], self.device(1))

    def left(self, hop):
        return self.copy(self.device(hop - 1), isinstance(hop, int) and hop == 1, self.lefts.at[hop], self.device(-1))

    def hand(self, src, first=False):
        return self.copy(src, first, self.partners.at[src], self.partner)

    def send(self, hop):
        if hop == 1:
            self.hand(self.me, True).start()
        if hop <= self.right_hops:
            self.right(hop).start()
        if hop <= self.left_hops:
            self.left(hop).start()

    def arrivals(self, hop):
        return ([-hop] if hop <= self.right_hops else []) + ([hop] if hop <= self.left_hops else [])

    def receive(self, hop):
        for away in self.arrivals(hop):
            self.receive_from(away)

    def receive_from(self, away):
        src = self.device(away)
        self.copy(src, False, self.rights.at[0], self.partner).wait_recv()
        self.hand(src).start()

    def receive_mate(self, away):
        src = self.mate(self.device(away))
        self.copy(src, False, self.rights.at[0], self.partner).wait_recv()
        return src

    def drain(self):
        self.hand(self.me, True).wait_send()
        for hop in range(1, self.right_hops + 1):
            self.right(hop).wait_send()
            if hop <= self.left_hops:
                self.left(hop).wait_send()
            for away in self.arrivals(hop):
                self.hand(self.device(away)).wait_send()


def ring_semaphores(n_dev):
    return [pltpu.SemaphoreType.DMA((n_dev,)) for k in range(4)]


def entry_barrier(n_dev, me):
    barrier = pltpu.get_barrier_semaphore()

    def signal(step, carry):
        pl.semaphore_signal(barrier, inc=1, device_id={GROUP_AXIS: lax.rem(me + step, n_dev)}, device_id_type=pl.DeviceIdType.MESH)
        return carry

    lax.fori_loop(1, n_dev, signal, 0)
    pl.semaphore_wait(barrier, n_dev - 1)


def pair_kernel(n_dev, with_bias, *refs):
    (z_ref, mrow_ref, start_ref, end_ref, m_ref,
     tmo_w, tmo_p, tmo_out, tmi_w, tmi_p, tmi_out, tas_w, tas_b, tas_out, tae_w, tae_b, tae_out, ptr_in, ptr_out, next_b,
     o_ref, mback_ref, bias_ref,
     zbuf, tbuf, stage, ab_send, ab_recv, x_send, x_recv, ln_stage, gate, proj, gated, bias_t, bias_send, bias_recv, z_send, z_recv, zb_recv, nb_send, nb_recv,
     sends, recvs, m_sends, m_recvs, m_own) = refs
    n_res, length, dim = z_ref.shape
    tri = tmo_out.shape[0]
    n_chan = tri // n_dev
    tokens = n_res * length
    me = lax.axis_index(GROUP_AXIS)
    entry_barrier(n_dev, me)
    exchange = Exchange(n_dev, me, sends, recvs)

    def m_copy(dst_dev, slot):
        return pltpu.make_async_remote_copy(
            src_ref=m_ref.at[dst_dev], dst_ref=mback_ref.at[slot], send_sem=m_sends.at[dst_dev], recv_sem=m_recvs.at[slot],
            device_id={GROUP_AXIS: dst_dev}, device_id_type=pl.DeviceIdType.MESH)

    own = pltpu.make_async_copy(m_ref.at[me], mback_ref.at[me], m_own)
    own.start()

    def m_steps(lo, hi):
        def send(step, carry):
            m_copy(lax.rem(me + step, n_dev), me).start()
            return carry
        lax.fori_loop(lo, hi, send, 0)

    def normed_tokens():
        return layer_norm_f32(zbuf[...].astype(F32).reshape(tokens, dim))

    def tri_mul(turn, w_ref, p_ref, out_ref, contract):
        x_norm = normed_tokens()
        for part in range(2):
            value = lax.dot_general(w_ref[part * tri:(part + 1) * tri, :], x_norm, NT, preferred_element_type=F32)
            opened = lax.dot_general(w_ref[(2 + part) * tri:(3 + part) * tri, :], x_norm, NT, preferred_element_type=F32)
            gated_t = mrow_ref[...] * jax.nn.sigmoid(opened) * value
            for d in range(n_dev):
                for i in range(n_res):
                    tile = gated_t[d * n_chan:(d + 1) * n_chan, i * length:(i + 1) * length]
                    stage[pl.ds(d * n_chan * n_res + i, n_chan, stride=n_res), :] = tile
            ab_send[turn, :, part] = stage[...].reshape(n_dev, n_chan, n_res, length).astype(BF16)
        arrived = exchange.start(ab_send.at[turn], ab_recv.at[turn])
        m_steps(3 + 2 * turn, 4 + 2 * turn)
        gate[...] = jax.nn.sigmoid(jnp.dot(x_norm, p_ref[:, 4 * tri:], preferred_element_type=F32))
        arrived()
        for c in range(n_chan):
            left = ab_recv[turn, :, 0, c].astype(F32).reshape(length, length).astype(BF16)
            right = ab_recv[turn, :, 1, c].astype(F32).reshape(length, length).astype(BF16)
            product = lax.dot_general(left, right, contract, preferred_element_type=F32)
            x_send[turn, :, c] = product.reshape(n_dev, n_res, length)
        arrived = exchange.start(x_send.at[turn], x_recv.at[turn])
        m_steps(4 + 2 * turn, 5 + 2 * turn)
        arrived()
        values = x_recv[turn].reshape(tri, n_res, length)
        centered = values - jnp.mean(values, axis=0, keepdims=True)
        inverse = lax.rsqrt(jnp.mean(centered * centered, axis=0, keepdims=True) + 1e-5)
        pitch = tri + 8
        for c in range(tri):
            ln_stage[pl.ds(c, n_res, stride=pitch), :] = centered[c] * inverse[0]
        for i in range(n_res):
            columns = ln_stage[i * pitch:i * pitch + tri, :].astype(BF16)
            update = gate[i * length:(i + 1) * length, :] * lax.dot_general(columns, out_ref[...], TN, preferred_element_type=F32)
            zbuf[i] = (zbuf[i].astype(F32) + update).astype(BF16)

    def local_bias(x_norm, b_ref, send_ref):
        heads_pad = b_ref.shape[0]
        rows = lax.dot_general(b_ref[...], x_norm, NT, preferred_element_type=F32)
        for i in range(n_res):
            stage[pl.ds(i, heads_pad, stride=n_res), :] = rows[:, i * length:(i + 1) * length]
        heads = send_ref.shape[0]
        send_ref[...] = stage[0:heads * n_res, :].reshape(heads, n_res, length).astype(BF16)

    def attention(source, w_ref, out_ref, mask_ref, heads):
        def store_row(j, value):
            source[j] = value.astype(BF16)

        attention_rows(proj, gated, 0, n_res, heads, out_ref.shape[0], lambda j: source[j].astype(F32), w_ref[...], out_ref[...],
                       lambda j: mask_ref[j], lambda h: bias_t[h], store_row)

    def swap_blocks(source):
        for i in range(n_res):
            row = source[i].astype(F32)
            for d in range(n_dev):
                stage[pl.ds(d * n_res * n_res + i, n_res, stride=n_res), :] = row[d * n_res:(d + 1) * n_res, :]
        return stage[...].reshape(n_dev, n_res, n_res, dim).astype(BF16)

    def rows_of(received, i):
        return received[:, i].astype(F32).reshape(length, dim).astype(BF16)

    heads = bias_send.shape[1]
    m_steps(1, 3)
    zbuf[...] = z_ref[...]
    tri_mul(0, tmo_w, tmo_p, tmo_out, NT)
    tri_mul(1, tmi_w, tmi_p, tmi_out, TN)
    local_bias(normed_tokens(), tas_b, bias_send.at[0])
    arrived = exchange.start(bias_send.at[0], bias_recv.at[0], broadcast=True)
    arrived()
    m_steps(7, 10)
    for h in range(heads):
        bias_t[h] = rows_of(bias_recv.at[0], h).astype(F32).T * LOG2E
    attention(zbuf, tas_w, tas_out, start_ref, heads)
    local_bias(normed_tokens(), tae_b, bias_send.at[1])
    bias_arrived = exchange.start(bias_send.at[1], bias_recv.at[1], broadcast=True)
    z_send[0] = swap_blocks(zbuf)
    arrived = exchange.start(z_send.at[0], z_recv)
    bias_arrived()
    for h in range(heads):
        bias_t[h] = rows_of(bias_recv.at[1], h).astype(F32) * LOG2E
    arrived()
    m_steps(10, 13)
    for j in range(n_res):
        tbuf[j] = rows_of(z_recv, j)
    attention(tbuf, tae_w, tae_out, end_ref, heads)
    z_send[1] = swap_blocks(tbuf)
    arrived = exchange.start(z_send.at[1], zb_recv)
    m_steps(13, n_dev)
    arrived()
    for i in range(n_res):
        zbuf[i] = rows_of(zb_recv, i)
    x_norm = normed_tokens()
    hidden = jnp.maximum(jnp.dot(x_norm, ptr_in[...], preferred_element_type=F32), 0.0).astype(BF16)
    update = jnp.dot(hidden, ptr_out[...], preferred_element_type=F32)
    result = (zbuf[...].astype(F32) + update.reshape(n_res, length, dim)).astype(BF16)
    o_ref[...] = result
    if with_bias:
        zbuf[...] = result
        local_bias(normed_tokens(), next_b, nb_send)
        arrived = exchange.start(nb_send, nb_recv, broadcast=True)
        arrived()
        for h in range(bias_ref.shape[0]):
            bias_ref[h] = rows_of(nb_recv, h).astype(F32).T * LOG2E
    else:
        bias_ref[...] = jnp.zeros_like(bias_ref)
    own.wait()

    def m_wait(step, carry):
        other = lax.rem(me + step, n_dev)
        m_copy(other, other).wait_recv()
        m_copy(other, me).wait_send()
        return carry

    lax.fori_loop(1, n_dev, m_wait, 0)


def pair_stack(pair_loc, m_half, masks, stacked, layer, with_bias):
    n_res, length, dim = pair_loc.shape
    n_dev = masks['n_dev']
    tri = stacked['tmo_out'].shape[1]
    heads = masks['pair_heads']
    row_heads = stacked['row_bias'].shape[1]
    n_chan = tri // n_dev
    next_layer = layer + 1 if with_bias else layer
    names = ('tmo_w', 'tmo_proj', 'tmo_out', 'tmi_w', 'tmi_proj', 'tmi_out', 'tas_qkvg', 'tas_bias', 'tas_out', 'tae_qkvg', 'tae_bias', 'tae_out', 'ptr_in', 'ptr_out')
    weights = [stacked[k] for k in names] + [stacked['row_bias']]
    specs = [layer_of(w, layer) for w in weights[:-1]] + [layer_of(weights[-1], next_layer)]
    width = stacked['tas_out'].shape[1]
    n_phases = 9
    scratch = [
        pltpu.VMEM((n_res, length, dim), BF16), pltpu.VMEM((n_res, length, dim), BF16),
        pltpu.VMEM((n_dev * n_res * n_res, LANES), F32),
        pltpu.VMEM((2, n_dev, 2, n_chan, n_res, length), BF16), pltpu.VMEM((2, n_dev, 2, n_chan, n_res, length), BF16),
        pltpu.VMEM((2, n_dev, n_chan, n_res, length), F32), pltpu.VMEM((2, n_dev, n_chan, n_res, length), F32),
        pltpu.VMEM((n_res * (tri + 8), length), F32), pltpu.VMEM((n_res * length, dim), F32),
        pltpu.VMEM((n_res, 4 * width, length), BF16), pltpu.VMEM((n_res, width, length), BF16),
        pltpu.VMEM((heads, length, length), F32),
        pltpu.VMEM((2, heads, n_res, length), BF16), pltpu.VMEM((2, n_dev, heads, n_res, length), BF16),
        pltpu.VMEM((2, n_dev, n_res, n_res, dim), BF16), pltpu.VMEM((n_dev, n_res, n_res, dim), BF16), pltpu.VMEM((n_dev, n_res, n_res, dim), BF16),
        pltpu.VMEM((row_heads, n_res, length), BF16), pltpu.VMEM((n_dev, row_heads, n_res, length), BF16),
        pltpu.SemaphoreType.DMA((n_phases, n_dev)), pltpu.SemaphoreType.DMA((n_phases, n_dev)),
        pltpu.SemaphoreType.DMA((n_dev,)), pltpu.SemaphoreType.DMA((n_dev,)), pltpu.SemaphoreType.DMA,
    ]
    return pl.pallas_call(
        functools.partial(pair_kernel, n_dev, with_bias),
        grid=(1,),
        in_specs=[VMEM_SPEC] * 4 + [ANY_SPEC] + specs,
        out_specs=[VMEM_SPEC, ANY_SPEC, VMEM_SPEC],
        out_shape=[jax.ShapeDtypeStruct(pair_loc.shape, BF16), jax.ShapeDtypeStruct(m_half.shape, BF16), jax.ShapeDtypeStruct((row_heads, length, length), F32)],
        scratch_shapes=scratch,
        compiler_params=pltpu.CompilerParams(collective_id=3 * layer + 2, has_side_effects=True),
        cost_estimate=pl.CostEstimate(flops=4_000_000_000, bytes_accessed=16_000_000, transcendentals=4_000_000),
        name='pair_stack',
    )(pair_loc, masks['pair_rows'].reshape(1, n_res * length), masks['start'], masks['end'], m_half, *weights)


def pair_stack(pair_loc, m_half, masks, stacked, layer, with_bias):
    n_res, length, dim = pair_loc.shape
    n_dev = masks['n_dev']
    tri = stacked['tmo_out'].shape[1]
    heads = masks['pair_heads']
    row_heads = stacked['row_bias'].shape[1]
    n_chan = tri // n_dev
    next_layer = layer + 1 if with_bias else layer
    names = ('tmo_w', 'tmo_proj', 'tmo_out', 'tmi_w', 'tmi_proj', 'tmi_out', 'tas_qkvg', 'tas_bias', 'tas_out', 'tae_qkvg', 'tae_bias', 'tae_out', 'ptr_in', 'ptr_out')
    weights = [stacked[k] for k in names] + [stacked['row_bias']]
    specs = [layer_of(w, layer) for w in weights[:-1]] + [layer_of(weights[-1], next_layer)]
    width = stacked['tas_out'].shape[1]
    n_phases = 9
    scratch = [
        pltpu.VMEM((n_res, length, dim), BF16), pltpu.VMEM((n_res, length, dim), BF16),
        pltpu.VMEM((n_dev * n_res * n_res, LANES), F32),
        pltpu.VMEM((2, n_dev, 2, n_chan, n_res, length), BF16), pltpu.VMEM((2, n_dev, 2, n_chan, n_res, length), BF16),
        pltpu.VMEM((2, n_dev, n_chan, n_res, length), F32), pltpu.VMEM((2, n_dev, n_chan, n_res, length), F32),
        pltpu.VMEM((n_res * (tri + 8), length), F32), pltpu.VMEM((n_res * length, dim), F32),
        pltpu.VMEM((n_res, 4 * width, length), BF16), pltpu.VMEM((n_res, width, length), BF16),
        pltpu.VMEM((heads, length, length), F32),
        pltpu.VMEM((2, heads, n_res, length), BF16), pltpu.VMEM((2, n_dev, heads, n_res, length), BF16),
        pltpu.VMEM((2, n_dev, n_res, n_res, dim), BF16), pltpu.VMEM((n_dev, n_res, n_res, dim), BF16), pltpu.VMEM((n_dev, n_res, n_res, dim), BF16),
        pltpu.VMEM((row_heads, n_res, length), BF16), pltpu.VMEM((n_dev, row_heads, n_res, length), BF16),
        pltpu.SemaphoreType.DMA((n_phases, n_dev)), pltpu.SemaphoreType.DMA((n_phases, n_dev)),
        pltpu.SemaphoreType.DMA((n_dev,)), pltpu.SemaphoreType.DMA((n_dev,)), pltpu.SemaphoreType.DMA,
    ]
    return pl.pallas_call(
        functools.partial(pair_kernel, n_dev, with_bias),
        grid=(1,),
        in_specs=[VMEM_SPEC] * 4 + [ANY_SPEC] + specs,
        out_specs=[VMEM_SPEC, ANY_SPEC, VMEM_SPEC],
        out_shape=[jax.ShapeDtypeStruct(pair_loc.shape, BF16), jax.ShapeDtypeStruct(m_half.shape, BF16), jax.ShapeDtypeStruct((row_heads, length, length), F32)],
        scratch_shapes=scratch,
        compiler_params=pltpu.CompilerParams(collective_id=3 * layer + 2, has_side_effects=True),
        cost_estimate=pl.CostEstimate(flops=4_000_000_000, bytes_accessed=16_000_000, transcendentals=4_000_000),
        name='pair_stack',
    )(pair_loc, masks['pair_rows'].reshape(1, n_res * length), masks['start'], masks['end'], m_half, *weights)


def head_bias(pair_norm, w_bias):
    return jnp.einsum('ijc,ch->hij', pair_norm, w_bias, preferred_element_type=F32).astype(BF16)


def gather_bias(pair_rows, w_bias):
    full = lax.all_gather(head_bias(layer_norm(pair_rows), w_bias), GROUP_AXIS, axis=1, tiled=True)
    return jnp.swapaxes(full, 1, 2).astype(F32) * LOG2E


def outer_product_kernel(n_dev, early_ref, late_ref, b_ref, w_ref, o_ref, stage, left, rows, flat, slots, *ring_sems):
    half = early_ref.shape[0]
    dim = early_ref.shape[1] // 2
    length = early_ref.shape[2]
    n_half = n_dev * half
    pitch = stage.shape[2] // dim
    parts = [slice(part * LANES, (part + 1) * LANES) for part in range(length // LANES)]
    me = lax.axis_index(GROUP_AXIS)
    entry_barrier(n_dev, me)
    ring = ChipRing(n_dev, me, late_ref.at[:, pl.ds(dim, dim)], slots, *ring_sems)
    ring.send(1)

    def spread(k, source, src):
        for r in range(half):
            tile = source(r).astype(F32)
            for part, lanes in enumerate(parts):
                for lo in range(0, dim, 8):
                    stage[k, part, pl.ds(lo * pitch + src * half + r, 8, stride=pitch), :] = tile[lo:lo + 8, lanes]

    def collect(k):
        for e in range(dim):
            for part, lanes in enumerate(parts):
                rows[e, k * n_half:(k + 1) * n_half, lanes] = stage[k, part, e * pitch:e * pitch + n_half, :].astype(BF16)

    def spread_early(lo, hi):
        def one(src, carry):
            spread(0, lambda r: b_ref[src, r], src)
            return carry
        lax.fori_loop(lo, hi, one, 0)

    def spread_late(src):
        spread(1, lambda r: slots[src, r], src)

    hops = ring.right_hops
    shares = [n_dev * k // hops for k in range(hops + 1)]
    spread(1, lambda r: late_ref[r, dim:2 * dim, :], me)
    for k, ab_ref in enumerate((early_ref, late_ref)):
        for r in range(half):
            left[(k * half + r) * dim:(k * half + r + 1) * dim, :] = ab_ref[r, 0:dim, :]
    for hop in range(1, hops + 1):
        spread_early(shares[hop - 1], shares[hop])
        if hop == hops:
            collect(0)
        ring.receive(hop)
        ring.send(hop + 1)
        for away in ([0] if hop == 1 else ring.arrivals(hop - 1)):
            spread_late(ring.receive_mate(away))
        for away in ring.arrivals(hop):
            spread_late(ring.device(away))
    for away in ring.arrivals(hops):
        spread_late(ring.receive_mate(away))
    collect(1)

    def one(step, carry):
        some = [step * 4 + k for k in range(4)]
        products = [lax.dot_general(left[...], rows[e], NT, preferred_element_type=F32).astype(BF16) for e in some]
        for e, product in zip(some, products):
            for i in range(2 * half):
                flat[i, pl.ds(pl.multiple_of(e * dim, dim), dim), :] = product[i * dim:(i + 1) * dim, :]
        return carry

    lax.fori_loop(0, dim // 4, one, 0)
    for i in range(2 * half):
        o_ref[i] = jnp.dot(w_ref[...], flat[i], preferred_element_type=F32).T
    ring.drain()


def outer_update(ab_halves, b_early, overlap, stacked, layer, n_dev):
    half, n_ab, seq_all = ab_halves[0].shape
    opm_dim = n_ab // 2
    n_half = n_dev * half
    length = 2 * n_half
    dim = stacked['opm_w'].shape[1]
    update = pl.pallas_call(
        functools.partial(outer_product_kernel, n_dev),
        grid=(1,),
        in_specs=[VMEM_SPEC] * 3 + [layer_of(stacked['opm_w'], layer)], out_specs=VMEM_SPEC,
        out_shape=jax.ShapeDtypeStruct((2 * half, length, dim), F32),
        scratch_shapes=[pltpu.VMEM((2, seq_all // LANES, opm_dim * (n_half + 8), LANES), F32),
                        pltpu.VMEM((2 * half * opm_dim, seq_all), BF16), pltpu.VMEM((opm_dim, length, seq_all), BF16),
                        pltpu.VMEM((2 * half, opm_dim * opm_dim, length), BF16), pltpu.VMEM(b_early.shape, BF16)] + ring_semaphores(n_dev),
        compiler_params=pltpu.CompilerParams(collective_id=3 * stacked['opm_w'].shape[0] + 1 + layer, has_side_effects=True),
        cost_estimate=pl.CostEstimate(flops=4_000_000_000, bytes_accessed=6_000_000, transcendentals=0),
        name='outer_product',
    )(ab_halves[0], ab_halves[1], b_early, stacked['opm_w'])
    update = update.reshape(2 * half, 2, n_dev, half, dim)
    update = jnp.swapaxes(update, 1, 2).reshape(2 * half, length, dim)
    return update / (1e-3 + overlap)[:, :, None]


def first_gather_kernel(n_dev, z_ref, b_ref, masks_ref, bias_ref, full_ref, stage, bias_send, bias_recv, sends, recvs):
    n_res, length, dim = z_ref.shape
    me = lax.axis_index(GROUP_AXIS)
    entry_barrier(n_dev, me)
    exchange = Exchange(n_dev, me, sends, recvs)
    masks_arrived = exchange.start(masks_ref, full_ref, broadcast=True)
    rows = lax.dot_general(b_ref[...], layer_norm_f32(z_ref[...].astype(F32).reshape(n_res * length, dim)), NT, preferred_element_type=F32)
    heads = bias_send.shape[0]
    for i in range(n_res):
        stage[pl.ds(i, heads, stride=n_res), :] = rows[:, i * length:(i + 1) * length]
    bias_send[...] = stage[...].reshape(heads, n_res, length).astype(BF16)
    exchange.start(bias_send, bias_recv, broadcast=True)()
    for h in range(heads):
        bias_ref[h] = bias_recv[:, h].astype(F32).reshape(length, length).T * LOG2E
    masks_arrived()


def first_gather(pair_loc, packed_masks, stacked, n_dev):
    n_res, length, dim = pair_loc.shape
    heads = stacked['row_bias'].shape[1]
    return pl.pallas_call(
        functools.partial(first_gather_kernel, n_dev),
        grid=(1,),
        in_specs=[VMEM_SPEC, layer_of(stacked['row_bias'], 0), VMEM_SPEC], out_specs=[VMEM_SPEC, VMEM_SPEC],
        out_shape=[jax.ShapeDtypeStruct((heads, length, length), F32), jax.ShapeDtypeStruct((n_dev,) + packed_masks.shape, BF16)],
        scratch_shapes=[pltpu.VMEM((heads * n_res, length), F32), pltpu.VMEM((heads, n_res, length), BF16), pltpu.VMEM((n_dev, heads, n_res, length), BF16),
                        pltpu.SemaphoreType.DMA((2, n_dev)), pltpu.SemaphoreType.DMA((2, n_dev))],
        compiler_params=pltpu.CompilerParams(collective_id=3 * stacked['row_bias'].shape[0], has_side_effects=True),
        cost_estimate=pl.CostEstimate(flops=1_000_000_000, bytes_accessed=2_000_000, transcendentals=0),
        name='first_gather',
    )(pair_loc, stacked['row_bias'], packed_masks)


def evoformer_block(m_arrays, pair_loc, bias_t, masks, stacked, layer, with_bias):
    heads = masks['msa_heads']
    early, ab_early, late = rows_and_columns(m_arrays, bias_t, masks, stacked, layer, heads)
    late, ab_late, m_early, b_early = late_columns(late, early, ab_early, masks, stacked, layer, heads)
    pair_loc = residual(pair_loc, outer_update((ab_early, ab_late), b_early, masks['overlap'], stacked, layer, masks['n_dev']))
    pair_loc, m_late, bias_t = pair_stack(pair_loc, late, masks, stacked, layer, with_bias)
    return (m_early, m_late), pair_loc, bias_t


WEIGHT_NAMES = ('row_qkvg', 'row_bias', 'row_out', 'col_qkvg', 'col_out', 'mtr_in', 'mtr_out', 'opm_proj', 'opm_out', 'tmo_proj', 'tmo_out',
                'tmi_proj', 'tmi_out', 'tas_qkvg', 'tas_bias', 'tas_out', 'tae_qkvg', 'tae_bias', 'tae_out', 'ptr_in', 'ptr_out')


def prepare_weights(weights):
    stacked = dict(zip(WEIGHT_NAMES, weights))
    for kind in ('tmo', 'tmi'):
        tri = stacked[kind + '_out'].shape[1]
        stacked[kind + '_w'] = jnp.swapaxes(stacked[kind + '_proj'][:, :, :4 * tri], 1, 2)
    for name in ('row_qkvg', 'col_qkvg', 'opm_proj', 'tas_qkvg', 'tae_qkvg'):
        stacked[name] = jnp.swapaxes(stacked[name], 1, 2)
    for name in ('row_bias', 'tas_bias', 'tae_bias'):
        stacked[name] = jnp.pad(jnp.swapaxes(stacked[name], 1, 2), ((0, 0), (0, -stacked[name].shape[2] % 8), (0, 0)))
    n_layers, flat, dim = stacked['opm_out'].shape
    opm_dim = stacked['opm_proj'].shape[1] // 2
    stacked['opm_w'] = jnp.transpose(stacked['opm_out'].reshape(n_layers, opm_dim, opm_dim, dim), (0, 3, 2, 1)).reshape(n_layers, dim, flat)
    return stacked


def pack_masks(msa_mask, pair_mask):
    return jnp.concatenate([msa_mask, pair_mask], 0).astype(BF16)


def make_masks(msa_mask, pair_mask, full, n_dev):
    shard_idx = lax.axis_index(GROUP_AXIS)
    n_seq, length = msa_mask.shape
    n_res = pair_mask.shape[0]
    full = full.astype(F32)
    full_msa = full[:, :n_seq].reshape(n_dev * n_seq, length)
    full_pair = full[:, n_seq:].reshape(n_dev * n_res, length)
    res_mask = lax.dynamic_slice_in_dim(full_msa, shard_idx * n_res, n_res, 1).T
    end_mask = lax.dynamic_slice_in_dim(full_pair, shard_idx * n_res, n_res, 1).T
    lanes = lambda mask: jnp.broadcast_to(mask.astype(F32)[:, :, None], mask.shape + (length,))
    return {
        'n_dev': n_dev,
        'seq': lanes(msa_mask),
        'res': lanes(res_mask),
        'res_row': res_mask[:, None, :],
        'pair_rows': pair_mask.astype(F32),
        'start': lanes(pair_mask),
        'end': lanes(end_mask),
        'overlap': jnp.dot(res_mask, full_msa, precision=lax.Precision.DEFAULT, preferred_element_type=F32),
    }


def solution(mesh):
    row_spec = P((PARTS_AXIS, GROUP_AXIS))
    n_dev = mesh.shape[GROUP_AXIS]

    def local_body(value_a7, pair_loc, msa_mask, pair_mask, *weights):
        stacked = prepare_weights(weights)
        bias_t, full = first_gather(pair_loc, pack_masks(msa_mask, pair_mask), stacked, n_dev)
        masks = make_masks(msa_mask, pair_mask, full, n_dev)
        masks['msa_heads'] = weights[1].shape[2]
        masks['pair_heads'] = weights[14].shape[2]
        n_layers = weights[0].shape[0]
        m_arrays = (value_a7,)
        for layer in range(n_layers):
            m_arrays, pair_loc, bias_t = evoformer_block(m_arrays, pair_loc, bias_t, masks, stacked, layer, layer + 1 < n_layers)
        n_seq, length, dim = value_a7.shape
        value_a7 = jnp.transpose(jnp.stack(m_arrays, 1), (3, 0, 1, 2, 4)).reshape(n_seq, length, dim)
        return value_a7, pair_loc

    def run_blocks(*arrays):
        n_weights = len(arrays) - 4
        return jax.shard_map(local_body, mesh=mesh, in_specs=(row_spec,) * 4 + (P(),) * n_weights, out_specs=(row_spec, row_spec), check_vma=False)(*arrays)

    return run_blocks
```

```python
import functools
import math

import jax
import jax.numpy as jnp
from jax import lax
from jax.experimental import pallas as pl
from jax.experimental.pallas import tpu as pltpu
from jax.sharding import PartitionSpec as P

GROUP_AXIS = 'dap'
PARTS_AXIS = 'req'
LOG2E = math.log2(math.e)
MASKED = -1e9 * LOG2E
LANES = 128
AHEAD = 4
F32 = jnp.float32
BF16 = jnp.bfloat16
NT = (((1,), (1,)), ((), ()))
TN = (((0,), (0,)), ((), ()))


def layer_norm_f32(values):
    centered = values - jnp.mean(values, axis=-1, keepdims=True)
    variance = jnp.mean(centered * centered, axis=-1, keepdims=True)
    return (centered * lax.rsqrt(variance + 1e-5)).astype(BF16)


def layer_norm(x):
    return layer_norm_f32(x.astype(F32))


def residual(x, update):
    return (x.astype(F32) + update).astype(BF16)


def dense(x, weight):
    return jnp.einsum('...c,cf->...f', x, weight, preferred_element_type=F32)


def softmax_keys_first(logits):
    top = jnp.max(logits, axis=0, keepdims=True)
    raised = jnp.exp2(logits - top)
    total = jnp.sum(raised, axis=0, keepdims=True)
    return (raised * (1.0 / total)).astype(BF16)


def pipelined_units(units, ahead, first_stage, second_stage):
    ready = {}
    for idx in range(min(ahead, len(units))):
        ready[idx] = first_stage(*units[idx])
    for idx in range(len(units)):
        if idx + ahead < len(units):
            ready[idx + ahead] = first_stage(*units[idx + ahead])
        second_stage(ready.pop(idx), *units[idx])


def attention_rows(proj, gated, base, rows, heads, width, load_row, w_t, w_out, mask_of, bias_of, store_row):
    head_dim = width // heads
    scale = head_dim ** -0.5 * LOG2E

    def head_rows(j, part, h):
        lo = part * width + h * head_dim
        return proj[j, lo:lo + head_dim, :]

    normed = [layer_norm_f32(load_row(base + j)) for j in range(rows)]
    for j in range(rows):
        proj[j] = lax.dot_general(w_t, normed[j], NT, preferred_element_type=F32).astype(BF16)

    def logits_of(j, h):
        return lax.dot_general(head_rows(j, 1, h), head_rows(j, 0, h), TN, preferred_element_type=F32)

    def finish(raw, j, h):
        logits = jnp.where(mask_of(base + j) > 0.0, raw * scale + bias_of(h), MASKED)
        out_t = jnp.dot(head_rows(j, 2, h), softmax_keys_first(logits), preferred_element_type=F32)
        gate = jax.nn.sigmoid(head_rows(j, 3, h).astype(F32))
        gated[j, h * head_dim:(h + 1) * head_dim, :] = (out_t * gate).astype(BF16)

    pipelined_units([(j, h) for j in range(rows) for h in range(heads)], AHEAD, logits_of, finish)
    for j in range(rows):
        store_row(base + j, load_row(base + j) + lax.dot_general(gated[j], w_out, TN, preferred_element_type=F32))


def column_residue(heads, x, proj, gated, mask_ref, mrow, w_ref, wo_ref, win_ref, wtr_ref, wopm_ref):
    width = wo_ref.shape[0]
    head_dim = width // heads
    scale = head_dim ** -0.5 * LOG2E
    length, lanes = mask_ref.shape
    proj[...] = lax.dot_general(w_ref[...], layer_norm_f32(x), NT, preferred_element_type=F32).astype(BF16)

    def head_rows(part, h, cols=slice(None)):
        lo = part * width + h * head_dim
        return proj[lo:lo + head_dim, cols]

    def columns(c):
        return slice(c * lanes, (c + 1) * lanes)

    def logits_of(h, c):
        return lax.dot_general(head_rows(1, h), head_rows(0, h, columns(c)), TN, preferred_element_type=F32)

    def finish(raw, h, c):
        logits = jnp.where(mask_ref[...] > 0.0, raw * scale, MASKED)
        out_t = jnp.dot(head_rows(2, h), softmax_keys_first(logits), preferred_element_type=F32)
        gate = jax.nn.sigmoid(head_rows(3, h, columns(c)).astype(F32))
        gated[h * head_dim:(h + 1) * head_dim, columns(c)] = (out_t * gate).astype(BF16)

    pipelined_units([(h, c) for h in range(heads) for c in range(length // lanes)], AHEAD, logits_of, finish)
    update = lax.dot_general(gated[...], wo_ref[...], TN, preferred_element_type=F32)
    x = (x + update).astype(BF16).astype(F32)
    hidden = jnp.maximum(jnp.dot(layer_norm_f32(x), win_ref[...], preferred_element_type=F32), 0.0).astype(BF16)
    x = (x + jnp.dot(hidden, wtr_ref[...], preferred_element_type=F32)).astype(BF16)
    ab_t = lax.dot_general(wopm_ref[...], layer_norm_f32(x.astype(F32)), NT, preferred_element_type=F32).astype(BF16)
    return x, (ab_t.astype(F32) * mrow).astype(BF16)


def peer_copy(source, target, send_sem, recv_sem, dst_dev):
    return pltpu.make_async_remote_copy(src_ref=source, dst_ref=target, send_sem=send_sem, recv_sem=recv_sem,
                                        device_id={GROUP_AXIS: dst_dev}, device_id_type=pl.DeviceIdType.MESH)


def for_peers(n_dev, me, body, lo=1, hi=None):
    def step(k, carry):
        body(lax.rem(me + k, n_dev))
        return carry
    lax.fori_loop(lo, n_dev if hi is None else hi, step, 0)


def rows_and_columns_kernel(heads, n_dev, first, group, *refs):
    n_m = 1 if first else 2
    m_refs, refs = refs[:n_m], refs[n_m:]
    (mask_ref, bias_ref, cmask_ref, mrow_ref, rw_ref, rwo_ref, cw_ref, cwo_ref, win_ref, wtr_ref, wopm_ref,
     o_ref, ab_ref, late_ref, proj, gated, cproj, cgated, stage_out, s_buf, r_buf, sends, recvs, own_sem) = refs[:24]
    n_seq, length = mask_ref.shape[:2]
    half = late_ref.shape[2]
    block = s_buf.shape[3]
    n_blocks = n_seq // block
    width = rwo_ref.shape[0]
    parts = stage_out.shape[0]
    me = lax.axis_index(GROUP_AXIS)
    entry_barrier(n_dev, me)
    if first:
        load_row = lambda s: m_refs[0][s].astype(F32)
    else:
        stage_in = refs[24]
        for part in range(parts):
            for d in range(n_dev):
                for k in range(2):
                    lo = (d * 2 + k) * half * n_seq
                    stage_in[part, lo:lo + half * n_seq, :] = m_refs[k][d, :, :, part * LANES:(part + 1) * LANES].astype(F32).reshape(half * n_seq, LANES)
        load_row = lambda s: jnp.concatenate([stage_in[part, pl.ds(s, length, stride=n_seq), :] for part in range(parts)], -1)

    def early(b, dst_dev, slot):
        return peer_copy(s_buf.at[b, dst_dev, pl.ds(0, half)], r_buf.at[slot, b], sends.at[0, b, dst_dev], recvs.at[0, b, slot], dst_dev)

    def late(b, dst_dev, slot):
        return peer_copy(s_buf.at[b, dst_dev, pl.ds(half, half)], late_ref.at[slot, b], sends.at[1, b, dst_dev], recvs.at[1, b, slot], dst_dev)

    def row_block(b, carry):
        def store_row(s, value):
            for part in range(parts):
                stage_out[part, pl.ds(s - b * block, length, stride=block), :] = value[:, part * LANES:(part + 1) * LANES]

        def some_rows(t, inner):
            attention_rows(proj, gated, b * block + t * group, group, heads, width, load_row, rw_ref[...], rwo_ref[...],
                           lambda s: mask_ref[s], lambda h: bias_ref[h], store_row)
            return inner

        lax.fori_loop(0, block // group, some_rows, 0)
        for part in range(parts):
            s_buf[b, :, :, :, part * LANES:(part + 1) * LANES] = stage_out[part].reshape(n_dev, 2 * half, block, LANES).astype(BF16)
        for_peers(n_dev, me, lambda d: early(b, d, me).start())
        r_buf[me, b] = s_buf[b, me, 0:half]
        return carry

    lax.fori_loop(0, n_blocks, row_block, 0)
    own = [pltpu.make_async_copy(s_buf.at[b, me, pl.ds(half, half)], late_ref.at[me, b], own_sem.at[b]) for b in range(n_blocks)]
    for b in range(n_blocks):
        for_peers(n_dev, me, lambda d: late(b, d, me).start())
        own[b].start()
    for b in range(n_blocks):
        for_peers(n_dev, me, lambda d: early(b, d, d).wait_recv())

    def residue(r, carry):
        x = r_buf[:, :, r].astype(F32).reshape(n_dev * n_seq, -1)
        x, ab = column_residue(heads, x, cproj, cgated, cmask_ref.at[r], mrow_ref[r], cw_ref, cwo_ref, win_ref, wtr_ref, wopm_ref)
        o_ref[:, r] = x.reshape(n_dev, n_seq, -1)
        ab_ref[r] = ab
        return carry

    lax.fori_loop(0, half, residue, 0)
    for b in range(n_blocks):
        own[b].wait()
        for_peers(n_dev, me, lambda d: late(b, d, d).wait_recv())
        for_peers(n_dev, me, lambda d: early(b, d, me).wait_send())
        for_peers(n_dev, me, lambda d: late(b, d, me).wait_send())


def layer_of(stacked, layer):
    return pl.BlockSpec((None,) + stacked.shape[1:], lambda step: (layer,) + (0,) * (stacked.ndim - 1))


VMEM_SPEC = pl.BlockSpec(memory_space=pltpu.VMEM)
ANY_SPEC = pl.BlockSpec(memory_space=pl.ANY)


def rows_and_columns(m_arrays, bias_t, masks, stacked, layer, heads, group=4, block=8):
    n_dev = masks['n_dev']
    n_seq, length = masks['seq'].shape[:2]
    first = len(m_arrays) == 1
    dim = m_arrays[0].shape[-1]
    half = length // n_dev // 2
    n_blocks = n_seq // block
    seq_all = n_dev * n_seq
    weights = [stacked[k] for k in ('row_qkvg', 'row_out', 'col_qkvg', 'col_out', 'mtr_in', 'mtr_out', 'opm_proj')]
    width = stacked['row_out'].shape[1]
    n_opm = stacked['opm_proj'].shape[1]
    scratch = [
        pltpu.VMEM((group, 4 * width, length), BF16), pltpu.VMEM((group, width, length), BF16),
        pltpu.VMEM((4 * width, seq_all), BF16), pltpu.VMEM((width, seq_all), BF16),
        pltpu.VMEM((dim // LANES, length * block, LANES), F32),
        pltpu.VMEM((n_blocks, n_dev, 2 * half, block, dim), BF16), pltpu.VMEM((n_dev, n_blocks, half, block, dim), BF16),
        pltpu.SemaphoreType.DMA((2, n_blocks, n_dev)), pltpu.SemaphoreType.DMA((2, n_blocks, n_dev)), pltpu.SemaphoreType.DMA((n_blocks,)),
    ]
    if not first:
        scratch.append(pltpu.VMEM((dim // LANES, length * n_seq, LANES), F32))
    n_data = len(m_arrays) + 4
    return pl.pallas_call(
        functools.partial(rows_and_columns_kernel, heads, n_dev, first, group),
        grid=(1,),
        in_specs=[VMEM_SPEC] * n_data + [layer_of(w, layer) for w in weights],
        out_specs=[VMEM_SPEC, VMEM_SPEC, ANY_SPEC],
        out_shape=[jax.ShapeDtypeStruct((n_dev, half, n_seq, dim), BF16), jax.ShapeDtypeStruct((half, n_opm, seq_all), BF16),
                   jax.ShapeDtypeStruct((n_dev, n_blocks, half, block, dim), BF16)],
        scratch_shapes=scratch,
        compiler_params=pltpu.CompilerParams(collective_id=3 * layer, has_side_effects=True),
        cost_estimate=pl.CostEstimate(flops=20_000_000_000, bytes_accessed=12_000_000, transcendentals=16_000_000),
        name='rows_and_columns',
    )(*m_arrays, masks['seq'], bias_t, masks['res'][:half], masks['res_row'][:half], *weights)


def late_columns_kernel(heads, n_dev, late_ref, cmask_ref, mrow_ref, m_ref, ab_early_ref, cw_ref, cwo_ref, win_ref, wtr_ref, wopm_ref,
                        o_ref, ab_ref, mback_ref, b_ref, cproj, cgated, sends, recvs, own_sem, b_sem, *ring_sems):
    me = lax.axis_index(GROUP_AXIS)
    half = late_ref.shape[2]
    n_seq = late_ref.shape[1] * late_ref.shape[3]
    entry_barrier(n_dev, me)
    n_opm = ab_early_ref.shape[1] // 2
    b_own = ab_early_ref.at[:, pl.ds(n_opm, n_opm)]
    ring = ChipRing(n_dev, me, b_own, b_ref, *ring_sems)
    b_local = pltpu.make_async_copy(b_own, b_ref.at[me], b_sem)
    ring.send(1)
    b_local.start()
    copy = lambda d, slot: peer_copy(m_ref.at[d], mback_ref.at[slot], sends.at[d], recvs.at[slot], d)
    own = pltpu.make_async_copy(m_ref.at[me], mback_ref.at[me], own_sem)
    own.start()

    def residue(r):
        x = late_ref[:, :, r].astype(F32).reshape(n_dev * n_seq, -1)
        x, ab = column_residue(heads, x, cproj, cgated, cmask_ref.at[r], mrow_ref[r], cw_ref, cwo_ref, win_ref, wtr_ref, wopm_ref)
        o_ref[:, r] = x.reshape(n_dev, n_seq, -1)
        ab_ref[r] = ab

    share = -(-(n_dev - 1) // half)

    def step(r, carry):
        hop = r + 1

        def send_m(k, inner):
            @pl.when(k < n_dev)
            def _():
                d = lax.rem(me + k, n_dev)
                copy(d, me).start()
            return inner

        lax.fori_loop(1 + r * share, 1 + (r + 1) * share, send_m, 0)
        residue(r)

        @pl.when(hop <= ring.right_hops)
        def _():
            ring.receive_from(-hop)

        @pl.when(hop <= ring.left_hops)
        def _():
            ring.receive_from(hop)

        @pl.when(hop + 1 <= ring.right_hops)
        def _():
            ring.right(hop + 1).start()

        @pl.when(hop + 1 <= ring.left_hops)
        def _():
            ring.left(hop + 1).start()

        return carry

    lax.fori_loop(0, half, step, 0)
    for hop in range(half + 1, ring.right_hops + 1):
        ring.receive(hop)
        ring.send(hop + 1)
    own.wait()
    b_local.wait()
    for_peers(n_dev, me, lambda d: copy(d, d).wait_recv())
    for_peers(n_dev, me, lambda d: copy(d, me).wait_send())
    ring.receive_mate(0)
    for k in range(1, ring.right_hops + 1):
        for away in ring.arrivals(k):
            ring.receive_mate(away)
    ring.drain()


def late_columns(late, m_half, ab_early, masks, stacked, layer, heads):
    n_dev, n_blocks, half, block, dim = late.shape
    seq_all = n_dev * n_blocks * block
    weights = [stacked[k] for k in ('col_qkvg', 'col_out', 'mtr_in', 'mtr_out', 'opm_proj')]
    width = stacked['row_out'].shape[1]
    n_opm = stacked['opm_proj'].shape[1]
    return pl.pallas_call(
        functools.partial(late_columns_kernel, heads, n_dev),
        grid=(1,),
        in_specs=[VMEM_SPEC] * 3 + [ANY_SPEC] * 2 + [layer_of(w, layer) for w in weights],
        out_specs=[VMEM_SPEC, VMEM_SPEC, ANY_SPEC, ANY_SPEC],
        out_shape=[jax.ShapeDtypeStruct(m_half.shape, BF16), jax.ShapeDtypeStruct((half, n_opm, seq_all), BF16), jax.ShapeDtypeStruct(m_half.shape, BF16),
                   jax.ShapeDtypeStruct((n_dev, half, n_opm // 2, seq_all), BF16)],
        scratch_shapes=[pltpu.VMEM((4 * width, seq_all), BF16), pltpu.VMEM((width, seq_all), BF16),
                        pltpu.SemaphoreType.DMA((n_dev,)), pltpu.SemaphoreType.DMA((n_dev,)), pltpu.SemaphoreType.DMA, pltpu.SemaphoreType.DMA] + ring_semaphores(n_dev),
        compiler_params=pltpu.CompilerParams(collective_id=3 * layer + 1, has_side_effects=True),
        cost_estimate=pl.CostEstimate(flops=20_000_000_000, bytes_accessed=12_000_000, transcendentals=8_000_000),
        name='late_columns',
    )(late, masks['res'][half:], masks['res_row'][half:], m_half, ab_early, *weights)


class Exchange:
    def __init__(self, n_dev, me, sends, recvs):
        self.n_dev, self.me, self.sends, self.recvs, self.used = n_dev, me, sends, recvs, 0

    def start(self, source, target, broadcast=False):
        phase = self.used
        self.used += 1
        pick = (lambda d: source) if broadcast else (lambda d: source.at[d])

        def copy(dst_dev, slot):
            return pltpu.make_async_remote_copy(
                src_ref=pick(dst_dev), dst_ref=target.at[slot], send_sem=self.sends.at[phase, dst_dev], recv_sem=self.recvs.at[phase, slot],
                device_id={GROUP_AXIS: dst_dev}, device_id_type=pl.DeviceIdType.MESH)

        def send(step, carry):
            copy(lax.rem(self.me + step, self.n_dev), self.me).start()
            return carry

        lax.fori_loop(1, self.n_dev, send, 0)
        target[self.me] = source[...] if broadcast else source[self.me]

        def finish():
            def wait(step, carry):
                other = lax.rem(self.me + step, self.n_dev)
                copy(other, other).wait_recv()
                copy(other, self.me).wait_send()
                return carry

            lax.fori_loop(1, self.n_dev, wait, 0)

        return finish


class ChipRing:
    def __init__(self, n_dev, me, own, slots, recvs, rights, lefts, partners):
        self.n_dev, self.me, self.own, self.slots = n_dev, me, own, slots
        self.recvs, self.rights, self.lefts, self.partners = recvs, rights, lefts, partners
        chips = n_dev // 2
        self.right_hops, self.left_hops = chips // 2, (chips - 1) // 2
        self.partner = me + 1 - 2 * lax.rem(me, 2)

    def device(self, chips_away):
        return lax.rem(self.me + 2 * chips_away + self.n_dev, self.n_dev)

    def mate(self, src):
        return src + 1 - 2 * lax.rem(src, 2)

    def copy(self, src, first, send_sem, to):
        return peer_copy(self.own if first else self.slots.at[src], self.slots.at[src], send_sem, self.recvs.at[src], to)

    def right(self, hop):
        return self.copy(self.device(1 - hop), isinstance(hop, int) and hop == 1, self.rights.at[hop], self.device(1))

    def left(self, hop):
        return self.copy(self.device(hop - 1), isinstance(hop, int) and hop == 1, self.lefts.at[hop], self.device(-1))

    def hand(self, src, first=False):
        return self.copy(src, first, self.partners.at[src], self.partner)

    def send(self, hop):
        if hop == 1:
            self.hand(self.me, True).start()
        if hop <= self.right_hops:
            self.right(hop).start()
        if hop <= self.left_hops:
            self.left(hop).start()

    def arrivals(self, hop):
        return ([-hop] if hop <= self.right_hops else []) + ([hop] if hop <= self.left_hops else [])

    def receive(self, hop):
        for away in self.arrivals(hop):
            self.receive_from(away)

    def receive_from(self, away):
        src = self.device(away)
        self.copy(src, False, self.rights.at[0], self.partner).wait_recv()
        self.hand(src).start()

    def receive_mate(self, away):
        src = self.mate(self.device(away))
        self.copy(src, False, self.rights.at[0], self.partner).wait_recv()
        return src

    def drain(self):
        self.hand(self.me, True).wait_send()
        for hop in range(1, self.right_hops + 1):
            self.right(hop).wait_send()
            if hop <= self.left_hops:
                self.left(hop).wait_send()
            for away in self.arrivals(hop):
                self.hand(self.device(away)).wait_send()


def ring_semaphores(n_dev):
    return [pltpu.SemaphoreType.DMA((n_dev,)) for k in range(4)]


def entry_barrier(n_dev, me):
    barrier = pltpu.get_barrier_semaphore()

    def signal(step, carry):
        pl.semaphore_signal(barrier, inc=1, device_id={GROUP_AXIS: lax.rem(me + step, n_dev)}, device_id_type=pl.DeviceIdType.MESH)
        return carry

    lax.fori_loop(1, n_dev, signal, 0)
    pl.semaphore_wait(barrier, n_dev - 1)


def pair_kernel(n_dev, with_bias, *refs):
    (z_ref, mrow_ref, start_ref, end_ref, m_ref,
     tmo_w, tmo_p, tmo_out, tmi_w, tmi_p, tmi_out, tas_w, tas_b, tas_out, tae_w, tae_b, tae_out, ptr_in, ptr_out, next_b,
     o_ref, mback_ref, bias_ref,
     zbuf, tbuf, stage, ab_send, ab_recv, x_send, x_recv, ln_stage, gate, proj, gated, bias_t, bias_send, bias_recv, z_send, z_recv, zb_recv, nb_send, nb_recv,
     sends, recvs, m_sends, m_recvs, m_own) = refs
    n_res, length, dim = z_ref.shape
    tri = tmo_out.shape[0]
    n_chan = tri // n_dev
    tokens = n_res * length
    me = lax.axis_index(GROUP_AXIS)
    entry_barrier(n_dev, me)
    exchange = Exchange(n_dev, me, sends, recvs)

    def m_copy(dst_dev, slot):
        return pltpu.make_async_remote_copy(
            src_ref=m_ref.at[dst_dev], dst_ref=mback_ref.at[slot], send_sem=m_sends.at[dst_dev], recv_sem=m_recvs.at[slot],
            device_id={GROUP_AXIS: dst_dev}, device_id_type=pl.DeviceIdType.MESH)

    own = pltpu.make_async_copy(m_ref.at[me], mback_ref.at[me], m_own)
    own.start()

    def m_steps(lo, hi):
        def send(step, carry):
            m_copy(lax.rem(me + step, n_dev), me).start()
            return carry
        lax.fori_loop(lo, hi, send, 0)

    def normed_tokens():
        return layer_norm_f32(zbuf[...].astype(F32).reshape(tokens, dim))

    def tri_mul(turn, w_ref, p_ref, out_ref, contract):
        x_norm = normed_tokens()
        for part in range(2):
            value = lax.dot_general(w_ref[part * tri:(part + 1) * tri, :], x_norm, NT, preferred_element_type=F32)
            opened = lax.dot_general(w_ref[(2 + part) * tri:(3 + part) * tri, :], x_norm, NT, preferred_element_type=F32)
            gated_t = mrow_ref[...] * jax.nn.sigmoid(opened) * value
            for d in range(n_dev):
                for i in range(n_res):
                    tile = gated_t[d * n_chan:(d + 1) * n_chan, i * length:(i + 1) * length]
                    stage[pl.ds(d * n_chan * n_res + i, n_chan, stride=n_res), :] = tile
            ab_send[turn, :, part] = stage[...].reshape(n_dev, n_chan, n_res, length).astype(BF16)
        arrived = exchange.start(ab_send.at[turn], ab_recv.at[turn])
        m_steps(3 + 3 * turn, 5 + 3 * turn)
        gate[...] = jax.nn.sigmoid(jnp.dot(x_norm, p_ref[:, 4 * tri:], preferred_element_type=F32))
        arrived()
        for c in range(n_chan):
            left = ab_recv[turn, :, 0, c].astype(F32).reshape(length, length).astype(BF16)
            right = ab_recv[turn, :, 1, c].astype(F32).reshape(length, length).astype(BF16)
            product = lax.dot_general(left, right, contract, preferred_element_type=F32)
            x_send[turn, :, c] = product.reshape(n_dev, n_res, length)
        arrived = exchange.start(x_send.at[turn], x_recv.at[turn])
        m_steps(5 + 3 * turn, 6 + 3 * turn)
        arrived()
        values = x_recv[turn].reshape(tri, n_res, length)
        centered = values - jnp.mean(values, axis=0, keepdims=True)
        inverse = lax.rsqrt(jnp.mean(centered * centered, axis=0, keepdims=True) + 1e-5)
        pitch = tri + 8
        for c in range(tri):
            ln_stage[pl.ds(c, n_res, stride=pitch), :] = centered[c] * inverse[0]
        for i in range(n_res):
            columns = ln_stage[i * pitch:i * pitch + tri, :].astype(BF16)
            update = gate[i * length:(i + 1) * length, :] * lax.dot_general(columns, out_ref[...], TN, preferred_element_type=F32)
            zbuf[i] = (zbuf[i].astype(F32) + update).astype(BF16)

    def local_bias(x_norm, b_ref, send_ref):
        heads_pad = b_ref.shape[0]
        rows = lax.dot_general(b_ref[...], x_norm, NT, preferred_element_type=F32)
        for i in range(n_res):
            stage[pl.ds(i, heads_pad, stride=n_res), :] = rows[:, i * length:(i + 1) * length]
        heads = send_ref.shape[0]
        send_ref[...] = stage[0:heads * n_res, :].reshape(heads, n_res, length).astype(BF16)

    def attention(source, w_ref, out_ref, mask_ref, heads):
        def store_row(j, value):
            source[j] = value.astype(BF16)

        attention_rows(proj, gated, 0, n_res, heads, out_ref.shape[0], lambda j: source[j].astype(F32), w_ref[...], out_ref[...],
                       lambda j: mask_ref[j], lambda h: bias_t[h], store_row)

    def swap_blocks(source):
        for i in range(n_res):
            row = source[i].astype(F32)
            for d in range(n_dev):
                stage[pl.ds(d * n_res * n_res + i, n_res, stride=n_res), :] = row[d * n_res:(d + 1) * n_res, :]
        return stage[...].reshape(n_dev, n_res, n_res, dim).astype(BF16)

    def rows_of(received, i):
        return received[:, i].astype(F32).reshape(length, dim).astype(BF16)

    heads = bias_send.shape[1]
    m_steps(1, 3)
    zbuf[...] = z_ref[...]
    tri_mul(0, tmo_w, tmo_p, tmo_out, NT)
    tri_mul(1, tmi_w, tmi_p, tmi_out, TN)
    local_bias(normed_tokens(), tas_b, bias_send.at[0])
    arrived = exchange.start(bias_send.at[0], bias_recv.at[0], broadcast=True)
    arrived()
    m_steps(9, 13)
    for h in range(heads):
        bias_t[h] = rows_of(bias_recv.at[0], h).astype(F32).T * LOG2E
    attention(zbuf, tas_w, tas_out, start_ref, heads)
    local_bias(normed_tokens(), tae_b, bias_send.at[1])
    bias_arrived = exchange.start(bias_send.at[1], bias_recv.at[1], broadcast=True)
    z_send[0] = swap_blocks(zbuf)
    arrived = exchange.start(z_send.at[0], z_recv)
    bias_arrived()
    for h in range(heads):
        bias_t[h] = rows_of(bias_recv.at[1], h).astype(F32) * LOG2E
    arrived()
    m_steps(13, n_dev)
    for j in range(n_res):
        tbuf[j] = rows_of(z_recv, j)
    attention(tbuf, tae_w, tae_out, end_ref, heads)
    z_send[1] = swap_blocks(tbuf)
    arrived = exchange.start(z_send.at[1], zb_recv)
    arrived()
    for i in range(n_res):
        zbuf[i] = rows_of(zb_recv, i)
    x_norm = normed_tokens()
    hidden = jnp.maximum(jnp.dot(x_norm, ptr_in[...], preferred_element_type=F32), 0.0).astype(BF16)
    update = jnp.dot(hidden, ptr_out[...], preferred_element_type=F32)
    result = (zbuf[...].astype(F32) + update.reshape(n_res, length, dim)).astype(BF16)
    o_ref[...] = result
    if with_bias:
        zbuf[...] = result
        local_bias(normed_tokens(), next_b, nb_send)
        arrived = exchange.start(nb_send, nb_recv, broadcast=True)
        arrived()
        for h in range(bias_ref.shape[0]):
            bias_ref[h] = rows_of(nb_recv, h).astype(F32).T * LOG2E
    else:
        bias_ref[...] = jnp.zeros_like(bias_ref)
    own.wait()

    def m_wait(step, carry):
        other = lax.rem(me + step, n_dev)
        m_copy(other, other).wait_recv()
        m_copy(other, me).wait_send()
        return carry

    lax.fori_loop(1, n_dev, m_wait, 0)


def pair_stack(pair_loc, m_half, masks, stacked, layer, with_bias):
    n_res, length, dim = pair_loc.shape
    n_dev = masks['n_dev']
    tri = stacked['tmo_out'].shape[1]
    heads = masks['pair_heads']
    row_heads = stacked['row_bias'].shape[1]
    n_chan = tri // n_dev
    next_layer = layer + 1 if with_bias else layer
    names = ('tmo_w', 'tmo_proj', 'tmo_out', 'tmi_w', 'tmi_proj', 'tmi_out', 'tas_qkvg', 'tas_bias', 'tas_out', 'tae_qkvg', 'tae_bias', 'tae_out', 'ptr_in', 'ptr_out')
    weights = [stacked[k] for k in names] + [stacked['row_bias']]
    specs = [layer_of(w, layer) for w in weights[:-1]] + [layer_of(weights[-1], next_layer)]
    width = stacked['tas_out'].shape[1]
    n_phases = 9
    scratch = [
        pltpu.VMEM((n_res, length, dim), BF16), pltpu.VMEM((n_res, length, dim), BF16),
        pltpu.VMEM((n_dev * n_res * n_res, LANES), F32),
        pltpu.VMEM((2, n_dev, 2, n_chan, n_res, length), BF16), pltpu.VMEM((2, n_dev, 2, n_chan, n_res, length), BF16),
        pltpu.VMEM((2, n_dev, n_chan, n_res, length), F32), pltpu.VMEM((2, n_dev, n_chan, n_res, length), F32),
        pltpu.VMEM((n_res * (tri + 8), length), F32), pltpu.VMEM((n_res * length, dim), F32),
        pltpu.VMEM((n_res, 4 * width, length), BF16), pltpu.VMEM((n_res, width, length), BF16),
        pltpu.VMEM((heads, length, length), F32),
        pltpu.VMEM((2, heads, n_res, length), BF16), pltpu.VMEM((2, n_dev, heads, n_res, length), BF16),
        pltpu.VMEM((2, n_dev, n_res, n_res, dim), BF16), pltpu.VMEM((n_dev, n_res, n_res, dim), BF16), pltpu.VMEM((n_dev, n_res, n_res, dim), BF16),
        pltpu.VMEM((row_heads, n_res, length), BF16), pltpu.VMEM((n_dev, row_heads, n_res, length), BF16),
        pltpu.SemaphoreType.DMA((n_phases, n_dev)), pltpu.SemaphoreType.DMA((n_phases, n_dev)),
        pltpu.SemaphoreType.DMA((n_dev,)), pltpu.SemaphoreType.DMA((n_dev,)), pltpu.SemaphoreType.DMA,
    ]
    return pl.pallas_call(
        functools.partial(pair_kernel, n_dev, with_bias),
        grid=(1,),
        in_specs=[VMEM_SPEC] * 4 + [ANY_SPEC] + specs,
        out_specs=[VMEM_SPEC, ANY_SPEC, VMEM_SPEC],
        out_shape=[jax.ShapeDtypeStruct(pair_loc.shape, BF16), jax.ShapeDtypeStruct(m_half.shape, BF16), jax.ShapeDtypeStruct((row_heads, length, length), F32)],
        scratch_shapes=scratch,
        compiler_params=pltpu.CompilerParams(collective_id=3 * layer + 2, has_side_effects=True),
        cost_estimate=pl.CostEstimate(flops=4_000_000_000, bytes_accessed=16_000_000, transcendentals=4_000_000),
        name='pair_stack',
    )(pair_loc, masks['pair_rows'].reshape(1, n_res * length), masks['start'], masks['end'], m_half, *weights)


def pair_stack(pair_loc, m_half, masks, stacked, layer, with_bias):
    n_res, length, dim = pair_loc.shape
    n_dev = masks['n_dev']
    tri = stacked['tmo_out'].shape[1]
    heads = masks['pair_heads']
    row_heads = stacked['row_bias'].shape[1]
    n_chan = tri // n_dev
    next_layer = layer + 1 if with_bias else layer
    names = ('tmo_w', 'tmo_proj', 'tmo_out', 'tmi_w', 'tmi_proj', 'tmi_out', 'tas_qkvg', 'tas_bias', 'tas_out', 'tae_qkvg', 'tae_bias', 'tae_out', 'ptr_in', 'ptr_out')
    weights = [stacked[k] for k in names] + [stacked['row_bias']]
    specs = [layer_of(w, layer) for w in weights[:-1]] + [layer_of(weights[-1], next_layer)]
    width = stacked['tas_out'].shape[1]
    n_phases = 9
    scratch = [
        pltpu.VMEM((n_res, length, dim), BF16), pltpu.VMEM((n_res, length, dim), BF16),
        pltpu.VMEM((n_dev * n_res * n_res, LANES), F32),
        pltpu.VMEM((2, n_dev, 2, n_chan, n_res, length), BF16), pltpu.VMEM((2, n_dev, 2, n_chan, n_res, length), BF16),
        pltpu.VMEM((2, n_dev, n_chan, n_res, length), F32), pltpu.VMEM((2, n_dev, n_chan, n_res, length), F32),
        pltpu.VMEM((n_res * (tri + 8), length), F32), pltpu.VMEM((n_res * length, dim), F32),
        pltpu.VMEM((n_res, 4 * width, length), BF16), pltpu.VMEM((n_res, width, length), BF16),
        pltpu.VMEM((heads, length, length), F32),
        pltpu.VMEM((2, heads, n_res, length), BF16), pltpu.VMEM((2, n_dev, heads, n_res, length), BF16),
        pltpu.VMEM((2, n_dev, n_res, n_res, dim), BF16), pltpu.VMEM((n_dev, n_res, n_res, dim), BF16), pltpu.VMEM((n_dev, n_res, n_res, dim), BF16),
        pltpu.VMEM((row_heads, n_res, length), BF16), pltpu.VMEM((n_dev, row_heads, n_res, length), BF16),
        pltpu.SemaphoreType.DMA((n_phases, n_dev)), pltpu.SemaphoreType.DMA((n_phases, n_dev)),
        pltpu.SemaphoreType.DMA((n_dev,)), pltpu.SemaphoreType.DMA((n_dev,)), pltpu.SemaphoreType.DMA,
    ]
    return pl.pallas_call(
        functools.partial(pair_kernel, n_dev, with_bias),
        grid=(1,),
        in_specs=[VMEM_SPEC] * 4 + [ANY_SPEC] + specs,
        out_specs=[VMEM_SPEC, ANY_SPEC, VMEM_SPEC],
        out_shape=[jax.ShapeDtypeStruct(pair_loc.shape, BF16), jax.ShapeDtypeStruct(m_half.shape, BF16), jax.ShapeDtypeStruct((row_heads, length, length), F32)],
        scratch_shapes=scratch,
        compiler_params=pltpu.CompilerParams(collective_id=3 * layer + 2, has_side_effects=True),
        cost_estimate=pl.CostEstimate(flops=4_000_000_000, bytes_accessed=16_000_000, transcendentals=4_000_000),
        name='pair_stack',
    )(pair_loc, masks['pair_rows'].reshape(1, n_res * length), masks['start'], masks['end'], m_half, *weights)


def head_bias(pair_norm, w_bias):
    return jnp.einsum('ijc,ch->hij', pair_norm, w_bias, preferred_element_type=F32).astype(BF16)


def gather_bias(pair_rows, w_bias):
    full = lax.all_gather(head_bias(layer_norm(pair_rows), w_bias), GROUP_AXIS, axis=1, tiled=True)
    return jnp.swapaxes(full, 1, 2).astype(F32) * LOG2E


def outer_product_kernel(n_dev, early_ref, late_ref, b_ref, w_ref, o_ref, stage, left, rows, flat, slots, *ring_sems):
    half = early_ref.shape[0]
    dim = early_ref.shape[1] // 2
    length = early_ref.shape[2]
    n_half = n_dev * half
    pitch = stage.shape[2] // dim
    parts = [slice(part * LANES, (part + 1) * LANES) for part in range(length // LANES)]
    me = lax.axis_index(GROUP_AXIS)
    entry_barrier(n_dev, me)
    ring = ChipRing(n_dev, me, late_ref.at[:, pl.ds(dim, dim)], slots, *ring_sems)
    ring.send(1)

    def spread(k, source, src):
        for r in range(half):
            tile = source(r).astype(F32)
            for part, lanes in enumerate(parts):
                for lo in range(0, dim, 8):
                    stage[k, part, pl.ds(lo * pitch + src * half + r, 8, stride=pitch), :] = tile[lo:lo + 8, lanes]

    def collect(k):
        for e in range(dim):
            for part, lanes in enumerate(parts):
                rows[e, k * n_half:(k + 1) * n_half, lanes] = stage[k, part, e * pitch:e * pitch + n_half, :].astype(BF16)

    def spread_early(lo, hi):
        def one(src, carry):
            spread(0, lambda r: b_ref[src, r], src)
            return carry
        lax.fori_loop(lo, hi, one, 0)

    def spread_late(src):
        spread(1, lambda r: slots[src, r], src)

    hops = ring.right_hops
    shares = [n_dev * k // hops for k in range(hops + 1)]
    spread(1, lambda r: late_ref[r, dim:2 * dim, :], me)
    for k, ab_ref in enumerate((early_ref, late_ref)):
        for r in range(half):
            left[(k * half + r) * dim:(k * half + r + 1) * dim, :] = ab_ref[r, 0:dim, :]
    for hop in range(1, hops + 1):
        spread_early(shares[hop - 1], shares[hop])
        if hop == hops:
            collect(0)
        ring.receive(hop)
        ring.send(hop + 1)
        for away in ([0] if hop == 1 else ring.arrivals(hop - 1)):
            spread_late(ring.receive_mate(away))
        for away in ring.arrivals(hop):
            spread_late(ring.device(away))
    for away in ring.arrivals(hops):
        spread_late(ring.receive_mate(away))
    collect(1)

    def one(step, carry):
        some = [step * 4 + k for k in range(4)]
        products = [lax.dot_general(left[...], rows[e], NT, preferred_element_type=F32).astype(BF16) for e in some]
        for e, product in zip(some, products):
            for i in range(2 * half):
                flat[i, pl.ds(pl.multiple_of(e * dim, dim), dim), :] = product[i * dim:(i + 1) * dim, :]
        return carry

    lax.fori_loop(0, dim // 4, one, 0)
    for i in range(2 * half):
        o_ref[i] = jnp.dot(w_ref[...], flat[i], preferred_element_type=F32).T
    ring.drain()


def outer_update(ab_halves, b_early, overlap, stacked, layer, n_dev):
    half, n_ab, seq_all = ab_halves[0].shape
    opm_dim = n_ab // 2
    n_half = n_dev * half
    length = 2 * n_half
    dim = stacked['opm_w'].shape[1]
    update = pl.pallas_call(
        functools.partial(outer_product_kernel, n_dev),
        grid=(1,),
        in_specs=[VMEM_SPEC] * 3 + [layer_of(stacked['opm_w'], layer)], out_specs=VMEM_SPEC,
        out_shape=jax.ShapeDtypeStruct((2 * half, length, dim), F32),
        scratch_shapes=[pltpu.VMEM((2, seq_all // LANES, opm_dim * (n_half + 8), LANES), F32),
                        pltpu.VMEM((2 * half * opm_dim, seq_all), BF16), pltpu.VMEM((opm_dim, length, seq_all), BF16),
                        pltpu.VMEM((2 * half, opm_dim * opm_dim, length), BF16), pltpu.VMEM(b_early.shape, BF16)] + ring_semaphores(n_dev),
        compiler_params=pltpu.CompilerParams(collective_id=3 * stacked['opm_w'].shape[0] + 1 + layer, has_side_effects=True),
        cost_estimate=pl.CostEstimate(flops=4_000_000_000, bytes_accessed=6_000_000, transcendentals=0),
        name='outer_product',
    )(ab_halves[0], ab_halves[1], b_early, stacked['opm_w'])
    update = update.reshape(2 * half, 2, n_dev, half, dim)
    update = jnp.swapaxes(update, 1, 2).reshape(2 * half, length, dim)
    return update / (1e-3 + overlap)[:, :, None]


def first_gather_kernel(n_dev, z_ref, b_ref, masks_ref, bias_ref, full_ref, stage, bias_send, bias_recv, sends, recvs):
    n_res, length, dim = z_ref.shape
    me = lax.axis_index(GROUP_AXIS)
    entry_barrier(n_dev, me)
    exchange = Exchange(n_dev, me, sends, recvs)
    masks_arrived = exchange.start(masks_ref, full_ref, broadcast=True)
    rows = lax.dot_general(b_ref[...], layer_norm_f32(z_ref[...].astype(F32).reshape(n_res * length, dim)), NT, preferred_element_type=F32)
    heads = bias_send.shape[0]
    for i in range(n_res):
        stage[pl.ds(i, heads, stride=n_res), :] = rows[:, i * length:(i + 1) * length]
    bias_send[...] = stage[...].reshape(heads, n_res, length).astype(BF16)
    exchange.start(bias_send, bias_recv, broadcast=True)()
    for h in range(heads):
        bias_ref[h] = bias_recv[:, h].astype(F32).reshape(length, length).T * LOG2E
    masks_arrived()


def first_gather(pair_loc, packed_masks, stacked, n_dev):
    n_res, length, dim = pair_loc.shape
    heads = stacked['row_bias'].shape[1]
    return pl.pallas_call(
        functools.partial(first_gather_kernel, n_dev),
        grid=(1,),
        in_specs=[VMEM_SPEC, layer_of(stacked['row_bias'], 0), VMEM_SPEC], out_specs=[VMEM_SPEC, VMEM_SPEC],
        out_shape=[jax.ShapeDtypeStruct((heads, length, length), F32), jax.ShapeDtypeStruct((n_dev,) + packed_masks.shape, BF16)],
        scratch_shapes=[pltpu.VMEM((heads * n_res, length), F32), pltpu.VMEM((heads, n_res, length), BF16), pltpu.VMEM((n_dev, heads, n_res, length), BF16),
                        pltpu.SemaphoreType.DMA((2, n_dev)), pltpu.SemaphoreType.DMA((2, n_dev))],
        compiler_params=pltpu.CompilerParams(collective_id=3 * stacked['row_bias'].shape[0], has_side_effects=True),
        cost_estimate=pl.CostEstimate(flops=1_000_000_000, bytes_accessed=2_000_000, transcendentals=0),
        name='first_gather',
    )(pair_loc, stacked['row_bias'], packed_masks)


def evoformer_block(m_arrays, pair_loc, bias_t, masks, stacked, layer, with_bias):
    heads = masks['msa_heads']
    early, ab_early, late = rows_and_columns(m_arrays, bias_t, masks, stacked, layer, heads)
    late, ab_late, m_early, b_early = late_columns(late, early, ab_early, masks, stacked, layer, heads)
    pair_loc = residual(pair_loc, outer_update((ab_early, ab_late), b_early, masks['overlap'], stacked, layer, masks['n_dev']))
    pair_loc, m_late, bias_t = pair_stack(pair_loc, late, masks, stacked, layer, with_bias)
    return (m_early, m_late), pair_loc, bias_t


WEIGHT_NAMES = ('row_qkvg', 'row_bias', 'row_out', 'col_qkvg', 'col_out', 'mtr_in', 'mtr_out', 'opm_proj', 'opm_out', 'tmo_proj', 'tmo_out',
                'tmi_proj', 'tmi_out', 'tas_qkvg', 'tas_bias', 'tas_out', 'tae_qkvg', 'tae_bias', 'tae_out', 'ptr_in', 'ptr_out')


def prepare_weights(weights):
    stacked = dict(zip(WEIGHT_NAMES, weights))
    for kind in ('tmo', 'tmi'):
        tri = stacked[kind + '_out'].shape[1]
        stacked[kind + '_w'] = jnp.swapaxes(stacked[kind + '_proj'][:, :, :4 * tri], 1, 2)
    for name in ('row_qkvg', 'col_qkvg', 'opm_proj', 'tas_qkvg', 'tae_qkvg'):
        stacked[name] = jnp.swapaxes(stacked[name], 1, 2)
    for name in ('row_bias', 'tas_bias', 'tae_bias'):
        stacked[name] = jnp.pad(jnp.swapaxes(stacked[name], 1, 2), ((0, 0), (0, -stacked[name].shape[2] % 8), (0, 0)))
    n_layers, flat, dim = stacked['opm_out'].shape
    opm_dim = stacked['opm_proj'].shape[1] // 2
    stacked['opm_w'] = jnp.transpose(stacked['opm_out'].reshape(n_layers, opm_dim, opm_dim, dim), (0, 3, 2, 1)).reshape(n_layers, dim, flat)
    return stacked


def pack_masks(msa_mask, pair_mask):
    return jnp.concatenate([msa_mask, pair_mask], 0).astype(BF16)


def make_masks(msa_mask, pair_mask, full, n_dev):
    shard_idx = lax.axis_index(GROUP_AXIS)
    n_seq, length = msa_mask.shape
    n_res = pair_mask.shape[0]
    full = full.astype(F32)
    full_msa = full[:, :n_seq].reshape(n_dev * n_seq, length)
    full_pair = full[:, n_seq:].reshape(n_dev * n_res, length)
    res_mask = lax.dynamic_slice_in_dim(full_msa, shard_idx * n_res, n_res, 1).T
    end_mask = lax.dynamic_slice_in_dim(full_pair, shard_idx * n_res, n_res, 1).T
    lanes = lambda mask: jnp.broadcast_to(mask.astype(F32)[:, :, None], mask.shape + (length,))
    return {
        'n_dev': n_dev,
        'seq': lanes(msa_mask),
        'res': lanes(res_mask),
        'res_row': res_mask[:, None, :],
        'pair_rows': pair_mask.astype(F32),
        'start': lanes(pair_mask),
        'end': lanes(end_mask),
        'overlap': jnp.dot(res_mask, full_msa, precision=lax.Precision.DEFAULT, preferred_element_type=F32),
    }


def solution(mesh):
    row_spec = P((PARTS_AXIS, GROUP_AXIS))
    n_dev = mesh.shape[GROUP_AXIS]

    def local_body(value_a7, pair_loc, msa_mask, pair_mask, *weights):
        stacked = prepare_weights(weights)
        bias_t, full = first_gather(pair_loc, pack_masks(msa_mask, pair_mask), stacked, n_dev)
        masks = make_masks(msa_mask, pair_mask, full, n_dev)
        masks['msa_heads'] = weights[1].shape[2]
        masks['pair_heads'] = weights[14].shape[2]
        n_layers = weights[0].shape[0]
        m_arrays = (value_a7,)
        for layer in range(n_layers):
            m_arrays, pair_loc, bias_t = evoformer_block(m_arrays, pair_loc, bias_t, masks, stacked, layer, layer + 1 < n_layers)
        n_seq, length, dim = value_a7.shape
        value_a7 = jnp.transpose(jnp.stack(m_arrays, 1), (3, 0, 1, 2, 4)).reshape(n_seq, length, dim)
        return value_a7, pair_loc

    def run_blocks(*arrays):
        n_weights = len(arrays) - 4
        return jax.shard_map(local_body, mesh=mesh, in_specs=(row_spec,) * 4 + (P(),) * n_weights, out_specs=(row_spec, row_spec), check_vma=False)(*arrays)

    return run_blocks
```
